128 devices in a mesh: enc: 8 (over z, core), ctx: 16 (over y, x).
Axes of the slice: x: 4, y: 4, z: 4, core: 2. Of those that a mesh axis runs over, the one named last changes fastest.
Arguments:
- patches: bfloat16 [6144, 1280], P('enc'), may hold values from -17 to 17
- patch_image: int32 [6144], P('enc'), may hold values from 63 to 1535, as said below
- vit_gain: float32 [1280], replicated, may hold values from 0.1 to 1.9
- vit_qkv: bfloat16 [1280, 16, 240], P(None, 'ctx')
- vit_proj: bfloat16 [1280, 1280], P('ctx'), may hold values from -0.15625 to 0.15625
- merge_gain: float32 [1280], replicated, may hold values from 0.1 to 1.9
- merge_up: bfloat16 [5120, 5120], P(None, 'ctx'), may hold values from -0.078125 to 0.078125
- merge_down: bfloat16 [5120, 8192], P('ctx', 'enc'), may hold values from -0.078125 to 0.078125
- text_embed: bfloat16 [6144, 8192], P('ctx', 'enc'), may hold values from -17 to 17
- placeholder_unit: int32 [6144], replicated, may hold values from -1 to 1535, as said below
- doc_id: int32 [6144], replicated, may hold values from 0 to 31, never falling along the last dimension, each value on 1 to 3456 neighbouring positions
- dec_gain: float32 [8192], replicated, may hold values from 0.1 to 1.9
- dec_wq: bfloat16 [8192, 4096], P(None, 'enc')
- dec_wk: bfloat16 [8192, 1024], P(None, 'enc')
- dec_wv: bfloat16 [8192, 1024], P(None, 'enc'), may hold values from -0.0625 to 0.0625
Outputs:
- attended: bfloat16 [6144, 4096], P('ctx', 'enc')
The draws below stay inside these ranges and needn't reach their ends.
Inputs may be any that keep to these rules, and one draw needn't show every extreme that they name: `patch_image`: the patches of an image are consecutive, start at a multiple of 4, number a multiple of 4 and at most 256, and lie within one aligned block of 768 patches; image numbers never fall and differ between images; in every such block some image has exactly 256 patches. `placeholder_unit`: -1 marks a text position. Every unit appears exactly once; the units of one image fill consecutive placeholders in their order; the placeholders of an aligned block of 384 positions are consecutive and number at most 192, and some block holds exactly 192. `doc_id`: document numbers never fall; a document has at most 3456 positions, and some document exactly 3456.
All inputs are finite; a program needn't handle non-finite values.
Results may differ from the reference program's by a relative error of at most 0.0085.
Values may be sent and summed in bfloat16 or wider, within the bound.
A program may use at most 128 MiB of HBM per device.

```python
import math
import jax
import jax.numpy as jnp
import numpy as np
from jax import lax

VW = 1280
VH = 16
D = 8192
HD = 128
QPK = 4
IMG_MAX = 256
TOK_CTX = 384
VHD = 80
MW = 5120
KV_HEADS = 8
TOKENS = 6144
PATCHES = 6144
GROUP_PATCHES = 768
UNITS = 1536
DOCS = 32
DOC_MAX = 3456
N_ENC = 8
N_CTX = 16


def drawn_table(key, row_count, col_count):
    return jnp.clip(jax.random.normal(jax.random.fold_in(key, 1), (row_count, col_count), jnp.float32), -4.0, 4.0)


def draw_patches(key, part):
    values = drawn_table(jax.random.fold_in(key, 101), PATCHES, VW)
    return values.astype(jnp.bfloat16)


def draw_text_embed(key, part):
    values = drawn_table(jax.random.fold_in(key, 102), TOKENS, D)
    return values.astype(jnp.bfloat16)


def unit_images(key):
    group_units = PATCHES // (4 * N_ENC)
    most_units = IMG_MAX // 4
    chance = jax.random.randint(jax.random.fold_in(key, 11), (N_ENC, group_units), 0, max(most_units // 2, 1))
    places = jnp.arange(group_units, dtype=jnp.int32)
    cuts = (chance == 0) | (places % most_units == 0)[None, :]
    cuts = jnp.where((places < most_units)[None, :], (places == 0)[None, :], cuts)
    closing = jnp.concatenate([cuts[:, 1:], jnp.ones((N_ENC, 1), dtype=bool)], axis=1)
    marks = jnp.where(closing, places[None, :], group_units).astype(jnp.int32)
    last_unit = lax.cummin(marks, axis=1, reverse=True)
    return (last_unit + group_units * jnp.arange(N_ENC, dtype=jnp.int32)[:, None]).reshape(-1).astype(jnp.int32)


def draw_patch_image(key, part):
    return jnp.repeat(unit_images(key), 4).astype(jnp.int32)


def draw_placeholder_unit(key, part):
    images = unit_images(key)
    image_rank = jax.random.permutation(jax.random.fold_in(key, 12), UNITS).astype(jnp.int32)
    scores = image_rank[images] * UNITS + jnp.arange(UNITS, dtype=jnp.int32)
    unit_order = jnp.argsort(scores, stable=True).astype(jnp.int32)
    quarter = TOK_CTX // 4
    pair_count = N_CTX // 2
    shifts = jax.random.randint(jax.random.fold_in(key, 13), (pair_count,), -quarter, quarter + 1)
    chosen = jax.random.randint(jax.random.fold_in(key, 14), (), 0, pair_count)
    flip_sign = 2 * jax.random.randint(jax.random.fold_in(key, 15), (), 0, 2) - 1
    shifts = jnp.where(jnp.arange(pair_count) == chosen, flip_sign * quarter, shifts)
    counts = jnp.stack([quarter + shifts, quarter - shifts], axis=1).reshape(-1)
    counts = counts[jax.random.permutation(jax.random.fold_in(key, 16), N_CTX)]
    starts = jax.random.randint(jax.random.fold_in(key, 17), (N_CTX,), 0, TOK_CTX - counts + 1)
    before = jnp.cumsum(counts) - counts
    places = jnp.arange(TOK_CTX, dtype=jnp.int32)
    inside = (places[None, :] >= starts[:, None]) & (places[None, :] < (starts + counts)[:, None])
    global_rank = jnp.clip(before[:, None] + places[None, :] - starts[:, None], 0, UNITS - 1)
    return jnp.where(inside, unit_order[global_rank], -1).reshape(-1).astype(jnp.int32)


def draw_vit_qkv(key, part):
    base = jnp.clip(jax.random.normal(jax.random.fold_in(key, 41), (VW, VH, 3, VHD), jnp.float32), -4.0, 4.0) * VW ** (-0.5)
    return base.reshape(VW, VH, 3 * VHD).astype(jnp.bfloat16)


def key_table(key):
    return jnp.clip(jax.random.normal(jax.random.fold_in(key, 31), (D, KV_HEADS, HD), jnp.float32), -4.0, 4.0) * D ** (-0.5)


def draw_dec_wk(key, part):
    return key_table(key).reshape(D, KV_HEADS * HD).astype(jnp.bfloat16)


def draw_dec_wq(key, part):
    noise = jnp.clip(jax.random.normal(jax.random.fold_in(key, 32), (D, KV_HEADS, QPK, HD), jnp.float32), -4.0, 4.0) * D ** (-0.5)
    return noise.reshape(D, KV_HEADS * QPK * HD).astype(jnp.bfloat16)


def steps_of(rng, extent, split, low, top_value):
    gain, own = 1.0, jax.random.fold_in(rng, 6)
    for dim, shards_of in split:
        draws = jnp.exp(jax.random.uniform(jax.random.fold_in(own, dim), (shards_of,), jnp.float32, low / len(split), top_value / len(split)))
        gain = gain * jnp.repeat(draws, extent[dim] // shards_of).reshape([-1 if axis == dim else 1 for axis in range(len(extent))])
    return gain


def split_up(amount, total, bound, skew):
    loads = [(1 << 20) // math.isqrt(grade ** skew) + 1 for grade in range(2, amount + 1)]
    rest, given = total - bound - (amount - 1), [1] * (amount - 1)
    while rest > 0:
        movable = [i for i in range(amount - 1) if given[i] < bound]
        whole, left = sum([loads[i] for i in movable]), rest
        for i in movable:
            addition = min(bound - given[i], max(1, left * loads[i] // whole), rest)
            given[i] = given[i] + addition
            rest = rest - addition
    return np.array([bound] + given)


def ragged_sizes(stream_key, number_of, total, limit, lean):
    if number_of == 2:
        one = jax.random.randint(stream_key, (), max(1, total - limit), min(limit, total - 1) + 1)
        return jnp.stack([one, total - one])
    tallies = jnp.asarray(split_up(number_of, total, limit, lean), jnp.int32)
    couples = (number_of - 1) // 2
    source_of, receiver = tallies[1:1 + 2 * couples:2], tallies[2:2 + 2 * couples:2]
    slack = jnp.minimum(source_of - 1, limit - receiver)
    passed = jax.random.randint(jax.random.fold_in(stream_key, 1), (couples,), 0, 1 << 20) % (slack + 1)
    tallies = tallies.at[1:1 + 2 * couples:2].set(source_of - passed).at[2:2 + 2 * couples:2].set(receiver + passed)
    return tallies[jax.random.permutation(jax.random.fold_in(stream_key, 2), number_of)]


def normal_values(stream_key, shape, deviation, limit, split=(), held_as=jnp.bfloat16):
    loudness = steps_of(stream_key, shape, split, -0.22, 0.18) if split else 1.0
    drawn = jax.random.normal(stream_key, shape, jnp.float32) * deviation * loudness
    return jnp.minimum(jnp.maximum(drawn, -limit), limit).astype(held_as)


def setup_inputs(seed: int = 0) -> dict:
    streams_of = jax.random.split(jax.random.key(seed), 16)
    return {
        "patches": draw_patches(jax.random.fold_in(streams_of[15], 71), 0),
        "patch_image": draw_patch_image(jax.random.fold_in(streams_of[15], 71), 0),
        "vit_gain": jnp.clip(1.0 + 0.18 * jax.random.normal(streams_of[2], (VW,), jnp.float32), 0.1, 1.9),
        "vit_qkv": draw_vit_qkv(jax.random.fold_in(streams_of[15], 71), 0),
        "vit_proj": normal_values(streams_of[4], (VH * VHD, VW), VW ** -0.5, 0.15625, ((0, 16),)),
        "merge_gain": jnp.clip(1.0 + 0.18 * jax.random.normal(streams_of[5], (VW,), jnp.float32), 0.1, 1.9),
        "merge_up": normal_values(streams_of[6], (MW, MW), MW ** -0.5, 0.078125, ((1, 16),)),
        "merge_down": normal_values(streams_of[7], (MW, D), MW ** -0.5, 0.078125, ((0, 16), (1, 8))),
        "text_embed": draw_text_embed(jax.random.fold_in(streams_of[15], 71), 0),
        "placeholder_unit": draw_placeholder_unit(jax.random.fold_in(streams_of[15], 71), 0),
        "doc_id": jnp.searchsorted(jnp.cumsum(ragged_sizes(streams_of[10], DOCS, TOKENS, DOC_MAX, 2)), jnp.arange(TOKENS), side="right").astype(jnp.int32),
        "dec_gain": jnp.clip(1.0 + 0.18 * jax.random.normal(streams_of[11], (D,), jnp.float32), 0.1, 1.9),
        "dec_wq": draw_dec_wq(jax.random.fold_in(streams_of[15], 71), 0),
        "dec_wk": draw_dec_wk(jax.random.fold_in(streams_of[15], 71), 0),
        "dec_wv": normal_values(streams_of[14], (D, KV_HEADS * HD), D ** -0.5, 0.0625, ((1, 8),)),
    }


EPSILON = 1e-06
NEGATIVE = -1e+30

def layer_norm(values, scaling):
    widened = values.astype(jnp.float32)
    center = widened - lax.optimization_barrier(jnp.mean(widened, axis=1, keepdims=True))
    spread = lax.optimization_barrier(jnp.mean(center * center, axis=1, keepdims=True))
    return (center * lax.rsqrt(spread + EPSILON) * scaling).astype(jnp.bfloat16)

def masked_attention(queries, keys_in, values_in, allowed_rows):
    head_count, row_count, head_width = queries.shape
    block_rows = math.gcd(row_count, 512)
    scaling = head_width ** (-0.5)
    keys_wide = keys_in.astype(jnp.float32)
    values_wide = values_in.astype(jnp.float32)

    def one_block(offset):
        query_block = lax.dynamic_slice_in_dim(queries, offset, block_rows, 1).astype(jnp.float32)
        allowed = allowed_rows(offset, block_rows)
        scores = jnp.einsum('hqd,hkd->hqk', query_block, keys_wide) * scaling
        scores = jnp.where(allowed[None], scores, NEGATIVE)
        highest = lax.optimization_barrier(jnp.max(scores, axis=2, keepdims=True))
        weights = jnp.exp(scores - highest)
        totals = lax.optimization_barrier(jnp.sum(weights, axis=2, keepdims=True))
        rounded = lax.optimization_barrier(weights.astype(jnp.bfloat16)).astype(jnp.float32)
        mixture = jnp.einsum('hqk,hkd->hqd', rounded, values_wide)
        return (mixture / totals).astype(jnp.bfloat16)
    offsets = (jnp.arange(row_count // block_rows) * block_rows).astype(jnp.int32)
    blocks = lax.map(one_block, offsets)
    return blocks.transpose(1, 0, 2, 3).reshape(head_count, row_count, head_width)

def reference(patches, patch_image, vit_gain, vit_qkv, vit_proj, merge_gain, merge_up, merge_down, text_embed, placeholder_unit, doc_id, dec_gain, dec_wq, dec_wk, dec_wv):

    def vision_group(inputs):
        group_rows, group_ids = inputs
        normed = layer_norm(group_rows, vit_gain)
        packed = jnp.dot(normed, vit_qkv.reshape(VW, VH * 3 * VHD), preferred_element_type=jnp.float32)
        packed = packed.astype(jnp.bfloat16).reshape(GROUP_PATCHES, VH, 3, VHD).transpose(2, 1, 0, 3)

        def same_image(offset, block_rows):
            block_ids = lax.dynamic_slice_in_dim(group_ids, offset, block_rows, 0)
            return block_ids[:, None] == group_ids[None, :]
        attended_heads = masked_attention(packed[0], packed[1], packed[2], same_image)
        flat_heads = attended_heads.transpose(1, 0, 2).reshape(GROUP_PATCHES, VH * VHD)
        head_terms = jnp.dot(flat_heads, vit_proj, preferred_element_type=jnp.float32)
        vit_out = (group_rows.astype(jnp.float32) + head_terms).astype(jnp.bfloat16)
        return layer_norm(lax.optimization_barrier(vit_out), merge_gain)
    merged = lax.map(vision_group, (patches.reshape(N_ENC, GROUP_PATCHES, VW), patch_image.reshape(N_ENC, GROUP_PATCHES)))
    unit_inputs = merged.reshape(UNITS, 4 * VW)
    hidden = jax.nn.gelu(jnp.dot(unit_inputs, merge_up, preferred_element_type=jnp.float32), approximate=False).astype(jnp.bfloat16)
    vision_rows = jnp.dot(hidden, merge_down, preferred_element_type=jnp.float32).astype(jnp.bfloat16)
    unit_index = jnp.clip(placeholder_unit, 0, UNITS - 1).astype(jnp.int32)
    sequence = jnp.where((placeholder_unit >= 0)[:, None], jnp.take(vision_rows, unit_index, axis=0), text_embed)
    widened = sequence.astype(jnp.float32)
    normed = (widened * lax.rsqrt(lax.optimization_barrier(jnp.mean(widened * widened, axis=1, keepdims=True)) + EPSILON) * dec_gain).astype(jnp.bfloat16)
    queries = jnp.dot(normed, dec_wq, preferred_element_type=jnp.float32).astype(jnp.bfloat16)
    queries = queries.reshape(TOKENS, KV_HEADS, QPK, HD).transpose(1, 2, 0, 3)
    keys_all = jnp.dot(normed, dec_wk, preferred_element_type=jnp.float32).astype(jnp.bfloat16)
    keys_all = keys_all.reshape(TOKENS, KV_HEADS, HD).transpose(1, 0, 2)
    values_all = jnp.dot(normed, dec_wv, preferred_element_type=jnp.float32).astype(jnp.bfloat16)
    values_all = values_all.reshape(TOKENS, KV_HEADS, HD).transpose(1, 0, 2)
    positions = jnp.arange(TOKENS, dtype=jnp.int32)

    def causal_docs(offset, block_rows):
        query_pos = offset + jnp.arange(block_rows, dtype=jnp.int32)
        query_docs = lax.dynamic_slice_in_dim(doc_id, offset, block_rows, 0)
        return (positions[None, :] <= query_pos[:, None]) & (doc_id[None, :] == query_docs[:, None])

    def one_group(inputs):
        group_queries, group_keys, group_values = inputs
        shared_keys = jnp.broadcast_to(group_keys[None], (QPK, TOKENS, HD))
        shared_values = jnp.broadcast_to(group_values[None], (QPK, TOKENS, HD))
        return masked_attention(group_queries, shared_keys, shared_values, causal_docs)
    attended = lax.map(one_group, (queries, keys_all, values_all))
    return attended.transpose(2, 0, 1, 3).reshape(TOKENS, KV_HEADS * QPK * HD)
```

```python
import functools
import math

import jax
import jax.numpy as jnp
from jax import lax
from jax.experimental import pallas as pl
from jax.experimental.pallas import tpu as pltpu
from jax.sharding import PartitionSpec as P

MESH = pl.DeviceIdType.MESH
VMEM = pltpu.VMEM
F32 = jnp.float32
BF16 = jnp.bfloat16

HD = 128
QPK = 4
EPSILON = 1e-06
NEGATIVE = -1e30
SIDE = 4


def places():
    e, c = lax.axis_index("enc"), lax.axis_index("ctx")
    return e // 2, lax.rem(e, 2), c // SIDE, lax.rem(c, SIDE)


def at_device(z, core, y, x):
    return {"enc": z * 2 + core, "ctx": y * SIDE + x}


def ring(position, distance):
    return lax.rem(position + distance, SIDE)


def remote(source, target, send_sem, recv_sem, device):
    return pltpu.make_async_remote_copy(
        src_ref=source,
        dst_ref=target,
        send_sem=send_sem,
        recv_sem=recv_sem,
        device_id=device,
        device_id_type=MESH,
    )


def greet():
    z, core, y, x = places()
    barrier = pltpu.get_barrier_semaphore()
    peers = []
    for d in range(1, SIDE):
        peers.append(at_device(z, core, y, ring(x, d)))
        peers.append(at_device(z, core, ring(y, d), x))
        peers.append(at_device(ring(z, d), core, y, x))
    peers.append(at_device(z, 1 - core, y, x))
    for peer in peers:
        pl.semaphore_signal(barrier, inc=1, device_id=peer, device_id_type=MESH)
    pl.semaphore_wait(barrier, len(peers))


class Gather:
    def __init__(self, buf, cut, rows, sems, columns=None):
        self.buf, self.cut, self.rows, self.columns = buf, cut, rows, columns
        self.send, self.recv = sems
        self.copies = {}

    def parts(self):
        cols = slice(None) if self.columns is None else self.columns
        return (slice(0, self.cut), cols), (slice(self.cut, self.rows), cols)

    def first(self, own):
        z, core, y, x = places()
        part_a, part_b = self.parts()
        copies = []
        for d in range(1, SIDE):
            copies.append(
                remote(
                    own.at[part_a],
                    self.buf.at[(y, x) + part_a],
                    self.send.at[0, d - 1],
                    self.recv.at[0, d - 1],
                    at_device(z, core, y, ring(x, d)),
                )
            )
            copies.append(
                remote(
                    own.at[part_b],
                    self.buf.at[(y, x) + part_b],
                    self.send.at[1, d - 1],
                    self.recv.at[1, d - 1],
                    at_device(z, core, ring(y, d), x),
                )
            )
        for copy in copies:
            copy.start()
        self.copies[1] = copies

    def second(self):
        z, core, y, x = places()
        for copy in self.copies[1]:
            copy.wait_recv()
        part_a, part_b = self.parts()
        copies = []
        for d in range(1, SIDE):
            rows_a = (y, slice(None)) + part_a
            rows_b = (slice(None), x) + part_b
            copies.append(
                remote(
                    self.buf.at[rows_a],
                    self.buf.at[rows_a],
                    self.send.at[2, d - 1],
                    self.recv.at[2, d - 1],
                    at_device(z, core, ring(y, d), x),
                )
            )
            copies.append(
                remote(
                    self.buf.at[rows_b],
                    self.buf.at[rows_b],
                    self.send.at[3, d - 1],
                    self.recv.at[3, d - 1],
                    at_device(z, core, y, ring(x, d)),
                )
            )
        for copy in copies:
            copy.start()
        self.copies[2] = copies

    def finish(self):
        for copy in self.copies[2]:
            copy.wait_recv()

    def drain(self):
        for copy in self.copies[1] + self.copies[2]:
            copy.wait_send()


class EncGather:
    def __init__(self, buf, sems):
        self.buf = buf
        self.send, self.recv = sems

    def first(self, own):
        z, core, y, x = places()
        slot = z * 2 + core
        copies = [
            remote(
                own,
                self.buf.at[slot],
                self.send.at[d - 1],
                self.recv.at[d - 1],
                at_device(ring(z, d), core, y, x),
            )
            for d in range(1, SIDE)
        ]
        copies.append(
            remote(
                own,
                self.buf.at[slot],
                self.send.at[3],
                self.recv.at[3],
                at_device(z, 1 - core, y, x),
            )
        )
        for copy in copies:
            copy.start()
        self.copies = copies

    def second(self):
        z, core, y, x = places()
        self.handed = []
        for d in range(1, SIDE):
            self.copies[d - 1].wait_recv()
            slot = ring(z, SIDE - d) * 2 + core
            copy = remote(
                self.buf.at[slot],
                self.buf.at[slot],
                self.send.at[3 + d],
                self.recv.at[3 + d],
                at_device(z, 1 - core, y, x),
            )
            copy.start()
            self.handed.append(copy)

    def finish(self):
        self.copies[3].wait_recv()
        for copy in self.handed:
            copy.wait_recv()

    def drain(self):
        for copy in self.copies + self.handed:
            copy.wait_send()


def normed(wide, gain):
    center = wide - jnp.mean(wide, axis=1, keepdims=True)
    spread = jnp.mean(center * center, axis=1, keepdims=True)
    return (center * lax.rsqrt(spread + EPSILON) * gain).astype(BF16)


def gelu(x):
    return 0.5 * x * (1.0 + lax.erf(x * math.sqrt(0.5)))


def vision_kernel(
    patches,
    image_row,
    gain,
    qkv,
    proj,
    merge_gain,
    up_hbm,
    text,
    hidden_all,
    text_all,
    heads_all,
    proj_all,
    q_s,
    k_s,
    v_s,
    o_s,
    lhs_s,
    norm_s,
    up_s,
    local_sem,
    heads_sems_s,
    heads_sems_r,
    proj_sems_s,
    proj_sems_r,
    swap_s,
    swap_r,
    text_s,
    text_r,
    hid_s,
    hid_r,
):
    z, core, y, x = places()
    rows = patches.shape[0]
    width = patches.shape[1]
    head = proj.shape[0]
    groups = heads_all.shape[3] // head
    group_rows = rows // groups
    half = width // 2
    cols = pl.ds(pl.multiple_of(core * half, 128), half)

    up_copy = pltpu.make_async_copy(up_hbm, up_s, local_sem.at[0])
    up_copy.start()
    own_text = pltpu.make_async_copy(text, text_all.at[z * 2 + core], local_sem.at[1])
    own_text.start()
    greet()
    proj_gather = Gather(proj_all, 48, head, (proj_sems_s, proj_sems_r), cols)
    proj_gather.first(proj)
    text_gather = EncGather(text_all, (text_s, text_r))
    text_gather.first(text)

    proj_all[y, x, :, cols] = proj[:, cols]

    chunk = 256

    def project(i, _):
        here = pl.ds(pl.multiple_of(i * chunk, chunk), chunk)
        block = normed(patches[here, :].astype(F32), gain[...])
        packed = jnp.dot(block, qkv[...], preferred_element_type=F32)
        q_s[here, :] = packed[:, 0:head].astype(BF16)
        k_s[here, :] = packed[:, head : 2 * head].astype(BF16)
        v_s[here, :] = packed[:, 2 * head : 3 * head].astype(BF16)
        return 0

    lax.fori_loop(0, rows // chunk, project, 0)
    proj_gather.second()

    scaling = head ** (-0.5)
    image_rows = jnp.broadcast_to(image_row[...], (128, rows))

    def attend(i, _):
        here = pl.ds(pl.multiple_of(i * chunk, chunk), chunk)
        ids_row = image_row[:, here]
        ids_col = jnp.broadcast_to(ids_row, (128, chunk)).T[:, 0:1]
        scores = lax.dot_general(
            q_s[here, :], k_s[...], (((1,), (1,)), ((), ())), preferred_element_type=F32
        )
        scores = jnp.where(ids_col == image_rows[0:1, :], scores * scaling, NEGATIVE)
        highest = jnp.max(scores, axis=1, keepdims=True)
        weights = jnp.exp(scores - highest)
        totals = jnp.sum(weights, axis=1, keepdims=True)
        mixture = jnp.dot(weights.astype(BF16), v_s[...], preferred_element_type=F32)
        o_s[here, :] = mixture / totals
        return 0

    lax.fori_loop(0, rows // chunk, attend, 0)
    packed_heads = jnp.concatenate(
        [o_s[j * group_rows : (j + 1) * group_rows, :] for j in range(groups)], axis=1
    )
    heads_all[y, x] = packed_heads.astype(BF16)
    heads_gather = Gather(heads_all, group_rows // 2, group_rows, (heads_sems_s, heads_sems_r))
    heads_gather.first(heads_all.at[y, x])
    proj_gather.finish()
    swap = remote(
        proj_all.at[:, :, :, cols],
        proj_all.at[:, :, :, cols],
        swap_s,
        swap_r,
        at_device(z, 1 - core, y, x),
    )
    proj_gather.drain()
    swap.start()
    heads_gather.second()
    swap.wait_recv()
    up_copy.wait()
    heads_gather.finish()

    for j in range(groups):
        lhs_s[j * group_rows : (j + 1) * group_rows, :] = jnp.concatenate(
            [
                heads_all[a, b, :, j * head : (j + 1) * head].astype(F32)
                for a in range(SIDE)
                for b in range(SIDE)
            ],
            axis=1,
        ).astype(BF16)

    def merge(i, _):
        here = pl.ds(pl.multiple_of(i * chunk, chunk), chunk)
        terms = jnp.dot(
            lhs_s[here, :], proj_all[...].reshape(width, width), preferred_element_type=F32
        )
        out = (patches[here, :].astype(F32) + terms).astype(BF16)
        ready = normed(out.astype(F32), merge_gain[...]).astype(F32)
        for g in range(width // 128):
            norm_s[g, here, :] = ready[:, g * 128 : (g + 1) * 128]
        return 0

    lax.fori_loop(0, rows // chunk, merge, 0)
    units = rows // 4
    total = jnp.zeros((units, up_s.shape[1]), F32)
    for k in range(4):
        quarter = jnp.concatenate(
            [norm_s[g, pl.ds(k, units, stride=4), :] for g in range(width // 128)], axis=1
        ).astype(BF16)
        total = total + jnp.dot(
            quarter, up_s[k * width : (k + 1) * width, :], preferred_element_type=F32
        )
    hidden_all[z * 2 + core] = gelu(total).astype(BF16)
    hidden_gather = EncGather(hidden_all, (hid_s, hid_r))
    hidden_gather.first(hidden_all.at[z * 2 + core])
    text_gather.second()
    hidden_gather.second()
    own_text.wait()
    text_gather.finish()
    hidden_gather.finish()
    heads_gather.drain()
    swap.wait_send()
    text_gather.drain()
    hidden_gather.drain()


def vision(patches, image_row, gain, qkv, proj, merge_gain, up, text):
    rows, width = patches.shape
    head = proj.shape[0]
    groups = 8
    units = rows // 4
    dma = pltpu.SemaphoreType.DMA
    whole = pl.BlockSpec(memory_space=VMEM)
    anywhere = pl.BlockSpec(memory_space=pl.ANY)
    return pl.pallas_call(
        vision_kernel,
        out_shape=(
            jax.ShapeDtypeStruct((8, units, up.shape[1]), BF16),
            jax.ShapeDtypeStruct((8, *text.shape), BF16),
        ),
        in_specs=[whole] * 6 + [anywhere, anywhere],
        out_specs=(whole, whole),
        scratch_shapes=[
            VMEM((SIDE, SIDE, rows // groups, groups * head), BF16),
            VMEM((SIDE, SIDE, head, width), BF16),
            VMEM((rows, head), BF16),
            VMEM((rows, head), BF16),
            VMEM((rows, head), BF16),
            VMEM((rows, head), F32),
            VMEM((rows, width), BF16),
            VMEM((width // 128, rows, 128), F32),
            VMEM(up.shape, BF16),
            dma((2,)),
            dma((4, 3)),
            dma((4, 3)),
            dma((4, 3)),
            dma((4, 3)),
            dma(()),
            dma(()),
            dma((7,)),
            dma((7,)),
            dma((7,)),
            dma((7,)),
        ],
        compiler_params=pltpu.CompilerParams(
            collective_id=1, has_side_effects=True, vmem_limit_bytes=44 * 2**20
        ),
        name="vision",
    )(patches, image_row, gain, qkv, proj, merge_gain, up, text)


def row_scale(total, count):
    return lax.rsqrt(total / count + EPSILON)


def merger_kernel(
    hidden_all,
    text_all,
    down,
    gain,
    wq_hbm,
    wk_hbm,
    wv_hbm,
    token_code,
    placeholder,
    text_q,
    text_kv,
    unit_qkv,
    unit_code,
    w_s,
    part_a,
    part_b,
    got_a,
    got_b,
    sum_a,
    sum_b,
    got_a2,
    got_b2,
    rows_all,
    norm_s,
    local_sem,
    rs_s,
    rs_r,
    row_s,
    row_r,
    kv_s,
    kv_r,
    uq_s,
    uq_r,
):
    z, core, y, x = places()
    slot = z * 2 + core
    nq = wq_hbm.shape[1]
    nk = wk_hbm.shape[1]
    blocks, tokens, cols = text_all.shape
    model = blocks * cols
    own_units = unit_qkv.shape[2]
    half = cols // 2

    loads = [
        pltpu.make_async_copy(wq_hbm, w_s.at[:, 0:nq], local_sem.at[0]),
        pltpu.make_async_copy(wk_hbm, w_s.at[:, nq : nq + nk], local_sem.at[1]),
        pltpu.make_async_copy(wv_hbm, w_s.at[:, nq + nk : nq + 2 * nk], local_sem.at[2]),
    ]
    for load in loads:
        load.start()
    greet()

    first = []
    for d in (1, 2, 3, 0):
        xp, yp = ring(x, d), ring(y, d)
        lhs_a = jnp.concatenate(
            [
                hidden_all[
                    2 * v + xp // 2,
                    pl.ds(pl.multiple_of(lax.rem(xp, 2) * own_units, own_units), own_units),
                    :,
                ]
                for v in range(SIDE)
            ],
            axis=0,
        )
        part_a[d] = jnp.dot(lhs_a, down[:, 0:half], preferred_element_type=F32).astype(BF16)
        if d:
            copy = remote(
                part_a.at[d],
                got_a.at[d - 1],
                rs_s.at[0, d - 1],
                rs_r.at[0, d - 1],
                at_device(z, core, y, xp),
            )
            copy.start()
            first.append(copy)
        lhs_b = jnp.concatenate([hidden_all[2 * yp], hidden_all[2 * yp + 1]], axis=0)
        part_b[d] = jnp.dot(lhs_b, down[:, half:], preferred_element_type=F32).astype(BF16)
        if d:
            copy = remote(
                part_b.at[d],
                got_b.at[d - 1],
                rs_s.at[1, d - 1],
                rs_r.at[1, d - 1],
                at_device(z, core, yp, x),
            )
            copy.start()
            first.append(copy)

    squares = jnp.zeros((tokens, 128), F32)
    for b in range(blocks):
        for g in range(cols // 128):
            piece = text_all[b, :, g * 128 : (g + 1) * 128].astype(F32)
            squares = squares + piece * piece
    scale = row_scale(jnp.sum(squares, axis=1, keepdims=True), model)
    for load in loads:
        load.wait()
    norm_s[...] = jnp.zeros_like(norm_s)

    def text_block(b, _):
        block = text_all[b].astype(F32) * scale * gain[pl.ds(b, 1), :]
        here = pl.ds(pl.multiple_of(b * cols, cols), cols)
        norm_s[...] += jnp.dot(block.astype(BF16), w_s[here, :], preferred_element_type=F32)
        return 0

    lax.fori_loop(0, blocks, text_block, 0)
    text_q[...] = norm_s[:, 0:nq].astype(BF16)
    text_kv[y, x] = norm_s[:, nq:].astype(BF16)

    lane_unit = lax.broadcasted_iota(jnp.int32, (128, 128), 0)
    token_rows = placeholder.shape[0]

    def units_block(b, _):
        unit = lane_unit + b * 128
        found = jnp.zeros((128, 128), jnp.int32)
        for r in range(token_rows):
            found = found + jnp.where(
                placeholder[r : r + 1, :] == unit, token_code[r : r + 1, :], 0
            )
        unit_code[pl.ds(b, 1), :] = jnp.sum(found.T, axis=0, keepdims=True)
        return 0

    lax.fori_loop(0, unit_code.shape[0], units_block, 0)

    for copy in first:
        copy.wait_recv()
    sum_a[...] = (
        part_a[0].astype(F32)
        + got_a[0].astype(F32)
        + got_a[1].astype(F32)
        + got_a[2].astype(F32)
    ).astype(BF16)
    sum_b[...] = (
        part_b[0].astype(F32)
        + got_b[0].astype(F32)
        + got_b[1].astype(F32)
        + got_b[2].astype(F32)
    ).astype(BF16)

    def own_rows(index):
        return pl.ds(pl.multiple_of(index * own_units, own_units), own_units)

    second = []
    for d in range(1, SIDE):
        xp, yp = ring(x, d), ring(y, d)
        second.append(
            remote(
                sum_a.at[own_rows(yp)],
                got_a2.at[d - 1],
                rs_s.at[2, d - 1],
                rs_r.at[2, d - 1],
                at_device(z, core, yp, x),
            )
        )
        second.append(
            remote(
                sum_b.at[own_rows(xp)],
                got_b2.at[d - 1],
                rs_s.at[3, d - 1],
                rs_r.at[3, d - 1],
                at_device(z, core, y, xp),
            )
        )
    for copy in second:
        copy.start()
    for copy in second:
        copy.wait_recv()
    rows_a = sum_a[own_rows(y), :].astype(F32)
    rows_b = sum_b[own_rows(x), :].astype(F32)
    for d in range(SIDE - 1):
        rows_a = rows_a + got_a2[d].astype(F32)
        rows_b = rows_b + got_b2[d].astype(F32)
    rows_all[slot] = jnp.concatenate([rows_a, rows_b], axis=1).astype(BF16)

    rows_gather = EncGather(rows_all, (row_s, row_r))
    rows_gather.first(rows_all.at[slot])
    kv_gather = Gather(text_kv, tokens // 2, tokens, (kv_s, kv_r))
    kv_gather.first(text_kv.at[y, x])
    rows_gather.second()
    rows_gather.finish()
    kv_gather.second()

    squares = jnp.zeros((own_units, 128), F32)
    for b in range(blocks):
        for g in range(cols // 128):
            piece = rows_all[b, :, g * 128 : (g + 1) * 128].astype(F32)
            squares = squares + piece * piece
    unit_scale = row_scale(jnp.sum(squares, axis=1, keepdims=True), model)
    norm_s[0:own_units, :] = jnp.zeros((own_units, nq + 2 * nk), F32)

    def unit_block(b, _):
        block = rows_all[b].astype(F32) * unit_scale * gain[pl.ds(b, 1), :]
        here = pl.ds(pl.multiple_of(b * cols, cols), cols)
        norm_s[0:own_units, :] += jnp.dot(
            block.astype(BF16), w_s[here, :], preferred_element_type=F32
        )
        return 0

    lax.fori_loop(0, blocks, unit_block, 0)
    unit_qkv[y, x] = norm_s[0:own_units, :].astype(BF16)
    unit_gather = Gather(unit_qkv, own_units // 2, own_units, (uq_s, uq_r))
    unit_gather.first(unit_qkv.at[y, x])
    unit_gather.second()
    unit_gather.finish()
    kv_gather.finish()
    for copy in first + second:
        copy.wait_send()
    rows_gather.drain()
    kv_gather.drain()
    unit_gather.drain()


def merger(hidden_all, text_all, down, gain, wq, wk, wv, token_code, placeholder):
    blocks, tokens, cols = text_all.shape
    nq, nk = wq.shape[1], wk.shape[1]
    wide = nq + 2 * nk
    own_units = hidden_all.shape[0] * hidden_all.shape[1] // (SIDE * SIDE)
    side_units = own_units * SIDE
    half = cols // 2
    dma = pltpu.SemaphoreType.DMA
    whole = pl.BlockSpec(memory_space=VMEM)
    anywhere = pl.BlockSpec(memory_space=pl.ANY)
    return pl.pallas_call(
        merger_kernel,
        out_shape=(
            jax.ShapeDtypeStruct((tokens, nq), BF16),
            jax.ShapeDtypeStruct((SIDE, SIDE, tokens, 2 * nk), BF16),
            jax.ShapeDtypeStruct((SIDE, SIDE, own_units, wide), BF16),
            jax.ShapeDtypeStruct((own_units * 16 // 128, 128), jnp.int32),
        ),
        in_specs=[whole] * 4 + [anywhere] * 3 + [whole] * 2,
        out_specs=(whole,) * 4,
        scratch_shapes=[
            VMEM((blocks * cols, wide), BF16),
            VMEM((SIDE, side_units, half), BF16),
            VMEM((SIDE, side_units, half), BF16),
            VMEM((SIDE - 1, side_units, half), BF16),
            VMEM((SIDE - 1, side_units, half), BF16),
            VMEM((side_units, half), BF16),
            VMEM((side_units, half), BF16),
            VMEM((SIDE - 1, own_units, half), BF16),
            VMEM((SIDE - 1, own_units, half), BF16),
            VMEM((blocks, own_units, cols), BF16),
            VMEM((tokens, wide), F32),
            dma((3,)),
            dma((4, 3)),
            dma((4, 3)),
            dma((7,)),
            dma((7,)),
            dma((4, 3)),
            dma((4, 3)),
            dma((4, 3)),
            dma((4, 3)),
        ],
        compiler_params=pltpu.CompilerParams(
            collective_id=2, has_side_effects=True, vmem_limit_bytes=56 * 2**20
        ),
        name="merger",
    )(hidden_all, text_all, down, gain, wq, wk, wv, token_code, placeholder)


def attention_kernel(
    where_ref,
    doc_smem,
    text_q,
    text_kv,
    unit_qkv,
    unit_code,
    doc_rows,
    unit_rows,
    out,
    q_s,
    peak_s,
    total_s,
    mix_s,
    bias_s,
):
    tokens, nq = text_q.shape
    nk = text_kv.shape[2] // 2
    heads = nq // HD
    units = unit_qkv.shape[0] * unit_qkv.shape[1]
    mine = where_ref[0]
    first_doc = doc_smem[mine, 0]
    scale = HD ** (-0.5) * math.log2(math.e)

    def column(rows):
        return jnp.concatenate(
            [jnp.broadcast_to(rows[g : g + 1, :], (128, 128)).T for g in range(tokens // 128)],
            axis=0,
        )

    query_doc = column(doc_rows[mine])
    query_unit = column(unit_rows[mine])
    query_at = mine * tokens + lax.broadcasted_iota(jnp.int32, (tokens, 128), 0)
    lane = lax.broadcasted_iota(jnp.int32, (tokens, 128), 1)

    picked = jnp.zeros((tokens, nq), F32)
    chunk = 384
    per_chunk = chunk // unit_qkv.shape[1]
    for b in range(units // chunk):
        chosen = jnp.concatenate(
            [
                (query_unit == lane + (b * chunk + g * 128)).astype(F32)
                for g in range(chunk // 128)
            ],
            axis=1,
        ).astype(BF16)
        source = unit_qkv[b * per_chunk : (b + 1) * per_chunk, :, 0:nq].reshape(chunk, nq)
        picked = picked + jnp.dot(chosen, source, preferred_element_type=F32)
    for j in range(heads):
        part = slice(j * HD, (j + 1) * HD)
        q_s[j] = jnp.where(query_unit >= 0, picked[:, part], text_q[:, part].astype(F32)).astype(
            BF16
        )
    peak_s[...] = jnp.full_like(peak_s, NEGATIVE)
    total_s[...] = jnp.zeros_like(total_s)
    mix_s[...] = jnp.zeros_like(mix_s)

    def fold(keys, values):
        for j in range(heads):
            scores = lax.dot_general(
                q_s[j], keys, (((1,), (1,)), ((), ())), preferred_element_type=F32
            )
            scores = scores + bias_s[...]
            before = peak_s[j]
            peak = jnp.maximum(before, jnp.max(scores, axis=1, keepdims=True))
            factor = jnp.exp2((before - peak) * scale)
            wide_peak = jnp.concatenate([peak] * (scores.shape[1] // 128), axis=1)
            weights = jnp.exp2((scores - wide_peak) * scale)
            peak_s[j] = peak
            total_s[j] = total_s[j] * factor + jnp.sum(weights, axis=1, keepdims=True)
            mix_s[j] = mix_s[j] * factor + jnp.dot(
                weights.astype(BF16), values, preferred_element_type=F32
            )

    def text_block(s, _):
        docs, unit_of = doc_rows[s], unit_rows[s]
        for g in range(tokens // 128):
            part = slice(g * 128, (g + 1) * 128)
            key_at = s * tokens + g * 128 + lane
            same = query_doc == docs[g : g + 1, :]
            text = unit_of[g : g + 1, :] < 0
            allowed = same & (key_at <= query_at) & text
            bias_s[:, part] = jnp.where(allowed, 0.0, NEGATIVE)
        block = text_kv[s]
        fold(block[:, 0:nk], block[:, nk:])
        return 0

    begin = jnp.int32(0)
    for s in range(doc_smem.shape[0]):
        begin = begin + (doc_smem[s, tokens - 1] < first_doc).astype(jnp.int32)
    lax.fori_loop(begin, mine + 1, text_block, 0)

    def unit_block(b, _):
        for g in range(chunk // 128):
            code = unit_code[pl.ds(b * (chunk // 128) + g, 1), :]
            allowed = (query_doc == (code & 63)) & ((code >> 6) <= query_at)
            bias_s[:, g * 128 : (g + 1) * 128] = jnp.where(allowed, 0.0, NEGATIVE)
        block = unit_qkv[pl.ds(b * per_chunk, per_chunk), :, nq:].reshape(chunk, 2 * nk)
        fold(block[:, 0:nk], block[:, nk:])
        return 0

    lax.fori_loop(0, units // chunk, unit_block, 0)
    for j in range(heads):
        out[:, j * HD : (j + 1) * HD] = (mix_s[j] / total_s[j]).astype(BF16)


def attention(where, doc, text_q, text_kv, unit_qkv, unit_code, placeholder):
    tokens, nq = text_q.shape
    heads = nq // HD
    whole = pl.BlockSpec(memory_space=VMEM)
    scalars = pl.BlockSpec(memory_space=pltpu.SMEM)
    return pl.pallas_call(
        attention_kernel,
        out_shape=jax.ShapeDtypeStruct((tokens, nq), BF16),
        in_specs=[scalars, scalars] + [whole] * 6,
        out_specs=whole,
        scratch_shapes=[
            VMEM((heads, tokens, HD), BF16),
            VMEM((heads, tokens, 128), F32),
            VMEM((heads, tokens, 128), F32),
            VMEM((heads, tokens, HD), F32),
            VMEM((tokens, tokens), F32),
        ],
        compiler_params=pltpu.CompilerParams(vmem_limit_bytes=40 * 2**20),
        name="attention",
    )(
        where,
        doc,
        text_q,
        text_kv,
        unit_qkv,
        unit_code,
        doc.reshape(-1, tokens // 128, 128),
        placeholder.reshape(-1, tokens // 128, 128),
    )


def body(
    patches,
    patch_image,
    vit_gain,
    vit_qkv,
    vit_proj,
    merge_gain,
    merge_up,
    merge_down,
    text_embed,
    placeholder_unit,
    doc_id,
    dec_gain,
    dec_wq,
    dec_wk,
    dec_wv,
):
    tokens = text_embed.shape[0]
    hidden_all, text_all = vision(
        patches,
        patch_image.reshape(1, -1),
        vit_gain.reshape(1, -1),
        vit_qkv.reshape(vit_qkv.shape[0], -1),
        vit_proj,
        merge_gain.reshape(1, -1),
        merge_up,
        text_embed,
    )
    token_code = jnp.arange(doc_id.shape[0], dtype=jnp.int32) * 64 + doc_id
    text_q, text_kv, unit_qkv, unit_code = merger(
        hidden_all,
        text_all,
        merge_down,
        dec_gain.reshape(8, -1),
        dec_wq,
        dec_wk,
        dec_wv,
        token_code.reshape(-1, 128),
        placeholder_unit.reshape(-1, 128),
    )
    where = lax.axis_index("ctx").astype(jnp.int32).reshape(1)
    return attention(
        where,
        doc_id.reshape(-1, tokens),
        text_q,
        text_kv.reshape(16, tokens, -1),
        unit_qkv.reshape(16, -1, unit_qkv.shape[-1]),
        unit_code,
        placeholder_unit.reshape(-1, tokens),
    )


def solution(mesh):
    placed = (
        P("enc", None),
        P("enc"),
        P(),
        P(None, "ctx", None),
        P("ctx", None),
        P(),
        P(None, "ctx"),
        P("ctx", "enc"),
        P("ctx", "enc"),
        P(),
        P(),
        P(),
        P(None, "enc"),
        P(None, "enc"),
        P(None, "enc"),
    )
    return jax.shard_map(
        body, mesh=mesh, in_specs=placed, out_specs=P("ctx", "enc"), check_vma=False
    )
```

```python
import functools
import math

import jax
import jax.numpy as jnp
from jax import lax
from jax.experimental import pallas as pl
from jax.experimental.pallas import tpu as pltpu
from jax.sharding import PartitionSpec as P

MESH = pl.DeviceIdType.MESH
VMEM = pltpu.VMEM
F32 = jnp.float32
BF16 = jnp.bfloat16

HD = 128
QPK = 4
EPSILON = 1e-06
NEGATIVE = -1e30
SIDE = 4


def places():
    e, c = lax.axis_index("enc"), lax.axis_index("ctx")
    return e // 2, lax.rem(e, 2), c // SIDE, lax.rem(c, SIDE)


def at_device(z, core, y, x):
    return {"enc": z * 2 + core, "ctx": y * SIDE + x}


def ring(position, distance):
    return lax.rem(position + distance, SIDE)


def remote(source, target, send_sem, recv_sem, device):
    return pltpu.make_async_remote_copy(
        src_ref=source,
        dst_ref=target,
        send_sem=send_sem,
        recv_sem=recv_sem,
        device_id=device,
        device_id_type=MESH,
    )


def greet():
    z, core, y, x = places()
    barrier = pltpu.get_barrier_semaphore()
    peers = []
    for d in range(1, SIDE):
        peers.append(at_device(z, core, y, ring(x, d)))
        peers.append(at_device(z, core, ring(y, d), x))
        peers.append(at_device(ring(z, d), core, y, x))
    peers.append(at_device(z, 1 - core, y, x))
    for peer in peers:
        pl.semaphore_signal(barrier, inc=1, device_id=peer, device_id_type=MESH)
    pl.semaphore_wait(barrier, len(peers))


class Gather:
    def __init__(self, buf, own, cut, sems, columns=None, own_sem=None):
        self.buf, self.own, self.own_sem = buf, own, own_sem
        self.send, self.recv = sems
        cols = slice(None) if columns is None else columns
        self.part_a = (slice(0, cut), cols)
        self.part_b = (slice(cut, own.shape[0]), cols)

    def start(self, phase, pairs):
        z, core, y, x = places()
        copies = []
        for d in range(1, SIDE):
            for way, (source, target) in enumerate(pairs):
                along_x = way == phase
                device = (
                    at_device(z, core, y, ring(x, d))
                    if along_x
                    else at_device(z, core, ring(y, d), x)
                )
                sem = (2 * phase + way, d - 1)
                copies.append(
                    remote(source, target, self.send.at[sem], self.recv.at[sem], device)
                )
        for copy in copies:
            copy.start()
        return copies

    def first(self):
        z, core, y, x = places()
        if self.own_sem is not None:
            self.own_copy = pltpu.make_async_copy(self.own, self.buf.at[y, x], self.own_sem)
            self.own_copy.start()
        self.one = self.start(
            0,
            [
                (self.own.at[part], self.buf.at[(y, x) + part])
                for part in (self.part_a, self.part_b)
            ],
        )

    def second(self):
        z, core, y, x = places()
        if self.own_sem is not None:
            self.own_copy.wait()
        for copy in self.one:
            copy.wait_recv()
        rows_a = self.buf.at[(y, slice(None)) + self.part_a]
        rows_b = self.buf.at[(slice(None), x) + self.part_b]
        self.two = self.start(1, [(rows_a, rows_a), (rows_b, rows_b)])

    def finish(self):
        for copy in self.two:
            copy.wait_recv()

    def drain(self):
        for copy in self.one + self.two:
            copy.wait_send()


class EncGather:
    def __init__(self, buf, sems):
        self.buf = buf
        self.send, self.recv = sems

    def first(self, own):
        z, core, y, x = places()
        slot = z * 2 + core
        copies = [
            remote(
                own,
                self.buf.at[slot],
                self.send.at[d - 1],
                self.recv.at[d - 1],
                at_device(ring(z, d), core, y, x),
            )
            for d in range(1, SIDE)
        ]
        copies.append(
            remote(
                own,
                self.buf.at[slot],
                self.send.at[3],
                self.recv.at[3],
                at_device(z, 1 - core, y, x),
            )
        )
        for copy in copies:
            copy.start()
        self.copies = copies

    def second(self):
        z, core, y, x = places()
        self.handed = []
        for d in range(1, SIDE):
            self.copies[d - 1].wait_recv()
            slot = ring(z, SIDE - d) * 2 + core
            copy = remote(
                self.buf.at[slot],
                self.buf.at[slot],
                self.send.at[3 + d],
                self.recv.at[3 + d],
                at_device(z, 1 - core, y, x),
            )
            copy.start()
            self.handed.append(copy)

    def finish(self):
        self.copies[3].wait_recv()
        for copy in self.handed:
            copy.wait_recv()

    def drain(self):
        for copy in self.copies + self.handed:
            copy.wait_send()


def normed(wide, gain):
    center = wide - jnp.mean(wide, axis=1, keepdims=True)
    spread = jnp.mean(center * center, axis=1, keepdims=True)
    return (center * lax.rsqrt(spread + EPSILON) * gain).astype(BF16)


def gelu(x):
    return 0.5 * x * (1.0 + lax.erf(x * math.sqrt(0.5)))


def row_scale(total, count):
    return lax.rsqrt(total / count + EPSILON)


def tower_kernel(
    image_row,
    gain,
    merge_gain,
    dec_gain,
    token_code,
    placeholder,
    patches_hbm,
    qkv_hbm,
    proj_hbm,
    up_hbm,
    text_hbm,
    down_hbm,
    wq_hbm,
    wk_hbm,
    wv_hbm,
    text_q,
    text_kv,
    unit_qkv,
    unit_code,
    patches,
    qkv,
    proj,
    up,
    down,
    w_s,
    q_s,
    k_s,
    v_s,
    o_s,
    lhs_s,
    norm_s,
    heads_all,
    proj_all,
    text_a,
    text_b,
    hidden_all,
    part_a,
    part_b,
    got_a,
    got_b,
    sum_a,
    sum_b,
    got_a2,
    got_b2,
    rows_all,
    acc_s,
    kv_own_a,
    kv_own_b,
    unit_own,
    local_sem,
    proj_s,
    proj_r,
    heads_s,
    heads_r,
    swap_s,
    swap_r,
    text_as,
    text_ar,
    text_bs,
    text_br,
    hid_s,
    hid_r,
    rs_s,
    rs_r,
    row_s,
    row_r,
    kva_s,
    kva_r,
    kvb_s,
    kvb_r,
    uq_s,
    uq_r,
):
    z, core, y, x = places()
    slot = z * 2 + core
    rows, width = patches.shape
    head = proj.shape[0]
    groups = heads_all.shape[3] // head
    group_rows = rows // groups
    side_cols = pl.ds(pl.multiple_of(core * (width // 2), 128), width // 2)
    blocks, tokens, cols = text_a.shape
    model = blocks * cols
    nq, nk = wq_hbm.shape[1], wk_hbm.shape[1]
    wide = nq + 2 * nk
    own_units = unit_own.shape[0]
    half = cols // 2
    chunk = 256

    def load(index, source, target):
        copy = pltpu.make_async_copy(source, target, local_sem.at[index])
        copy.start()
        return copy

    proj_load = load(0, proj_hbm, proj)
    patches_load = load(1, patches_hbm, patches)
    qkv_load = load(2, qkv_hbm, qkv)
    text_loads = [
        load(3, text_hbm.at[0:tokens], text_a.at[slot]),
        load(4, text_hbm.at[tokens:], text_b.at[slot]),
    ]
    up_load = load(5, up_hbm, up)
    down_load = load(6, down_hbm, down)
    w_loads = [
        load(7, wq_hbm, w_s.at[:, 0:nq]),
        load(8, wk_hbm, w_s.at[:, nq : nq + nk]),
        load(9, wv_hbm, w_s.at[:, nq + nk : wide]),
    ]
    proj_load.wait()
    greet()
    proj_gather = Gather(proj_all, proj, 48, (proj_s, proj_r), columns=side_cols)
    proj_gather.first()
    text_gathers = [EncGather(text_a, (text_as, text_ar)), EncGather(text_b, (text_bs, text_br))]
    text_gathers[0].first(text_hbm.at[0:tokens])
    text_gathers[1].first(text_hbm.at[tokens:])
    proj_all[y, x, :, side_cols] = proj[:, side_cols]

    patches_load.wait()
    qkv_load.wait()

    def project(i, _):
        here = pl.ds(pl.multiple_of(i * chunk, chunk), chunk)
        block = normed(patches[here, :].astype(F32), gain[...])
        packed = lax.dot_general(
            block, qkv[...], (((1,), (1,)), ((), ())), preferred_element_type=F32
        )
        q_s[here, :] = packed[:, 0:head].astype(BF16)
        k_s[here, :] = packed[:, head : 2 * head].astype(BF16)
        v_s[here, :] = packed[:, 2 * head : 3 * head].astype(BF16)
        return 0

    lax.fori_loop(0, rows // chunk, project, 0)
    proj_gather.second()

    scaling = head ** (-0.5)

    def attend(i, _):
        here = pl.ds(pl.multiple_of(i * chunk, chunk), chunk)
        ids_col = jnp.broadcast_to(image_row[:, here], (128, chunk)).T[:, 0:1]
        scores = lax.dot_general(
            q_s[here, :], k_s[...], (((1,), (1,)), ((), ())), preferred_element_type=F32
        )
        scores = jnp.where(ids_col == image_row[...], scores * scaling, NEGATIVE)
        highest = jnp.max(scores, axis=1, keepdims=True)
        weights = jnp.exp(scores - highest)
        totals = jnp.sum(weights, axis=1, keepdims=True)
        mixture = jnp.dot(weights.astype(BF16), v_s[...], preferred_element_type=F32)
        o_s[here, :] = mixture / totals
        return 0

    lax.fori_loop(0, rows // chunk, attend, 0)
    heads_all[y, x] = jnp.concatenate(
        [o_s[j * group_rows : (j + 1) * group_rows, :] for j in range(groups)], axis=1
    ).astype(BF16)
    heads_gather = Gather(heads_all, heads_all.at[y, x], group_rows // 2, (heads_s, heads_r))
    heads_gather.first()
    proj_gather.finish()
    swap = remote(
        proj_all.at[:, :, :, side_cols],
        proj_all.at[:, :, :, side_cols],
        swap_s,
        swap_r,
        at_device(z, 1 - core, y, x),
    )
    swap.start()
    heads_gather.second()

    def scale_of(source):
        squares = jnp.zeros((source.shape[1], 128), F32)
        for b in range(blocks):
            for g in range(cols // 128):
                piece = source[b, :, g * 128 : (g + 1) * 128].astype(F32)
                squares = squares + piece * piece
        return row_scale(jnp.sum(squares, axis=1, keepdims=True), model)

    def decode(source):
        count = source.shape[1]
        scale = scale_of(source)
        acc_s[0:count, :] = jnp.zeros((count, wide), F32)

        def one_block(b, _):
            block = source[b].astype(F32) * scale * dec_gain[pl.ds(b, 1), :]
            here = pl.ds(pl.multiple_of(b * cols, cols), cols)
            acc_s[0:count, :] += jnp.dot(
                block.astype(BF16), w_s[here, :], preferred_element_type=F32
            )
            return 0

        lax.fori_loop(0, blocks, one_block, 0)

    def text_part(index, source, kv_own):
        text_loads[index].wait()
        text_gathers[index].second()
        text_gathers[index].finish()
        decode(source)
        text_q[index] = acc_s[:, 0:nq].astype(BF16)
        kv_own[...] = acc_s[:, nq:].astype(BF16)

    for w_load in w_loads:
        w_load.wait()
    text_part(0, text_a, kv_own_a)
    kv_a = Gather(
        text_kv.at[0], kv_own_a, tokens // 2, (kva_s, kva_r), own_sem=local_sem.at[10]
    )
    kv_a.first()
    swap.wait_recv()
    heads_gather.finish()

    for j in range(groups):
        lhs_s[j * group_rows : (j + 1) * group_rows, :] = jnp.concatenate(
            [
                heads_all[a, b, :, j * head : (j + 1) * head].astype(F32)
                for a in range(SIDE)
                for b in range(SIDE)
            ],
            axis=1,
        ).astype(BF16)
    kv_a.second()

    def merge(i, _):
        here = pl.ds(pl.multiple_of(i * chunk, chunk), chunk)
        terms = jnp.dot(
            lhs_s[here, :], proj_all[...].reshape(width, width), preferred_element_type=F32
        )
        out = (patches[here, :].astype(F32) + terms).astype(BF16)
        ready = normed(out.astype(F32), merge_gain[...]).astype(F32)
        for g in range(width // 128):
            norm_s[g, here, :] = ready[:, g * 128 : (g + 1) * 128]
        return 0

    lax.fori_loop(0, rows // chunk, merge, 0)
    units = rows // 4
    up_load.wait()
    total = jnp.zeros((units, up.shape[0]), F32)
    for k in range(4):
        quarter = jnp.concatenate(
            [norm_s[g, pl.ds(k, units, stride=4), :] for g in range(width // 128)], axis=1
        ).astype(BF16)
        total = total + lax.dot_general(
            quarter,
            up[:, k * width : (k + 1) * width],
            (((1,), (1,)), ((), ())),
            preferred_element_type=F32,
        )
    hidden_all[slot] = gelu(total).astype(BF16)
    hidden_gather = EncGather(hidden_all, (hid_s, hid_r))
    hidden_gather.first(hidden_all.at[slot])
    text_part(1, text_b, kv_own_b)
    kv_b = Gather(
        text_kv.at[1], kv_own_b, tokens // 2, (kvb_s, kvb_r), own_sem=local_sem.at[11]
    )
    hidden_gather.second()
    down_load.wait()
    hidden_gather.finish()

    one = []
    for d in (1, 2, 3, 0):
        xp, yp = ring(x, d), ring(y, d)
        lhs_a = jnp.concatenate(
            [
                hidden_all[
                    2 * v + xp // 2,
                    pl.ds(pl.multiple_of(lax.rem(xp, 2) * own_units, own_units), own_units),
                    :,
                ]
                for v in range(SIDE)
            ],
            axis=0,
        )
        part_a[d] = jnp.dot(lhs_a, down[:, 0:half], preferred_element_type=F32).astype(BF16)
        if d:
            copy = remote(
                part_a.at[d],
                got_a.at[d - 1],
                rs_s.at[0, d - 1],
                rs_r.at[0, d - 1],
                at_device(z, core, y, xp),
            )
            copy.start()
            one.append(copy)
        lhs_b = jnp.concatenate([hidden_all[2 * yp], hidden_all[2 * yp + 1]], axis=0)
        part_b[d] = jnp.dot(lhs_b, down[:, half:], preferred_element_type=F32).astype(BF16)
        if d:
            copy = remote(
                part_b.at[d],
                got_b.at[d - 1],
                rs_s.at[1, d - 1],
                rs_r.at[1, d - 1],
                at_device(z, core, yp, x),
            )
            copy.start()
            one.append(copy)
    kv_b.first()

    lane_unit = lax.broadcasted_iota(jnp.int32, (128, 128), 0)

    def units_block(b, _):
        unit = lane_unit + b * 128
        found = jnp.zeros((128, 128), jnp.int32)
        for r in range(placeholder.shape[0]):
            found = found + jnp.where(
                placeholder[r : r + 1, :] == unit, token_code[r : r + 1, :], 0
            )
        unit_code[pl.ds(b, 1), :] = jnp.sum(found.T, axis=0, keepdims=True)
        return 0

    lax.fori_loop(0, unit_code.shape[0], units_block, 0)

    for copy in one:
        copy.wait_recv()

    def summed(own, others):
        return sum((others[d].astype(F32) for d in range(SIDE - 1)), own.astype(F32))

    def own_rows(index):
        return pl.ds(pl.multiple_of(index * own_units, own_units), own_units)

    sum_a[...] = summed(part_a[0], got_a).astype(BF16)
    sum_b[...] = summed(part_b[0], got_b).astype(BF16)
    two = []
    for d in range(1, SIDE):
        xp, yp = ring(x, d), ring(y, d)
        two.append(
            remote(
                sum_a.at[own_rows(yp)],
                got_a2.at[d - 1],
                rs_s.at[2, d - 1],
                rs_r.at[2, d - 1],
                at_device(z, core, yp, x),
            )
        )
        two.append(
            remote(
                sum_b.at[own_rows(xp)],
                got_b2.at[d - 1],
                rs_s.at[3, d - 1],
                rs_r.at[3, d - 1],
                at_device(z, core, y, xp),
            )
        )
    for copy in two:
        copy.start()
    for copy in two:
        copy.wait_recv()
    rows_all[slot] = jnp.concatenate(
        [summed(sum_a[own_rows(y), :], got_a2), summed(sum_b[own_rows(x), :], got_b2)], axis=1
    ).astype(BF16)

    rows_gather = EncGather(rows_all, (row_s, row_r))
    rows_gather.first(rows_all.at[slot])
    kv_b.second()
    rows_gather.second()
    rows_gather.finish()
    decode(rows_all)
    unit_own[...] = acc_s[0:own_units, :].astype(BF16)
    unit_gather = Gather(
        unit_qkv, unit_own, own_units // 2, (uq_s, uq_r), own_sem=local_sem.at[12]
    )
    unit_gather.first()
    unit_gather.second()
    unit_gather.finish()
    kv_a.finish()
    kv_b.finish()
    swap.wait_send()
    for copy in one + two:
        copy.wait_send()
    for gather in [proj_gather, heads_gather, kv_a, kv_b, unit_gather]:
        gather.drain()
    for gather in text_gathers + [hidden_gather, rows_gather]:
        gather.drain()


def tower(
    image_row,
    gain,
    merge_gain,
    dec_gain,
    token_code,
    placeholder,
    patches,
    qkv,
    proj,
    up,
    text,
    down,
    wq,
    wk,
    wv,
):
    rows, width = patches.shape
    head = proj.shape[0]
    groups = 8
    units = rows // 4
    cols = text.shape[1]
    tokens = text.shape[0] // 2
    nq, nk = wq.shape[1], wk.shape[1]
    wide = nq + 2 * nk
    own_units = 8 * units // (SIDE * SIDE)
    side_units = own_units * SIDE
    half = cols // 2
    dma = pltpu.SemaphoreType.DMA
    whole = pl.BlockSpec(memory_space=VMEM)
    anywhere = pl.BlockSpec(memory_space=pl.ANY)

    def both(shape):
        return [dma(shape), dma(shape)]

    return pl.pallas_call(
        tower_kernel,
        out_shape=(
            jax.ShapeDtypeStruct((2, tokens, nq), BF16),
            jax.ShapeDtypeStruct((2, SIDE, SIDE, tokens, 2 * nk), BF16),
            jax.ShapeDtypeStruct((SIDE, SIDE, own_units, wide), BF16),
            jax.ShapeDtypeStruct((own_units * 16 // 128, 128), jnp.int32),
        ),
        in_specs=[whole] * 6 + [anywhere] * 9,
        out_specs=(whole, anywhere, anywhere, whole),
        scratch_shapes=[
            VMEM((rows, width), BF16),
            VMEM(qkv.shape, BF16),
            VMEM((head, width), BF16),
            VMEM(up.shape, BF16),
            VMEM(down.shape, BF16),
            VMEM((8 * cols, wide), BF16),
            VMEM((rows, head), BF16),
            VMEM((rows, head), BF16),
            VMEM((rows, head), BF16),
            VMEM((rows, head), F32),
            VMEM((rows, width), BF16),
            VMEM((width // 128, rows, 128), F32),
            VMEM((SIDE, SIDE, rows // groups, groups * head), BF16),
            VMEM((SIDE, SIDE, head, width), BF16),
            VMEM((8, tokens, cols), BF16),
            VMEM((8, tokens, cols), BF16),
            VMEM((8, units, up.shape[0]), BF16),
            VMEM((SIDE, side_units, half), BF16),
            VMEM((SIDE, side_units, half), BF16),
            VMEM((SIDE - 1, side_units, half), BF16),
            VMEM((SIDE - 1, side_units, half), BF16),
            VMEM((side_units, half), BF16),
            VMEM((side_units, half), BF16),
            VMEM((SIDE - 1, own_units, half), BF16),
            VMEM((SIDE - 1, own_units, half), BF16),
            VMEM((8, own_units, cols), BF16),
            VMEM((tokens, wide), F32),
            VMEM((tokens, 2 * nk), BF16),
            VMEM((tokens, 2 * nk), BF16),
            VMEM((own_units, wide), BF16),
            dma((13,)),
            *both((4, 3)),
            *both((4, 3)),
            *both(()),
            *both((7,)),
            *both((7,)),
            *both((7,)),
            *both((4, 3)),
            *both((7,)),
            *both((4, 3)),
            *both((4, 3)),
            *both((4, 3)),
        ],
        compiler_params=pltpu.CompilerParams(
            collective_id=1, has_side_effects=True, vmem_limit_bytes=60 * 2**20
        ),
        name="tower",
    )(
        image_row,
        gain,
        merge_gain,
        dec_gain,
        token_code,
        placeholder,
        patches,
        qkv,
        proj,
        up,
        text,
        down,
        wq,
        wk,
        wv,
    )


def attention_kernel(
    where_ref,
    doc_smem,
    text_q,
    unit_code,
    doc_rows,
    unit_rows,
    text_kv_hbm,
    unit_qkv_hbm,
    out,
    text_kv,
    unit_qkv,
    load_sem,
    q_s,
    peak_s,
    total_s,
    mix_s,
    bias_s,
):
    tokens, nq = text_q.shape
    nk = text_kv.shape[2] // 2
    unit_load = pltpu.make_async_copy(unit_qkv_hbm, unit_qkv, load_sem.at[0])
    unit_load.start()
    text_loads = []
    for p in range(2):
        here = slice(p * (tokens // 2), (p + 1) * (tokens // 2))
        text_loads.append(
            pltpu.make_async_copy(text_kv_hbm.at[p], text_kv.at[:, here, :], load_sem.at[1 + p])
        )
        text_loads[p].start()
    heads = nq // HD
    units = unit_qkv.shape[0] * unit_qkv.shape[1]
    mine = where_ref[0]
    first_doc = doc_smem[mine, 0]
    scale = HD ** (-0.5) * math.log2(math.e)

    def column(rows):
        return jnp.concatenate(
            [jnp.broadcast_to(rows[g : g + 1, :], (128, 128)).T for g in range(tokens // 128)],
            axis=0,
        )

    query_doc = column(doc_rows[mine])
    query_unit = column(unit_rows[mine])
    query_at = mine * tokens + lax.broadcasted_iota(jnp.int32, (tokens, 128), 0)
    lane = lax.broadcasted_iota(jnp.int32, (tokens, 128), 1)

    picked = jnp.zeros((tokens, nq), F32)
    chunk = 384
    unit_load.wait()
    per_chunk = chunk // unit_qkv.shape[1]
    for b in range(units // chunk):
        chosen = jnp.concatenate(
            [
                (query_unit == lane + (b * chunk + g * 128)).astype(F32)
                for g in range(chunk // 128)
            ],
            axis=1,
        ).astype(BF16)
        source = unit_qkv[b * per_chunk : (b + 1) * per_chunk, :, 0:nq].reshape(chunk, nq)
        picked = picked + jnp.dot(chosen, source, preferred_element_type=F32)
    for j in range(heads):
        part = slice(j * HD, (j + 1) * HD)
        q_s[j] = jnp.where(query_unit >= 0, picked[:, part], text_q[:, part].astype(F32)).astype(
            BF16
        )
    peak_s[...] = jnp.full_like(peak_s, NEGATIVE)
    total_s[...] = jnp.zeros_like(total_s)
    mix_s[...] = jnp.zeros_like(mix_s)

    def fold(keys, values):
        for j in range(heads):
            scores = lax.dot_general(
                q_s[j], keys, (((1,), (1,)), ((), ())), preferred_element_type=F32
            )
            scores = scores + bias_s[...]
            before = peak_s[j]
            peak = jnp.maximum(before, jnp.max(scores, axis=1, keepdims=True))
            factor = jnp.exp2((before - peak) * scale)
            wide_peak = jnp.concatenate([peak] * (scores.shape[1] // 128), axis=1)
            weights = jnp.exp2((scores - wide_peak) * scale)
            peak_s[j] = peak
            total_s[j] = total_s[j] * factor + jnp.sum(weights, axis=1, keepdims=True)
            mix_s[j] = mix_s[j] * factor + jnp.dot(
                weights.astype(BF16), values, preferred_element_type=F32
            )

    def text_block(s, _):
        docs, unit_of = doc_rows[s], unit_rows[s]
        for g in range(tokens // 128):
            part = slice(g * 128, (g + 1) * 128)
            key_at = s * tokens + g * 128 + lane
            same = query_doc == docs[g : g + 1, :]
            text = unit_of[g : g + 1, :] < 0
            allowed = same & (key_at <= query_at) & text
            bias_s[:, part] = jnp.where(allowed, 0.0, NEGATIVE)
        block = text_kv[s]
        fold(block[:, 0:nk], block[:, nk:])
        return 0

    begin = jnp.int32(0)
    for s in range(doc_smem.shape[0]):
        begin = begin + (doc_smem[s, tokens - 1] < first_doc).astype(jnp.int32)
    for text_load in text_loads:
        text_load.wait()
    lax.fori_loop(begin, mine + 1, text_block, 0)

    def unit_block(b, _):
        for g in range(chunk // 128):
            code = unit_code[pl.ds(b * (chunk // 128) + g, 1), :]
            allowed = (query_doc == (code & 63)) & ((code >> 6) <= query_at)
            bias_s[:, g * 128 : (g + 1) * 128] = jnp.where(allowed, 0.0, NEGATIVE)
        block = unit_qkv[pl.ds(b * per_chunk, per_chunk), :, nq:].reshape(chunk, 2 * nk)
        fold(block[:, 0:nk], block[:, nk:])
        return 0

    lax.fori_loop(0, units // chunk, unit_block, 0)
    for j in range(heads):
        out[:, j * HD : (j + 1) * HD] = (mix_s[j] / total_s[j]).astype(BF16)


def attention(where, doc, text_q, text_kv, unit_qkv, unit_code, placeholder):
    tokens, nq = text_q.shape
    heads = nq // HD
    shards = text_kv.shape[1]
    whole = pl.BlockSpec(memory_space=VMEM)
    anywhere = pl.BlockSpec(memory_space=pl.ANY)
    scalars = pl.BlockSpec(memory_space=pltpu.SMEM)
    return pl.pallas_call(
        attention_kernel,
        out_shape=jax.ShapeDtypeStruct((tokens, nq), BF16),
        in_specs=[scalars, scalars] + [whole] * 4 + [anywhere] * 2,
        out_specs=whole,
        scratch_shapes=[
            VMEM((shards, tokens, text_kv.shape[3]), BF16),
            VMEM(unit_qkv.shape, BF16),
            pltpu.SemaphoreType.DMA((3,)),
            VMEM((heads, tokens, HD), BF16),
            VMEM((heads, tokens, 128), F32),
            VMEM((heads, tokens, 128), F32),
            VMEM((heads, tokens, HD), F32),
            VMEM((tokens, tokens), F32),
        ],
        compiler_params=pltpu.CompilerParams(vmem_limit_bytes=60 * 2**20),
        name="attention",
    )(
        where,
        doc,
        text_q,
        unit_code,
        doc.reshape(-1, tokens // 128, 128),
        placeholder.reshape(-1, tokens // 128, 128),
        text_kv,
        unit_qkv,
    )


def body(
    patches,
    patch_image,
    vit_gain,
    vit_qkv,
    vit_proj,
    merge_gain,
    merge_up,
    merge_down,
    text_embed,
    placeholder_unit,
    doc_id,
    dec_gain,
    dec_wq,
    dec_wk,
    dec_wv,
):
    tokens = text_embed.shape[0]
    token_code = jnp.arange(doc_id.shape[0], dtype=jnp.int32) * 64 + doc_id
    text_q, text_kv, unit_qkv, unit_code = tower(
        patch_image.reshape(1, -1),
        vit_gain.reshape(1, -1),
        merge_gain.reshape(1, -1),
        dec_gain.reshape(8, -1),
        token_code.reshape(-1, 128),
        placeholder_unit.reshape(-1, 128),
        patches,
        vit_qkv.transpose(1, 2, 0).reshape(-1, vit_qkv.shape[0]),
        vit_proj,
        merge_up.T,
        text_embed,
        merge_down,
        dec_wq,
        dec_wk,
        dec_wv,
    )
    where = lax.axis_index("ctx").astype(jnp.int32).reshape(1)
    return attention(
        where,
        doc_id.reshape(-1, tokens),
        text_q.reshape(tokens, -1),
        text_kv.reshape(2, 16, tokens // 2, -1),
        unit_qkv.reshape(16, -1, unit_qkv.shape[-1]),
        unit_code,
        placeholder_unit.reshape(-1, tokens),
    )


def solution(mesh):
    placed = (
        P("enc", None),
        P("enc"),
        P(),
        P(None, "ctx", None),
        P("ctx", None),
        P(),
        P(None, "ctx"),
        P("ctx", "enc"),
        P("ctx", "enc"),
        P(),
        P(),
        P(),
        P(None, "enc"),
        P(None, "enc"),
        P(None, "enc"),
    )
    return jax.shard_map(
        body, mesh=mesh, in_specs=placed, out_specs=P("ctx", "enc"), check_vma=False
    )
```

```python
import functools
import math

import jax
import jax.numpy as jnp
from jax import lax
from jax.experimental import pallas as pl
from jax.experimental.pallas import tpu as pltpu
from jax.sharding import PartitionSpec as P

MESH = pl.DeviceIdType.MESH
VMEM = pltpu.VMEM
F32 = jnp.float32
BF16 = jnp.bfloat16

HD = 128
QPK = 4
EPSILON = 1e-06
NEGATIVE = -1e30
SIDE = 4


def places():
    e, c = lax.axis_index("enc"), lax.axis_index("ctx")
    return e // 2, lax.rem(e, 2), c // SIDE, lax.rem(c, SIDE)


def at_device(z, core, y, x):
    return {"enc": z * 2 + core, "ctx": y * SIDE + x}


def ring(position, distance):
    return lax.rem(position + distance, SIDE)


def remote(source, target, send_sem, recv_sem, device):
    return pltpu.make_async_remote_copy(
        src_ref=source,
        dst_ref=target,
        send_sem=send_sem,
        recv_sem=recv_sem,
        device_id=device,
        device_id_type=MESH,
    )


def ring_peers():
    z, core, y, x = places()
    peers = []
    for d in range(1, SIDE):
        peers.append(at_device(z, core, y, ring(x, d)))
        peers.append(at_device(z, core, ring(y, d), x))
        peers.append(at_device(ring(z, d), core, y, x))
    peers.append(at_device(z, 1 - core, y, x))
    return peers


def greet():
    for peer in ring_peers():
        pl.semaphore_signal(
            pltpu.get_barrier_semaphore(), inc=1, device_id=peer, device_id_type=MESH
        )


def meet():
    pl.semaphore_wait(pltpu.get_barrier_semaphore(), len(ring_peers()))


def row_of(ref, first, count):
    return jnp.concatenate([ref[pl.ds(first + g, 1), :] for g in range(count)], axis=1)


def column_of(ref, first, count):
    return jnp.concatenate(
        [jnp.broadcast_to(ref[pl.ds(first + g, 1), :], (128, 128)).T for g in range(count)],
        axis=0,
    )


class Gather:
    def __init__(self, buf, own, parts, sems, own_sem=None):
        self.buf, self.own, self.own_sem = buf, own, own_sem
        self.send, self.recv = sems
        self.part_a, self.part_b = parts

    def start(self, phase, pairs):
        z, core, y, x = places()
        copies = []
        for d in range(1, SIDE):
            for way, (source, target) in enumerate(pairs):
                along_x = way == phase
                device = (
                    at_device(z, core, y, ring(x, d))
                    if along_x
                    else at_device(z, core, ring(y, d), x)
                )
                sem = (2 * phase + way, d - 1)
                copies.append(
                    remote(source, target, self.send.at[sem], self.recv.at[sem], device)
                )
        for copy in copies:
            copy.start()
        return copies

    def first(self):
        z, core, y, x = places()
        if self.own_sem is not None:
            self.own_copy = pltpu.make_async_copy(self.own, self.buf.at[y, x], self.own_sem)
            self.own_copy.start()
        self.one = self.start(
            0,
            [
                (self.own.at[part], self.buf.at[(y, x) + part])
                for part in (self.part_a, self.part_b)
            ],
        )

    def second(self):
        z, core, y, x = places()
        if self.own_sem is not None:
            self.own_copy.wait()
        for copy in self.one:
            copy.wait_recv()
        rows_a = self.buf.at[(y, slice(None)) + self.part_a]
        rows_b = self.buf.at[(slice(None), x) + self.part_b]
        self.two = self.start(1, [(rows_a, rows_a), (rows_b, rows_b)])

    def finish(self):
        for copy in self.two:
            copy.wait_recv()

    def drain(self):
        for copy in self.one + self.two:
            copy.wait_send()


class EncGather:
    def __init__(self, buf, sems):
        self.buf = buf
        self.send, self.recv = sems

    def first(self, own):
        z, core, y, x = places()
        slot = z * 2 + core
        copies = [
            remote(
                own,
                self.buf.at[slot],
                self.send.at[d - 1],
                self.recv.at[d - 1],
                at_device(ring(z, d), core, y, x),
            )
            for d in range(1, SIDE)
        ]
        copies.append(
            remote(
                own,
                self.buf.at[slot],
                self.send.at[3],
                self.recv.at[3],
                at_device(z, 1 - core, y, x),
            )
        )
        for copy in copies:
            copy.start()
        self.copies = copies

    def second(self):
        z, core, y, x = places()
        self.handed = []
        for d in range(1, SIDE):
            self.copies[d - 1].wait_recv()
            slot = ring(z, SIDE - d) * 2 + core
            copy = remote(
                self.buf.at[slot],
                self.buf.at[slot],
                self.send.at[3 + d],
                self.recv.at[3 + d],
                at_device(z, 1 - core, y, x),
            )
            copy.start()
            self.handed.append(copy)

    def finish(self):
        self.copies[3].wait_recv()
        for copy in self.handed:
            copy.wait_recv()

    def drain(self):
        for copy in self.copies + self.handed:
            copy.wait_send()


class RelayGather:
    def __init__(self, buf, sems):
        self.buf = buf
        self.send, self.recv = sems

    def copy(self, index, source, target, device):
        copy = remote(source, target, self.send.at[index], self.recv.at[index], device)
        copy.start()
        self.copies.append(copy)

    def first(self, own):
        z, core, y, x = places()
        self.copies = []
        here = self.buf.at[z * 2 + core]
        self.copy(0, own, here, at_device(ring(z, 1), core, y, x))
        self.copy(1, own, here, at_device(ring(z, 3), core, y, x))
        self.copy(2, own, here, at_device(z, 1 - core, y, x))

    def relay(self):
        z, core, y, x = places()
        middle = self.buf.shape[1] // 2
        left, right = ring(z, 3) * 2 + core, ring(z, 1) * 2 + core
        self.copies[0].wait_recv()
        low = self.buf.at[left, 0:middle]
        self.copy(3, low, low, at_device(ring(z, 1), core, y, x))
        self.copies[1].wait_recv()
        high = self.buf.at[right, middle:]
        self.copy(4, high, high, at_device(ring(z, 3), core, y, x))
        for index, block in ((5, left), (6, right)):
            whole = self.buf.at[block]
            self.copy(index, whole, whole, at_device(z, 1 - core, y, x))

    def second(self):
        z, core, y, x = places()
        self.copies[3].wait_recv()
        self.copies[4].wait_recv()
        far = self.buf.at[ring(z, 2) * 2 + core]
        self.copy(7, far, far, at_device(z, 1 - core, y, x))

    def finish(self):
        for index in (2, 5, 6, 7):
            self.copies[index].wait_recv()

    def drain(self):
        for copy in self.copies:
            copy.wait_send()


def halves(rows):
    return (slice(0, rows // 2), slice(None)), (slice(rows // 2, rows), slice(None))


def normed(wide, gain):
    center = wide - jnp.mean(wide, axis=1, keepdims=True)
    spread = jnp.mean(center * center, axis=1, keepdims=True)
    return (center * lax.rsqrt(spread + EPSILON) * gain).astype(BF16)


def gelu(x):
    return 0.5 * x * (1.0 + lax.erf(x * math.sqrt(0.5)))


def row_scale(total, count):
    return lax.rsqrt(total / count + EPSILON)


def tower_kernel(
    image,
    gain_rows,
    merge_gain_rows,
    dec_gain,
    doc,
    placeholder,
    patches_hbm,
    qkv_hbm,
    proj_hbm,
    up_hbm,
    text_hbm,
    down_hbm,
    wq_hbm,
    wk_hbm,
    wv_hbm,
    text_q,
    text_kv,
    unit_qkv,
    unit_code,
    patches,
    qkv,
    proj,
    up,
    down,
    w_s,
    q_s,
    k_s,
    v_s,
    o_s,
    lhs_s,
    norm_s,
    heads_all,
    proj_all,
    text_a,
    text_b,
    hidden_all,
    part_a,
    part_b,
    got_a,
    got_b,
    sum_a,
    sum_b,
    got_a2,
    got_b2,
    rows_all,
    acc_s,
    kv_own_a,
    kv_own_b,
    unit_own,
    code_s,
    local_sem,
    proj_s,
    proj_r,
    heads_s,
    heads_r,
    swap_s,
    swap_r,
    text_as,
    text_ar,
    text_bs,
    text_br,
    hid_s,
    hid_r,
    rs_s,
    rs_r,
    row_s,
    row_r,
    kva_s,
    kva_r,
    kvb_s,
    kvb_r,
    uq_s,
    uq_r,
):
    z, core, y, x = places()
    slot = z * 2 + core
    rows, width = patches.shape
    head = proj.shape[0]
    groups = heads_all.shape[3] // head
    group_rows = rows // groups
    side_cols = pl.ds(pl.multiple_of(core * (width // 2), 128), width // 2)
    blocks, tokens, cols = text_a.shape
    model = blocks * cols
    nq, nk = wq_hbm.shape[1], wk_hbm.shape[1]
    wide = nq + 2 * nk
    own_units = 2 * unit_own.shape[1]
    half = cols // 2
    chunk = 256

    def load(index, source, target):
        copy = pltpu.make_async_copy(source, target, local_sem.at[index])
        copy.start()
        return copy

    patches_load = load(1, patches_hbm, patches)
    qkv_load = load(2, qkv_hbm, qkv)
    proj_load = load(0, proj_hbm, proj)
    greet()
    text_loads = [
        load(3, text_hbm.at[0:tokens], text_a.at[slot]),
        load(4, text_hbm.at[tokens:], text_b.at[slot]),
    ]
    w_loads = [
        load(7, wq_hbm, w_s.at[:, 0:nq]),
        load(8, wk_hbm, w_s.at[:, nq : nq + nk]),
        load(9, wv_hbm, w_s.at[:, nq + nk : wide]),
    ]
    up_load = load(5, up_hbm, up)
    down_load = load(6, down_hbm, down)

    gain = row_of(gain_rows, 0, width // 128)
    merge_gain = row_of(merge_gain_rows, 0, width // 128)
    image_row = row_of(image, 0, rows // 128)
    patches_load.wait()
    qkv_load.wait()

    def project(i, _):
        here = pl.ds(pl.multiple_of(i * chunk, chunk), chunk)
        block = normed(patches[here, :].astype(F32), gain)
        packed = lax.dot_general(
            block, qkv[...], (((1,), (1,)), ((), ())), preferred_element_type=F32
        )
        q_s[here, :] = packed[:, 0:head].astype(BF16)
        k_s[here, :] = packed[:, head : 2 * head].astype(BF16)
        v_s[here, :] = packed[:, 2 * head : 3 * head].astype(BF16)
        return 0

    lax.fori_loop(0, rows // chunk, project, 0)

    scaling = head ** (-0.5)

    def attend(i, _):
        here = pl.ds(pl.multiple_of(i * chunk, chunk), chunk)
        ids_col = column_of(image, i * (chunk // 128), chunk // 128)[:, 0:1]
        scores = lax.dot_general(
            q_s[here, :], k_s[...], (((1,), (1,)), ((), ())), preferred_element_type=F32
        )
        scores = jnp.where(ids_col == image_row, scores * scaling, NEGATIVE)
        highest = jnp.max(scores, axis=1, keepdims=True)
        weights = jnp.exp(scores - highest)
        totals = jnp.sum(weights, axis=1, keepdims=True)
        mixture = jnp.dot(weights.astype(BF16), v_s[...], preferred_element_type=F32)
        o_s[here, :] = mixture / totals
        return 0

    lax.fori_loop(0, rows // chunk, attend, 0)
    heads_all[y, x] = jnp.concatenate(
        [o_s[j * group_rows : (j + 1) * group_rows, :] for j in range(groups)], axis=1
    ).astype(BF16)
    proj_load.wait()
    proj_all[y, x, :, side_cols] = proj[:, side_cols]
    meet()
    proj_gather = Gather(
        proj_all,
        proj,
        ((slice(0, 48), side_cols), (slice(48, head), side_cols)),
        (proj_s, proj_r),
    )
    proj_gather.first()
    heads_gather = Gather(
        heads_all, heads_all.at[y, x], halves(group_rows), (heads_s, heads_r)
    )
    heads_gather.first()
    text_gathers = [
        RelayGather(text_a, (text_as, text_ar)),
        RelayGather(text_b, (text_bs, text_br)),
    ]
    text_gathers[0].first(text_hbm.at[0:tokens])

    def scale_of(source):
        squares = jnp.zeros((source.shape[1], 128), F32)
        for b in range(blocks):
            for g in range(cols // 128):
                piece = source[b, :, g * 128 : (g + 1) * 128].astype(F32)
                squares = squares + piece * piece
        return row_scale(jnp.sum(squares, axis=1, keepdims=True), model)

    def decode(source):
        count = source.shape[1]
        scale = scale_of(source)
        acc_s[0:count, :] = jnp.zeros((count, wide), F32)

        def one_block(b, _):
            block = source[b].astype(F32) * scale * row_of(dec_gain, b * (cols // 128), cols // 128)
            here = pl.ds(pl.multiple_of(b * cols, cols), cols)
            acc_s[0:count, :] += jnp.dot(
                block.astype(BF16), w_s[here, :], preferred_element_type=F32
            )
            return 0

        lax.fori_loop(0, blocks, one_block, 0)

    def text_part(index, source, kv_own):
        text_loads[index].wait()
        text_gathers[index].finish()
        decode(source)
        text_q[index] = acc_s[:, 0:nq].astype(BF16)
        kv_own[...] = acc_s[:, nq:].astype(BF16)

    proj_gather.second()
    heads_gather.second()
    text_gathers[0].relay()
    text_gathers[1].first(text_hbm.at[tokens:])
    proj_gather.finish()
    swap = remote(
        proj_all.at[:, :, :, side_cols],
        proj_all.at[:, :, :, side_cols],
        swap_s,
        swap_r,
        at_device(z, 1 - core, y, x),
    )
    swap.start()
    for w_load in w_loads:
        w_load.wait()
    text_gathers[0].second()
    text_part(0, text_a, kv_own_a)
    kv_a = Gather(
        text_kv.at[0], kv_own_a, halves(tokens), (kva_s, kva_r), own_sem=local_sem.at[10]
    )
    kv_a.first()
    text_gathers[1].relay()
    swap.wait_recv()
    heads_gather.finish()

    for j in range(groups):
        lhs_s[j * group_rows : (j + 1) * group_rows, :] = jnp.concatenate(
            [
                heads_all[a, b, :, j * head : (j + 1) * head].astype(F32)
                for a in range(SIDE)
                for b in range(SIDE)
            ],
            axis=1,
        ).astype(BF16)

    def merge(i, _):
        here = pl.ds(pl.multiple_of(i * chunk, chunk), chunk)
        terms = jnp.dot(
            lhs_s[here, :], proj_all[...].reshape(width, width), preferred_element_type=F32
        )
        out = (patches[here, :].astype(F32) + terms).astype(BF16)
        ready = normed(out.astype(F32), merge_gain).astype(F32)
        for g in range(width // 128):
            norm_s[g, here, :] = ready[:, g * 128 : (g + 1) * 128]
        return 0

    lax.fori_loop(0, rows // chunk, merge, 0)
    kv_a.second()
    text_gathers[1].second()
    units = rows // 4
    up_load.wait()
    total = jnp.zeros((units, up.shape[0]), F32)
    for k in range(4):
        quarter = jnp.concatenate(
            [norm_s[g, pl.ds(k, units, stride=4), :] for g in range(width // 128)], axis=1
        ).astype(BF16)
        total = total + lax.dot_general(
            quarter,
            up[:, k * width : (k + 1) * width],
            (((1,), (1,)), ((), ())),
            preferred_element_type=F32,
        )
    hidden = gelu(total).astype(BF16)
    share = own_units // 2
    hidden_gathers = []
    for h in range(2):
        hidden_all[h, slot] = jnp.concatenate(
            [
                hidden[(2 * v + h) * share : (2 * v + h + 1) * share, :]
                for v in range(units // own_units)
            ],
            axis=0,
        )
        hidden_gathers.append(EncGather(hidden_all.at[h], (hid_s.at[h], hid_r.at[h])))
        hidden_gathers[h].first(hidden_all.at[h, slot])
    text_part(1, text_b, kv_own_b)
    kv_b = Gather(
        text_kv.at[1], kv_own_b, halves(tokens), (kvb_s, kvb_r), own_sem=local_sem.at[11]
    )
    kv_b.first()
    down_load.wait()

    lane_unit = lax.broadcasted_iota(jnp.int32, (128, 128), 0)
    position = lax.broadcasted_iota(jnp.int32, doc.shape, 0) * 128 + lax.broadcasted_iota(
        jnp.int32, doc.shape, 1
    )
    code_s[...] = position * 64 + doc[...]

    def units_block(b, _):
        unit = lane_unit + b * 128
        found = jnp.zeros((128, 128), jnp.int32)
        for r in range(placeholder.shape[0]):
            found = found + jnp.where(
                placeholder[r : r + 1, :] == unit, code_s[r : r + 1, :], 0
            )
        unit_code[pl.ds(b, 1), :] = jnp.sum(found.T, axis=0, keepdims=True)
        return 0

    one, two = [[], []], [[], []]

    def share_rows(index):
        return pl.ds(pl.multiple_of(index * share, share), share)

    def summed(own, others):
        return sum((others[d].astype(F32) for d in range(SIDE - 1)), own.astype(F32))

    def terms(h, distances):
        for d in distances:
            xp, yp = ring(x, d), ring(y, d)
            lhs_a = jnp.concatenate(
                [
                    hidden_all[h, 2 * v + xp // 2, share_rows(lax.rem(xp, 2)), :]
                    for v in range(SIDE)
                ],
                axis=0,
            )
            lhs_b = jnp.concatenate(
                [
                    hidden_all[h, 2 * yp + v // 2, share_rows(v % 2), :]
                    for v in range(SIDE)
                ],
                axis=0,
            )
            for way, (lhs, columns, part, got, device) in enumerate(
                (
                    (lhs_a, slice(0, half), part_a, got_a, at_device(z, core, y, xp)),
                    (lhs_b, slice(half, cols), part_b, got_b, at_device(z, core, yp, x)),
                )
            ):
                part[h, d] = jnp.dot(
                    lhs, down[:, columns], preferred_element_type=F32
                ).astype(BF16)
                if d:
                    copy = remote(
                        part.at[h, d],
                        got.at[h, d - 1],
                        rs_s.at[h, way, d - 1],
                        rs_r.at[h, way, d - 1],
                        device,
                    )
                    copy.start()
                    one[h].append(copy)

    def ring_sums(h):
        for copy in one[h]:
            copy.wait_recv()
        sum_a[h] = summed(part_a[h, 0], got_a.at[h]).astype(BF16)
        sum_b[h] = summed(part_b[h, 0], got_b.at[h]).astype(BF16)
        for d in range(1, SIDE):
            xp, yp = ring(x, d), ring(y, d)
            for way, (total_s, place, got, device) in enumerate(
                (
                    (sum_a, yp, got_a2, at_device(z, core, yp, x)),
                    (sum_b, xp, got_b2, at_device(z, core, y, xp)),
                )
            ):
                copy = remote(
                    total_s.at[h, share_rows(place)],
                    got.at[h, d - 1],
                    rs_s.at[h, 2 + way, d - 1],
                    rs_r.at[h, 2 + way, d - 1],
                    device,
                )
                copy.start()
                two[h].append(copy)

    rows_gathers = [
        EncGather(rows_all.at[h], (row_s.at[h], row_r.at[h])) for h in range(2)
    ]

    def full_sums(h):
        for copy in two[h]:
            copy.wait_recv()
        rows_all[h, slot] = jnp.concatenate(
            [
                summed(sum_a[h, share_rows(y), :], got_a2.at[h]),
                summed(sum_b[h, share_rows(x), :], got_b2.at[h]),
            ],
            axis=1,
        ).astype(BF16)
        rows_gathers[h].first(rows_all.at[h, slot])

    unit_parts = (
        (slice(0, share), slice(0, wide // 2)),
        (slice(0, share), slice(wide // 2, wide)),
    )
    unit_gathers = [
        Gather(
            unit_qkv.at[h],
            unit_own.at[h],
            unit_parts,
            (uq_s.at[h], uq_r.at[h]),
            own_sem=local_sem.at[12 + h],
        )
        for h in range(2)
    ]

    def decode_units(h):
        decode(rows_all.at[h])
        unit_own[h] = acc_s[0:share, :].astype(BF16)
        unit_gathers[h].first()

    hidden_gathers[0].second()
    hidden_gathers[0].finish()
    terms(0, (2, 1, 3, 0))
    hidden_gathers[1].second()
    hidden_gathers[1].finish()
    terms(1, (2,))
    lax.fori_loop(0, unit_code.shape[0], units_block, 0)
    ring_sums(0)
    terms(1, (1, 3, 0))
    full_sums(0)
    ring_sums(1)
    kv_b.second()
    rows_gathers[0].second()
    full_sums(1)
    rows_gathers[0].finish()
    decode_units(0)
    rows_gathers[1].second()
    unit_gathers[0].second()
    rows_gathers[1].finish()
    decode_units(1)
    unit_gathers[1].second()
    for gather in unit_gathers + [kv_a, kv_b]:
        gather.finish()
    swap.wait_send()
    for copy in one[0] + one[1] + two[0] + two[1]:
        copy.wait_send()
    for gather in [proj_gather, heads_gather, kv_a, kv_b] + unit_gathers:
        gather.drain()
    for gather in text_gathers + hidden_gathers + rows_gathers:
        gather.drain()


def tower(
    image,
    gain,
    merge_gain,
    dec_gain,
    doc,
    placeholder,
    patches,
    qkv,
    proj,
    up,
    text,
    down,
    wq,
    wk,
    wv,
):
    rows, width = patches.shape
    head = proj.shape[0]
    groups = 8
    units = rows // 4
    cols = text.shape[1]
    tokens = text.shape[0] // 2
    nq, nk = wq.shape[1], wk.shape[1]
    wide = nq + 2 * nk
    own_units = 8 * units // (SIDE * SIDE)
    share = own_units // 2
    half = cols // 2
    dma = pltpu.SemaphoreType.DMA
    whole = pl.BlockSpec(memory_space=VMEM)
    anywhere = pl.BlockSpec(memory_space=pl.ANY)

    def both(shape):
        return [dma(shape), dma(shape)]

    return pl.pallas_call(
        tower_kernel,
        out_shape=(
            jax.ShapeDtypeStruct((2, tokens, nq), BF16),
            jax.ShapeDtypeStruct((2, SIDE, SIDE, tokens, 2 * nk), BF16),
            jax.ShapeDtypeStruct((2, SIDE, SIDE, share, wide), BF16),
            jax.ShapeDtypeStruct((own_units * 16 // 128, 128), jnp.int32),
        ),
        in_specs=[whole] * 6 + [anywhere] * 9,
        out_specs=(whole, anywhere, anywhere, whole),
        scratch_shapes=[
            VMEM((rows, width), BF16),
            VMEM(qkv.shape, BF16),
            VMEM((head, width), BF16),
            VMEM(up.shape, BF16),
            VMEM(down.shape, BF16),
            VMEM((8 * cols, wide), BF16),
            VMEM((rows, head), BF16),
            VMEM((rows, head), BF16),
            VMEM((rows, head), BF16),
            VMEM((rows, head), F32),
            VMEM((rows, width), BF16),
            VMEM((width // 128, rows, 128), F32),
            VMEM((SIDE, SIDE, rows // groups, groups * head), BF16),
            VMEM((SIDE, SIDE, head, width), BF16),
            VMEM((8, tokens, cols), BF16),
            VMEM((8, tokens, cols), BF16),
            VMEM((2, 8, units // 2, up.shape[0]), BF16),
            VMEM((2, SIDE, SIDE * share, half), BF16),
            VMEM((2, SIDE, SIDE * share, half), BF16),
            VMEM((2, SIDE - 1, SIDE * share, half), BF16),
            VMEM((2, SIDE - 1, SIDE * share, half), BF16),
            VMEM((2, SIDE * share, half), BF16),
            VMEM((2, SIDE * share, half), BF16),
            VMEM((2, SIDE - 1, share, half), BF16),
            VMEM((2, SIDE - 1, share, half), BF16),
            VMEM((2, 8, share, cols), BF16),
            VMEM((tokens, wide), F32),
            VMEM((tokens, 2 * nk), BF16),
            VMEM((tokens, 2 * nk), BF16),
            VMEM((2, share, wide), BF16),
            VMEM(doc.shape, jnp.int32),
            dma((14,)),
            *both((4, 3)),
            *both((4, 3)),
            *both(()),
            *both((8,)),
            *both((8,)),
            *both((2, 7)),
            *both((2, 4, 3)),
            *both((2, 7)),
            *both((4, 3)),
            *both((4, 3)),
            *both((2, 4, 3)),
        ],
        compiler_params=pltpu.CompilerParams(
            collective_id=1, has_side_effects=True, vmem_limit_bytes=60 * 2**20
        ),
        name="tower",
    )(
        image,
        gain,
        merge_gain,
        dec_gain,
        doc,
        placeholder,
        patches,
        qkv,
        proj,
        up,
        text,
        down,
        wq,
        wk,
        wv,
    )


def attention_kernel(
    where_ref,
    doc_smem,
    text_q,
    unit_code,
    doc_rows,
    unit_rows,
    text_kv_hbm,
    unit_qkv_hbm,
    out,
    text_kv,
    unit_qkv,
    load_sem,
    q_s,
    peak_s,
    mix_s,
    bias_s,
):
    tokens, nq = text_q.shape
    nk = text_kv.shape[2] // 2
    unit_loads = []
    for p in range(2):
        share = unit_qkv.shape[1] // 2
        here = slice(p * share, (p + 1) * share)
        unit_loads.append(
            pltpu.make_async_copy(
                unit_qkv_hbm.at[p], unit_qkv.at[:, here, :], load_sem.at[2 + p]
            )
        )
        unit_loads[p].start()
    text_loads = []
    for p in range(2):
        here = slice(p * (tokens // 2), (p + 1) * (tokens // 2))
        text_loads.append(
            pltpu.make_async_copy(text_kv_hbm.at[p], text_kv.at[:, here, :], load_sem.at[p])
        )
        text_loads[p].start()
    heads = nq // HD
    units = unit_qkv.shape[0] * unit_qkv.shape[1]
    mine = where_ref[0]
    first_doc = doc_smem[mine * tokens]
    scale = HD ** (-0.5) * math.log2(math.e)

    lines = tokens // 128
    query_doc = column_of(doc_rows, mine * lines, lines)
    query_unit = column_of(unit_rows, mine * lines, lines)
    query_at = mine * tokens + lax.broadcasted_iota(jnp.int32, (tokens, 128), 0)
    lane = lax.broadcasted_iota(jnp.int32, (tokens, 128), 1)

    picked = jnp.zeros((tokens, nq), F32)
    chunk = 384
    for unit_load in unit_loads:
        unit_load.wait()
    per_chunk = chunk // unit_qkv.shape[1]
    for b in range(units // chunk):
        chosen = jnp.concatenate(
            [
                (query_unit == lane + (b * chunk + g * 128)).astype(F32)
                for g in range(chunk // 128)
            ],
            axis=1,
        ).astype(BF16)
        source = unit_qkv[b * per_chunk : (b + 1) * per_chunk, :, 0:nq].reshape(chunk, nq)
        picked = picked + jnp.dot(chosen, source, preferred_element_type=F32)
    for j in range(heads):
        part = slice(j * HD, (j + 1) * HD)
        q_s[j] = jnp.where(query_unit >= 0, picked[:, part], text_q[:, part].astype(F32)).astype(
            BF16
        )
    peak_s[...] = jnp.full_like(peak_s, NEGATIVE)
    mix_s[...] = jnp.zeros_like(mix_s)
    row_chunk = 128

    def fold(keys, values):
        values = jnp.concatenate([values, jnp.ones_like(values)], axis=1)
        for r in range(0, tokens, row_chunk):
            here = slice(r, r + row_chunk)
            for j in range(heads):
                scores = lax.dot_general(
                    q_s[j, here, :], keys, (((1,), (1,)), ((), ())), preferred_element_type=F32
                )
                scores = scores + bias_s[here, :]
                before = peak_s[j, here, :]
                peak = jnp.maximum(before, jnp.max(scores, axis=1, keepdims=True))
                factor = jnp.exp2((before - peak) * scale)
                wide_peak = jnp.concatenate([peak] * (scores.shape[1] // 128), axis=1)
                weights = jnp.exp2((scores - wide_peak) * scale).astype(BF16)
                peak_s[j, here, :] = peak
                mix_s[j, here, :] = mix_s[j, here, :] * jnp.concatenate(
                    [factor] * 2, axis=1
                ) + jnp.dot(weights, values, preferred_element_type=F32)

    def text_block(i, _):
        blocks = []
        for t in range(2):
            s = begin + 2 * i + t
            held = jnp.minimum(s, text_kv.shape[0] - 1)
            for g in range(lines):
                key_at = s * tokens + g * 128 + lane
                same = query_doc == doc_rows[pl.ds(held * lines + g, 1), :]
                text = unit_rows[pl.ds(held * lines + g, 1), :] < 0
                allowed = same & (key_at <= query_at) & text
                bias_s[:, t * tokens + g * 128 : t * tokens + (g + 1) * 128] = jnp.where(
                    allowed, 0.0, NEGATIVE
                )
            blocks.append(text_kv[held])
        both = jnp.concatenate(blocks, axis=0)
        fold(both[:, 0:nk], both[:, nk:])
        return 0

    begin = jnp.int32(0)
    for s in range(text_kv.shape[0]):
        begin = begin + (doc_smem[(s + 1) * tokens - 1] < first_doc).astype(jnp.int32)
    for text_load in text_loads:
        text_load.wait()
    lax.fori_loop(0, (mine + 2 - begin) // 2, text_block, 0)

    pair = 2 * chunk

    def unit_block(b, _):
        for g in range(pair // 128):
            code = unit_code[pl.ds(b * (pair // 128) + g, 1), :]
            allowed = (query_doc == (code & 63)) & ((code >> 6) <= query_at)
            bias_s[:, g * 128 : (g + 1) * 128] = jnp.where(allowed, 0.0, NEGATIVE)
        block = unit_qkv[pl.ds(b * 2 * per_chunk, 2 * per_chunk), :, nq:].reshape(pair, 2 * nk)
        fold(block[:, 0:nk], block[:, nk:])
        return 0

    lax.fori_loop(0, units // pair, unit_block, 0)
    for j in range(heads):
        out[:, j * HD : (j + 1) * HD] = (mix_s[j, :, 0:HD] / mix_s[j, :, HD:]).astype(BF16)


def attention(where, doc, text_q, text_kv, unit_qkv, unit_code, placeholder):
    tokens, nq = text_q.shape
    heads = nq // HD
    shards = text_kv.shape[1]
    whole = pl.BlockSpec(memory_space=VMEM)
    anywhere = pl.BlockSpec(memory_space=pl.ANY)
    scalars = pl.BlockSpec(memory_space=pltpu.SMEM)
    return pl.pallas_call(
        attention_kernel,
        out_shape=jax.ShapeDtypeStruct((tokens, nq), BF16),
        in_specs=[scalars, scalars] + [whole] * 4 + [anywhere] * 2,
        out_specs=whole,
        scratch_shapes=[
            VMEM((shards, tokens, text_kv.shape[3]), BF16),
            VMEM((shards, 2 * unit_qkv.shape[2], unit_qkv.shape[3]), BF16),
            pltpu.SemaphoreType.DMA((4,)),
            VMEM((heads, tokens, HD), BF16),
            VMEM((heads, tokens, 128), F32),
            VMEM((heads, tokens, 2 * HD), F32),
            VMEM((tokens, 2 * tokens), F32),
        ],
        compiler_params=pltpu.CompilerParams(vmem_limit_bytes=60 * 2**20),
        name="attention",
    )(
        where,
        doc,
        text_q,
        unit_code,
        doc.reshape(-1, 128),
        placeholder.reshape(-1, 128),
        text_kv,
        unit_qkv,
    )


def body(
    patches,
    patch_image,
    vit_gain,
    vit_qkv,
    vit_proj,
    merge_gain,
    merge_up,
    merge_down,
    text_embed,
    placeholder_unit,
    doc_id,
    dec_gain,
    dec_wq,
    dec_wk,
    dec_wv,
):
    tokens = text_embed.shape[0]
    text_q, text_kv, unit_qkv, unit_code = tower(
        patch_image.reshape(-1, 128),
        vit_gain.reshape(-1, 128),
        merge_gain.reshape(-1, 128),
        dec_gain.reshape(-1, 128),
        doc_id.reshape(-1, 128),
        placeholder_unit.reshape(-1, 128),
        patches,
        vit_qkv.transpose(1, 2, 0).reshape(-1, vit_qkv.shape[0]),
        vit_proj,
        merge_up.T,
        text_embed,
        merge_down,
        dec_wq,
        dec_wk,
        dec_wv,
    )
    where = lax.axis_index("ctx").astype(jnp.int32).reshape(1)
    return attention(
        where,
        doc_id,
        text_q.reshape(tokens, -1),
        text_kv.reshape(2, 16, tokens // 2, -1),
        unit_qkv.reshape(2, 16, -1, unit_qkv.shape[-1]),
        unit_code,
        placeholder_unit,
    )


def solution(mesh):
    placed = (
        P("enc", None),
        P("enc"),
        P(),
        P(None, "ctx", None),
        P("ctx", None),
        P(),
        P(None, "ctx"),
        P("ctx", "enc"),
        P("ctx", "enc"),
        P(),
        P(),
        P(),
        P(None, "enc"),
        P(None, "enc"),
        P(None, "enc"),
    )
    return jax.shard_map(
        body, mesh=mesh, in_specs=placed, out_specs=P("ctx", "enc"), check_vma=False
    )
```

```python
import functools
import math

import jax
import jax.numpy as jnp
from jax import lax
from jax.experimental import pallas as pl
from jax.experimental.pallas import tpu as pltpu
from jax.sharding import PartitionSpec as P

MESH = pl.DeviceIdType.MESH
VMEM = pltpu.VMEM
F32 = jnp.float32
BF16 = jnp.bfloat16

HD = 128
QPK = 4
EPSILON = 1e-06
NEGATIVE = -1e30
SIDE = 4


def places():
    e, c = lax.axis_index("enc"), lax.axis_index("ctx")
    return e // 2, lax.rem(e, 2), c // SIDE, lax.rem(c, SIDE)


def at_device(z, core, y, x):
    return {"enc": z * 2 + core, "ctx": y * SIDE + x}


def ring(position, distance):
    return lax.rem(position + distance, SIDE)


def remote(source, target, send_sem, recv_sem, device):
    return pltpu.make_async_remote_copy(
        src_ref=source,
        dst_ref=target,
        send_sem=send_sem,
        recv_sem=recv_sem,
        device_id=device,
        device_id_type=MESH,
    )


def ring_peers():
    z, core, y, x = places()
    peers = []
    for d in range(1, SIDE):
        peers.append(at_device(z, core, y, ring(x, d)))
        peers.append(at_device(z, core, ring(y, d), x))
        peers.append(at_device(ring(z, d), core, y, x))
    peers.append(at_device(z, 1 - core, y, x))
    return peers


def greet():
    for peer in ring_peers():
        pl.semaphore_signal(
            pltpu.get_barrier_semaphore(), inc=1, device_id=peer, device_id_type=MESH
        )


def meet():
    pl.semaphore_wait(pltpu.get_barrier_semaphore(), len(ring_peers()))


def row_of(ref, first, count):
    return jnp.concatenate([ref[pl.ds(first + g, 1), :] for g in range(count)], axis=1)


def column_of(ref, first, count):
    return jnp.concatenate(
        [jnp.broadcast_to(ref[pl.ds(first + g, 1), :], (128, 128)).T for g in range(count)],
        axis=0,
    )


class Gather:
    def __init__(self, buf, own, parts, sems, own_sem=None):
        self.buf, self.own, self.own_sem = buf, own, own_sem
        self.send, self.recv = sems
        self.part_a, self.part_b = parts

    def start(self, phase, pairs, distances):
        z, core, y, x = places()
        copies = {}
        for d in distances:
            for way, (source, target) in enumerate(pairs):
                along_x = way == phase
                device = (
                    at_device(z, core, y, ring(x, d))
                    if along_x
                    else at_device(z, core, ring(y, d), x)
                )
                sem = (2 * phase + way, d - 1)
                copies[way, d] = remote(
                    source, target, self.send.at[sem], self.recv.at[sem], device
                )
        for copy in copies.values():
            copy.start()
        return copies

    def first(self):
        z, core, y, x = places()
        if self.own_sem is not None:
            self.own_copy = pltpu.make_async_copy(self.own, self.buf.at[y, x], self.own_sem)
            self.own_copy.start()
        self.one = self.start(
            0,
            [
                (self.own.at[part], self.buf.at[(y, x) + part])
                for part in (self.part_a, self.part_b)
            ],
            (1, 2, 3),
        )

    def lines(self, row, column, some=slice(None)):
        return (
            self.buf.at[(row, some) + self.part_a],
            self.buf.at[(some, column) + self.part_b],
        )

    def second(self, relayed=False):
        z, core, y, x = places()
        if self.own_sem is not None:
            self.own_copy.wait()
        for copy in self.one.values():
            copy.wait_recv()
        self.relayed = relayed
        self.two = self.start(
            1, [(line, line) for line in self.lines(y, x)], (1, 3) if relayed else (1, 2, 3)
        )
        self.handed = {}

    def relay(self):
        z, core, y, x = places()
        for index, (d, some) in enumerate(((1, slice(0, 2)), (3, slice(2, 4)))):
            for way in range(2):
                self.two[way, d].wait_recv()
                line = self.lines(ring(y, SIDE - d), ring(x, SIDE - d), some)[way]
                device = (
                    at_device(z, core, ring(y, d), x)
                    if way == 0
                    else at_device(z, core, y, ring(x, d))
                )
                sem = (2 + way, 1 + 2 * index)
                self.handed[way, d] = remote(
                    line, line, self.send.at[sem], self.recv.at[sem], device
                )
                self.handed[way, d].start()

    def finish(self):
        for copy in (self.handed if self.relayed else self.two).values():
            copy.wait_recv()

    def drain(self):
        for copies in (self.one, self.two, self.handed):
            for copy in copies.values():
                copy.wait_send()


class EncGather:
    def __init__(self, buf, sems):
        self.buf = buf
        self.send, self.recv = sems

    def first(self, own):
        z, core, y, x = places()
        slot = z * 2 + core
        copies = [
            remote(
                own,
                self.buf.at[slot],
                self.send.at[d - 1],
                self.recv.at[d - 1],
                at_device(ring(z, d), core, y, x),
            )
            for d in range(1, SIDE)
        ]
        copies.append(
            remote(
                own,
                self.buf.at[slot],
                self.send.at[3],
                self.recv.at[3],
                at_device(z, 1 - core, y, x),
            )
        )
        for copy in copies:
            copy.start()
        self.copies = copies

    def second(self):
        z, core, y, x = places()
        self.handed = []
        for d in range(1, SIDE):
            self.copies[d - 1].wait_recv()
            slot = ring(z, SIDE - d) * 2 + core
            copy = remote(
                self.buf.at[slot],
                self.buf.at[slot],
                self.send.at[3 + d],
                self.recv.at[3 + d],
                at_device(z, 1 - core, y, x),
            )
            copy.start()
            self.handed.append(copy)

    def finish(self):
        self.copies[3].wait_recv()
        for copy in self.handed:
            copy.wait_recv()

    def drain(self):
        for copy in self.copies + self.handed:
            copy.wait_send()


class RelayGather:
    def __init__(self, buf, sems):
        self.buf = buf
        self.send, self.recv = sems
        self.copies = {}

    def copy(self, index, source, target, device):
        copy = remote(source, target, self.send.at[index], self.recv.at[index], device)
        copy.start()
        self.copies[index] = copy

    def first(self, own, high):
        z, core, y, x = places()
        middle, rows = self.buf.shape[1] // 2, self.buf.shape[1]
        slot = z * 2 + core
        part = slice(middle, rows) if high else slice(0, middle)
        for index, d in ((8, 1), (9, 3)) if high else ((0, 1), (1, 3)):
            self.copy(
                index,
                own.at[part],
                self.buf.at[slot, part],
                at_device(ring(z, d), core, y, x),
            )
        if not high:
            self.copy(2, own, self.buf.at[slot], at_device(z, 1 - core, y, x))

    def relay(self):
        z, core, y, x = places()
        middle = self.buf.shape[1] // 2
        left, right = ring(z, 3) * 2 + core, ring(z, 1) * 2 + core
        self.copies[0].wait_recv()
        low = self.buf.at[left, 0:middle]
        self.copy(3, low, low, at_device(ring(z, 1), core, y, x))
        self.copies[9].wait_recv()
        high = self.buf.at[right, middle:]
        self.copy(4, high, high, at_device(ring(z, 3), core, y, x))
        self.copies[1].wait_recv()
        self.copies[8].wait_recv()
        for index, block in ((5, left), (6, right)):
            whole = self.buf.at[block]
            self.copy(index, whole, whole, at_device(z, 1 - core, y, x))

    def second(self):
        z, core, y, x = places()
        self.copies[3].wait_recv()
        self.copies[4].wait_recv()
        far = self.buf.at[ring(z, 2) * 2 + core]
        self.copy(7, far, far, at_device(z, 1 - core, y, x))

    def finish(self):
        for index in (2, 5, 6, 7):
            self.copies[index].wait_recv()

    def drain(self):
        for copy in self.copies.values():
            copy.wait_send()


def halves(rows):
    return (slice(0, rows // 2), slice(None)), (slice(rows // 2, rows), slice(None))


def normed(wide, gain):
    center = wide - jnp.mean(wide, axis=1, keepdims=True)
    spread = jnp.mean(center * center, axis=1, keepdims=True)
    return (center * lax.rsqrt(spread + EPSILON) * gain).astype(BF16)


def gelu(x):
    return 0.5 * x * (1.0 + lax.erf(x * math.sqrt(0.5)))


def row_scale(total, count):
    return lax.rsqrt(total / count + EPSILON)


def tower_kernel(
    image,
    gain_rows,
    merge_gain_rows,
    dec_gain,
    doc,
    placeholder,
    patches_hbm,
    qkv_hbm,
    proj_hbm,
    up_hbm,
    text_hbm,
    down_hbm,
    wq_hbm,
    wk_hbm,
    wv_hbm,
    text_q,
    text_kv,
    unit_qkv,
    unit_code,
    patches,
    qkv,
    proj,
    up,
    down,
    w_s,
    q_s,
    k_s,
    v_s,
    o_s,
    lhs_s,
    norm_s,
    heads_all,
    proj_all,
    text_a,
    text_b,
    hidden_all,
    part_a,
    part_b,
    got_a,
    got_b,
    both_a,
    both_b,
    sum_a,
    sum_b,
    got_a2,
    got_b2,
    rows_all,
    acc_s,
    kv_own_a,
    kv_own_b,
    unit_own,
    code_s,
    local_sem,
    proj_s,
    proj_r,
    heads_s,
    heads_r,
    swap_s,
    swap_r,
    text_as,
    text_ar,
    text_bs,
    text_br,
    hid_s,
    hid_r,
    rs_s,
    rs_r,
    row_s,
    row_r,
    kva_s,
    kva_r,
    kvb_s,
    kvb_r,
    uq_s,
    uq_r,
):
    z, core, y, x = places()
    slot = z * 2 + core
    rows, width = patches.shape
    head = proj.shape[0]
    groups = heads_all.shape[3] // head
    group_rows = rows // groups
    side_cols = pl.ds(pl.multiple_of(core * (width // 2), 128), width // 2)
    blocks, tokens, cols = text_a.shape
    model = blocks * cols
    nq, nk = wq_hbm.shape[1], wk_hbm.shape[1]
    wide = nq + 2 * nk
    own_units = 2 * unit_own.shape[1]
    half = cols // 2
    chunk = 256

    def load(index, source, target):
        copy = pltpu.make_async_copy(source, target, local_sem.at[index])
        copy.start()
        return copy

    patches_load = load(1, patches_hbm, patches)
    qkv_load = load(2, qkv_hbm, qkv)
    proj_load = load(0, proj_hbm, proj)
    greet()
    text_loads = [
        load(3, text_hbm.at[0:tokens], text_a.at[slot]),
        load(4, text_hbm.at[tokens:], text_b.at[slot]),
    ]
    w_loads = [
        load(7, wq_hbm, w_s.at[:, 0:nq]),
        load(8, wk_hbm, w_s.at[:, nq : nq + nk]),
        load(9, wv_hbm, w_s.at[:, nq + nk : wide]),
    ]
    up_load = load(5, up_hbm, up)
    down_load = load(6, down_hbm, down)

    gain = row_of(gain_rows, 0, width // 128)
    merge_gain = row_of(merge_gain_rows, 0, width // 128)
    image_row = row_of(image, 0, rows // 128)
    patches_load.wait()
    qkv_load.wait()

    def project(i, _):
        here = pl.ds(pl.multiple_of(i * chunk, chunk), chunk)
        block = normed(patches[here, :].astype(F32), gain)
        packed = lax.dot_general(
            block, qkv[...], (((1,), (1,)), ((), ())), preferred_element_type=F32
        )
        q_s[here, :] = packed[:, 0:head].astype(BF16)
        k_s[here, :] = packed[:, head : 2 * head].astype(BF16)
        v_s[here, :] = packed[:, 2 * head : 3 * head].astype(BF16)
        return 0

    lax.fori_loop(0, rows // chunk, project, 0)

    proj_load.wait()
    proj_all[y, x, :, side_cols] = proj[:, side_cols]
    meet()
    proj_gather = Gather(
        proj_all,
        proj,
        ((slice(0, 48), side_cols), (slice(48, head), side_cols)),
        (proj_s, proj_r),
    )
    proj_gather.first()
    text_gathers = [
        RelayGather(text_a, (text_as, text_ar)),
        RelayGather(text_b, (text_bs, text_br)),
    ]
    text_gathers[0].first(text_hbm.at[0:tokens], False)
    text_gathers[0].first(text_hbm.at[0:tokens], True)
    text_gathers[1].first(text_hbm.at[tokens:], False)

    scaling = head ** (-0.5)

    def attend(i, _):
        here = pl.ds(pl.multiple_of(i * chunk, chunk), chunk)
        ids_col = column_of(image, i * (chunk // 128), chunk // 128)[:, 0:1]
        scores = lax.dot_general(
            q_s[here, :], k_s[...], (((1,), (1,)), ((), ())), preferred_element_type=F32
        )
        scores = jnp.where(ids_col == image_row, scores * scaling, NEGATIVE)
        highest = jnp.max(scores, axis=1, keepdims=True)
        weights = jnp.exp(scores - highest)
        totals = jnp.sum(weights, axis=1, keepdims=True)
        mixture = jnp.dot(weights.astype(BF16), v_s[...], preferred_element_type=F32)
        o_s[here, :] = mixture / totals
        return 0

    lax.fori_loop(0, rows // chunk, attend, 0)
    heads_all[y, x] = jnp.concatenate(
        [o_s[j * group_rows : (j + 1) * group_rows, :] for j in range(groups)], axis=1
    ).astype(BF16)
    heads_gather = Gather(
        heads_all, heads_all.at[y, x], halves(group_rows), (heads_s, heads_r)
    )
    heads_gather.first()

    def scale_of(source):
        squares = jnp.zeros((source.shape[1], 128), F32)
        for b in range(blocks):
            for g in range(cols // 128):
                piece = source[b, :, g * 128 : (g + 1) * 128].astype(F32)
                squares = squares + piece * piece
        return row_scale(jnp.sum(squares, axis=1, keepdims=True), model)

    def decode(source):
        count = source.shape[1]
        scale = scale_of(source)
        acc_s[0:count, :] = jnp.zeros((count, wide), F32)

        def one_block(b, _):
            block = source[b].astype(F32) * scale * row_of(dec_gain, b * (cols // 128), cols // 128)
            here = pl.ds(pl.multiple_of(b * cols, cols), cols)
            acc_s[0:count, :] += jnp.dot(
                block.astype(BF16), w_s[here, :], preferred_element_type=F32
            )
            return 0

        lax.fori_loop(0, blocks, one_block, 0)

    def text_part(index, source, kv_own):
        text_loads[index].wait()
        text_gathers[index].finish()
        decode(source)
        text_q[index] = acc_s[:, 0:nq].astype(BF16)
        kv_own[...] = acc_s[:, nq:].astype(BF16)

    lane_unit = lax.broadcasted_iota(jnp.int32, (128, 128), 0)
    position = lax.broadcasted_iota(jnp.int32, doc.shape, 0) * 128 + lax.broadcasted_iota(
        jnp.int32, doc.shape, 1
    )
    code_s[...] = position * 64 + doc[...]

    def units_block(b, _):
        unit = lane_unit + b * 128
        found = jnp.zeros((128, 128), jnp.int32)
        for r in range(placeholder.shape[0]):
            found = found + jnp.where(
                placeholder[r : r + 1, :] == unit, code_s[r : r + 1, :], 0
            )
        unit_code[pl.ds(b, 1), :] = jnp.sum(found.T, axis=0, keepdims=True)
        return 0

    proj_gather.second(relayed=True)
    heads_gather.second(relayed=True)
    text_gathers[0].relay()
    text_gathers[1].first(text_hbm.at[tokens:], True)
    lax.fori_loop(0, unit_code.shape[0] // 2, units_block, 0)
    proj_gather.relay()
    lax.fori_loop(unit_code.shape[0] // 2, unit_code.shape[0], units_block, 0)
    heads_gather.relay()
    text_gathers[0].second()
    proj_gather.finish()
    swap = remote(
        proj_all.at[:, :, :, side_cols],
        proj_all.at[:, :, :, side_cols],
        swap_s,
        swap_r,
        at_device(z, 1 - core, y, x),
    )
    swap.start()
    for w_load in w_loads:
        w_load.wait()
    text_part(0, text_a, kv_own_a)
    kv_a = Gather(
        text_kv.at[0], kv_own_a, halves(tokens), (kva_s, kva_r), own_sem=local_sem.at[10]
    )
    kv_a.first()
    text_gathers[1].relay()
    swap.wait_recv()
    heads_gather.finish()

    for j in range(groups):
        lhs_s[j * group_rows : (j + 1) * group_rows, :] = jnp.concatenate(
            [
                heads_all[a, b, :, j * head : (j + 1) * head].astype(F32)
                for a in range(SIDE)
                for b in range(SIDE)
            ],
            axis=1,
        ).astype(BF16)

    def merge(i, _):
        here = pl.ds(pl.multiple_of(i * chunk, chunk), chunk)
        terms = jnp.dot(
            lhs_s[here, :], proj_all[...].reshape(width, width), preferred_element_type=F32
        )
        out = (patches[here, :].astype(F32) + terms).astype(BF16)
        ready = normed(out.astype(F32), merge_gain).astype(F32)
        for g in range(width // 128):
            norm_s[g, here, :] = ready[:, g * 128 : (g + 1) * 128]
        return 0

    lax.fori_loop(0, rows // chunk, merge, 0)
    kv_a.second(relayed=True)
    text_gathers[1].second()
    units = rows // 4
    up_load.wait()
    total = jnp.zeros((units, up.shape[0]), F32)
    for k in range(4):
        quarter = jnp.concatenate(
            [norm_s[g, pl.ds(k, units, stride=4), :] for g in range(width // 128)], axis=1
        ).astype(BF16)
        total = total + lax.dot_general(
            quarter,
            up[:, k * width : (k + 1) * width],
            (((1,), (1,)), ((), ())),
            preferred_element_type=F32,
        )
    hidden = gelu(total).astype(BF16)
    share = own_units // 2
    hidden_gathers = []
    for h in range(2):
        hidden_all[h, slot] = jnp.concatenate(
            [
                hidden[(2 * v + h) * share : (2 * v + h + 1) * share, :]
                for v in range(units // own_units)
            ],
            axis=0,
        )
        hidden_gathers.append(EncGather(hidden_all.at[h], (hid_s.at[h], hid_r.at[h])))
        hidden_gathers[h].first(hidden_all.at[h, slot])
    text_part(1, text_b, kv_own_b)
    kv_b = Gather(
        text_kv.at[1], kv_own_b, halves(tokens), (kvb_s, kvb_r), own_sem=local_sem.at[11]
    )
    kv_a.relay()
    kv_b.first()
    down_load.wait()

    one, two = [{}, {}], [[], []]

    def share_rows(index):
        return pl.ds(pl.multiple_of(index * share, share), share)

    def summed(own, others):
        return sum((others[d].astype(F32) for d in range(SIDE - 1)), own.astype(F32))

    ring_ways = (
        (part_a, got_a, both_a, slice(0, half)),
        (part_b, got_b, both_b, slice(half, cols)),
    )
    low, high = slice(0, half // 2), slice(half // 2, half)

    def neighbour(way, d):
        return at_device(z, core, y, ring(x, d)) if way == 0 else at_device(z, core, ring(y, d), x)

    def pass_on(h, way, index, source, d):
        copy = remote(
            source,
            ring_ways[way][1].at[h, index],
            rs_s.at[h, way, index],
            rs_r.at[h, way, index],
            neighbour(way, d),
        )
        copy.start()
        one[h][way, index] = copy

    def terms(h):
        for d in (2, 1, 3, 0):
            xp, yp = ring(x, d), ring(y, d)
            lhs_a = jnp.concatenate(
                [
                    hidden_all[h, 2 * v + xp // 2, share_rows(lax.rem(xp, 2)), :]
                    for v in range(SIDE)
                ],
                axis=0,
            )
            lhs_b = jnp.concatenate(
                [hidden_all[h, 2 * yp + v // 2, share_rows(v % 2), :] for v in range(SIDE)],
                axis=0,
            )
            for way, lhs in enumerate((lhs_a, lhs_b)):
                part, got, both, columns = ring_ways[way]
                part[h, d] = jnp.dot(
                    lhs, down[:, columns], preferred_element_type=F32
                ).astype(BF16)
                if d == 2:
                    pass_on(h, way, 0, part.at[h, d, :, low], 1)
                    pass_on(h, way, 1, part.at[h, d, :, high], 3)
                elif d == 1:
                    pass_on(h, way, 2, part.at[h, d, :, high], 1)
                elif d == 3:
                    pass_on(h, way, 3, part.at[h, d, :, low], 3)

    def combine(h):
        for way in range(2):
            part, got, both, columns = ring_ways[way]
            for index, (d, side) in enumerate(((1, low), (3, high))):
                one[h][way, index].wait_recv()
                both[h, index] = (
                    part[h, d, :, side].astype(F32) + got[h, index].astype(F32)
                ).astype(BF16)
                pass_on(h, way, 4 + index, both.at[h, index], d)

    def ring_total(h, way):
        part, got, both, columns = ring_ways[way]
        for index in range(2, 6):
            one[h][way, index].wait_recv()
        others = jnp.concatenate(
            [
                got[h, 4].astype(F32) + got[h, 3].astype(F32),
                got[h, 2].astype(F32) + got[h, 5].astype(F32),
            ],
            axis=1,
        )
        return (part[h, 0].astype(F32) + others).astype(BF16)

    def ring_sums(h):
        sum_a[h] = ring_total(h, 0)
        sum_b[h] = ring_total(h, 1)
        for d in range(1, SIDE):
            xp, yp = ring(x, d), ring(y, d)
            for way, (total_s, place, got, device) in enumerate(
                (
                    (sum_a, yp, got_a2, at_device(z, core, yp, x)),
                    (sum_b, xp, got_b2, at_device(z, core, y, xp)),
                )
            ):
                copy = remote(
                    total_s.at[h, share_rows(place)],
                    got.at[h, d - 1],
                    rs_s.at[h, 2 + way, d - 1],
                    rs_r.at[h, 2 + way, d - 1],
                    device,
                )
                copy.start()
                two[h].append(copy)

    rows_gathers = [
        EncGather(rows_all.at[h], (row_s.at[h], row_r.at[h])) for h in range(2)
    ]

    def full_sums(h):
        for copy in two[h]:
            copy.wait_recv()
        rows_all[h, slot] = jnp.concatenate(
            [
                summed(sum_a[h, share_rows(y), :], got_a2.at[h]),
                summed(sum_b[h, share_rows(x), :], got_b2.at[h]),
            ],
            axis=1,
        ).astype(BF16)
        rows_gathers[h].first(rows_all.at[h, slot])

    unit_parts = (
        (slice(0, share), slice(0, wide // 2)),
        (slice(0, share), slice(wide // 2, wide)),
    )
    unit_gathers = [
        Gather(
            unit_qkv.at[h],
            unit_own.at[h],
            unit_parts,
            (uq_s.at[h], uq_r.at[h]),
            own_sem=local_sem.at[12 + h],
        )
        for h in range(2)
    ]

    def decode_units(h):
        decode(rows_all.at[h])
        unit_own[h] = acc_s[0:share, :].astype(BF16)
        unit_gathers[h].first()

    hidden_gathers[0].second()
    hidden_gathers[0].finish()
    terms(0)
    hidden_gathers[1].second()
    hidden_gathers[1].finish()
    combine(0)
    terms(1)
    ring_sums(0)
    combine(1)
    full_sums(0)
    ring_sums(1)
    kv_b.second(relayed=True)
    rows_gathers[0].second()
    full_sums(1)
    rows_gathers[0].finish()
    decode_units(0)
    kv_b.relay()
    rows_gathers[1].second()
    rows_gathers[1].finish()
    decode_units(1)
    unit_gathers[0].second(relayed=True)
    unit_gathers[1].second()
    unit_gathers[0].relay()
    for gather in unit_gathers + [kv_a, kv_b]:
        gather.finish()
    swap.wait_send()
    for copy in [*one[0].values(), *one[1].values(), *two[0], *two[1]]:
        copy.wait_send()
    for gather in [proj_gather, heads_gather, kv_a, kv_b] + unit_gathers:
        gather.drain()
    for gather in text_gathers + hidden_gathers + rows_gathers:
        gather.drain()


def tower(
    image,
    gain,
    merge_gain,
    dec_gain,
    doc,
    placeholder,
    patches,
    qkv,
    proj,
    up,
    text,
    down,
    wq,
    wk,
    wv,
):
    rows, width = patches.shape
    head = proj.shape[0]
    groups = 8
    units = rows // 4
    cols = text.shape[1]
    tokens = text.shape[0] // 2
    nq, nk = wq.shape[1], wk.shape[1]
    wide = nq + 2 * nk
    own_units = 8 * units // (SIDE * SIDE)
    share = own_units // 2
    half = cols // 2
    dma = pltpu.SemaphoreType.DMA
    whole = pl.BlockSpec(memory_space=VMEM)
    anywhere = pl.BlockSpec(memory_space=pl.ANY)

    def both(shape):
        return [dma(shape), dma(shape)]

    return pl.pallas_call(
        tower_kernel,
        out_shape=(
            jax.ShapeDtypeStruct((2, tokens, nq), BF16),
            jax.ShapeDtypeStruct((2, SIDE, SIDE, tokens, 2 * nk), BF16),
            jax.ShapeDtypeStruct((2, SIDE, SIDE, share, wide), BF16),
            jax.ShapeDtypeStruct((own_units * 16 // 128, 128), jnp.int32),
        ),
        in_specs=[whole] * 6 + [anywhere] * 9,
        out_specs=(whole, anywhere, anywhere, whole),
        scratch_shapes=[
            VMEM((rows, width), BF16),
            VMEM(qkv.shape, BF16),
            VMEM((head, width), BF16),
            VMEM(up.shape, BF16),
            VMEM(down.shape, BF16),
            VMEM((8 * cols, wide), BF16),
            VMEM((rows, head), BF16),
            VMEM((rows, head), BF16),
            VMEM((rows, head), BF16),
            VMEM((rows, head), F32),
            VMEM((rows, width), BF16),
            VMEM((width // 128, rows, 128), F32),
            VMEM((SIDE, SIDE, rows // groups, groups * head), BF16),
            VMEM((SIDE, SIDE, head, width), BF16),
            VMEM((8, tokens, cols), BF16),
            VMEM((8, tokens, cols), BF16),
            VMEM((2, 8, units // 2, up.shape[0]), BF16),
            VMEM((2, SIDE, SIDE * share, half), BF16),
            VMEM((2, SIDE, SIDE * share, half), BF16),
            VMEM((2, 6, SIDE * share, half // 2), BF16),
            VMEM((2, 6, SIDE * share, half // 2), BF16),
            VMEM((2, 2, SIDE * share, half // 2), BF16),
            VMEM((2, 2, SIDE * share, half // 2), BF16),
            VMEM((2, SIDE * share, half), BF16),
            VMEM((2, SIDE * share, half), BF16),
            VMEM((2, SIDE - 1, share, half), BF16),
            VMEM((2, SIDE - 1, share, half), BF16),
            VMEM((2, 8, share, cols), BF16),
            VMEM((tokens, wide), F32),
            VMEM((tokens, 2 * nk), BF16),
            VMEM((tokens, 2 * nk), BF16),
            VMEM((2, share, wide), BF16),
            VMEM(doc.shape, jnp.int32),
            dma((14,)),
            *both((4, 4)),
            *both((4, 4)),
            *both(()),
            *both((10,)),
            *both((10,)),
            *both((2, 7)),
            *both((2, 4, 6)),
            *both((2, 7)),
            *both((4, 4)),
            *both((4, 4)),
            *both((2, 4, 4)),
        ],
        compiler_params=pltpu.CompilerParams(
            collective_id=1, has_side_effects=True, vmem_limit_bytes=60 * 2**20
        ),
        name="tower",
    )(
        image,
        gain,
        merge_gain,
        dec_gain,
        doc,
        placeholder,
        patches,
        qkv,
        proj,
        up,
        text,
        down,
        wq,
        wk,
        wv,
    )


def attention_kernel(
    where_ref,
    doc_smem,
    text_q,
    unit_code,
    doc_rows,
    unit_rows,
    text_kv_hbm,
    unit_qkv_hbm,
    out,
    text_kv,
    unit_qkv,
    load_sem,
    q_s,
    peak_s,
    mix_s,
    bias_s,
):
    tokens, nq = text_q.shape
    nk = text_kv.shape[2] // 2
    unit_loads = []
    for p in range(2):
        share = unit_qkv.shape[1] // 2
        here = slice(p * share, (p + 1) * share)
        unit_loads.append(
            pltpu.make_async_copy(
                unit_qkv_hbm.at[p], unit_qkv.at[:, here, :], load_sem.at[2 + p]
            )
        )
        unit_loads[p].start()
    text_loads = []
    for p in range(2):
        here = slice(p * (tokens // 2), (p + 1) * (tokens // 2))
        text_loads.append(
            pltpu.make_async_copy(text_kv_hbm.at[p], text_kv.at[:, here, :], load_sem.at[p])
        )
        text_loads[p].start()
    heads = nq // HD
    units = unit_qkv.shape[0] * unit_qkv.shape[1]
    mine = where_ref[0]
    first_doc = doc_smem[mine * tokens]
    scale = HD ** (-0.5) * math.log2(math.e)

    lines = tokens // 128
    query_doc = column_of(doc_rows, mine * lines, lines)
    query_unit = column_of(unit_rows, mine * lines, lines)
    query_at = mine * tokens + lax.broadcasted_iota(jnp.int32, (tokens, 128), 0)
    lane = lax.broadcasted_iota(jnp.int32, (tokens, 128), 1)

    picked = jnp.zeros((tokens, nq), F32)
    chunk = 384
    for unit_load in unit_loads:
        unit_load.wait()
    per_chunk = chunk // unit_qkv.shape[1]
    for b in range(units // chunk):
        chosen = jnp.concatenate(
            [
                (query_unit == lane + (b * chunk + g * 128)).astype(F32)
                for g in range(chunk // 128)
            ],
            axis=1,
        ).astype(BF16)
        source = unit_qkv[b * per_chunk : (b + 1) * per_chunk, :, 0:nq].reshape(chunk, nq)
        picked = picked + jnp.dot(chosen, source, preferred_element_type=F32)
    for j in range(heads):
        part = slice(j * HD, (j + 1) * HD)
        q_s[j] = jnp.where(query_unit >= 0, picked[:, part], text_q[:, part].astype(F32)).astype(
            BF16
        )
    peak_s[...] = jnp.full_like(peak_s, NEGATIVE)
    mix_s[...] = jnp.zeros_like(mix_s)
    row_chunk = 128

    def fold(keys, values):
        values = jnp.concatenate([values, jnp.ones_like(values)], axis=1)
        for r in range(0, tokens, row_chunk):
            here = slice(r, r + row_chunk)
            for j in range(heads):
                scores = lax.dot_general(
                    q_s[j, here, :], keys, (((1,), (1,)), ((), ())), preferred_element_type=F32
                )
                scores = scores + bias_s[here, :]
                before = peak_s[j, here, :]
                peak = jnp.maximum(before, jnp.max(scores, axis=1, keepdims=True))
                factor = jnp.exp2((before - peak) * scale)
                wide_peak = jnp.concatenate([peak] * (scores.shape[1] // 128), axis=1)
                weights = jnp.exp2((scores - wide_peak) * scale).astype(BF16)
                peak_s[j, here, :] = peak
                mix_s[j, here, :] = mix_s[j, here, :] * jnp.concatenate(
                    [factor] * 2, axis=1
                ) + jnp.dot(weights, values, preferred_element_type=F32)

    def text_block(i, _):
        blocks = []
        for t in range(2):
            s = begin + 2 * i + t
            held = jnp.minimum(s, text_kv.shape[0] - 1)
            for g in range(lines):
                key_at = s * tokens + g * 128 + lane
                same = query_doc == doc_rows[pl.ds(held * lines + g, 1), :]
                text = unit_rows[pl.ds(held * lines + g, 1), :] < 0
                allowed = same & (key_at <= query_at) & text
                bias_s[:, t * tokens + g * 128 : t * tokens + (g + 1) * 128] = jnp.where(
                    allowed, 0.0, NEGATIVE
                )
            blocks.append(text_kv[held])
        both = jnp.concatenate(blocks, axis=0)
        fold(both[:, 0:nk], both[:, nk:])
        return 0

    begin = jnp.int32(0)
    for s in range(text_kv.shape[0]):
        begin = begin + (doc_smem[(s + 1) * tokens - 1] < first_doc).astype(jnp.int32)
    for text_load in text_loads:
        text_load.wait()
    lax.fori_loop(0, (mine + 2 - begin) // 2, text_block, 0)

    pair = 2 * chunk

    def unit_block(b, _):
        for g in range(pair // 128):
            code = unit_code[pl.ds(b * (pair // 128) + g, 1), :]
            allowed = (query_doc == (code & 63)) & ((code >> 6) <= query_at)
            bias_s[:, g * 128 : (g + 1) * 128] = jnp.where(allowed, 0.0, NEGATIVE)
        block = unit_qkv[pl.ds(b * 2 * per_chunk, 2 * per_chunk), :, nq:].reshape(pair, 2 * nk)
        fold(block[:, 0:nk], block[:, nk:])
        return 0

    lax.fori_loop(0, units // pair, unit_block, 0)
    for j in range(heads):
        out[:, j * HD : (j + 1) * HD] = (mix_s[j, :, 0:HD] / mix_s[j, :, HD:]).astype(BF16)


def attention(where, doc, text_q, text_kv, unit_qkv, unit_code, placeholder):
    tokens, nq = text_q.shape
    heads = nq // HD
    shards = text_kv.shape[1]
    whole = pl.BlockSpec(memory_space=VMEM)
    anywhere = pl.BlockSpec(memory_space=pl.ANY)
    scalars = pl.BlockSpec(memory_space=pltpu.SMEM)
    return pl.pallas_call(
        attention_kernel,
        out_shape=jax.ShapeDtypeStruct((tokens, nq), BF16),
        in_specs=[scalars, scalars] + [whole] * 4 + [anywhere] * 2,
        out_specs=whole,
        scratch_shapes=[
            VMEM((shards, tokens, text_kv.shape[3]), BF16),
            VMEM((shards, 2 * unit_qkv.shape[2], unit_qkv.shape[3]), BF16),
            pltpu.SemaphoreType.DMA((4,)),
            VMEM((heads, tokens, HD), BF16),
            VMEM((heads, tokens, 128), F32),
            VMEM((heads, tokens, 2 * HD), F32),
            VMEM((tokens, 2 * tokens), F32),
        ],
        compiler_params=pltpu.CompilerParams(vmem_limit_bytes=60 * 2**20),
        name="attention",
    )(
        where,
        doc,
        text_q,
        unit_code,
        doc.reshape(-1, 128),
        placeholder.reshape(-1, 128),
        text_kv,
        unit_qkv,
    )


def body(
    patches,
    patch_image,
    vit_gain,
    vit_qkv,
    vit_proj,
    merge_gain,
    merge_up,
    merge_down,
    text_embed,
    placeholder_unit,
    doc_id,
    dec_gain,
    dec_wq,
    dec_wk,
    dec_wv,
):
    tokens = text_embed.shape[0]
    text_q, text_kv, unit_qkv, unit_code = tower(
        patch_image.reshape(-1, 128),
        vit_gain.reshape(-1, 128),
        merge_gain.reshape(-1, 128),
        dec_gain.reshape(-1, 128),
        doc_id.reshape(-1, 128),
        placeholder_unit.reshape(-1, 128),
        patches,
        vit_qkv.transpose(1, 2, 0).reshape(-1, vit_qkv.shape[0]),
        vit_proj,
        merge_up.T,
        text_embed,
        merge_down,
        dec_wq,
        dec_wk,
        dec_wv,
    )
    where = lax.axis_index("ctx").astype(jnp.int32).reshape(1)
    return attention(
        where,
        doc_id,
        text_q.reshape(tokens, -1),
        text_kv.reshape(2, 16, tokens // 2, -1),
        unit_qkv.reshape(2, 16, -1, unit_qkv.shape[-1]),
        unit_code,
        placeholder_unit,
    )


def solution(mesh):
    placed = (
        P("enc", None),
        P("enc"),
        P(),
        P(None, "ctx", None),
        P("ctx", None),
        P(),
        P(None, "ctx"),
        P("ctx", "enc"),
        P("ctx", "enc"),
        P(),
        P(),
        P(),
        P(None, "enc"),
        P(None, "enc"),
        P(None, "enc"),
    )
    return jax.shard_map(
        body, mesh=mesh, in_specs=placed, out_specs=P("ctx", "enc"), check_vma=False
    )
```

```python
import functools
import math

import jax
import jax.numpy as jnp
from jax import lax
from jax.experimental import pallas as pl
from jax.experimental.pallas import tpu as pltpu
from jax.sharding import PartitionSpec as P

MESH = pl.DeviceIdType.MESH
VMEM = pltpu.VMEM
F32 = jnp.float32
BF16 = jnp.bfloat16

HD = 128
QPK = 4
EPSILON = 1e-06
NEGATIVE = -1e30
SIDE = 4


def places():
    e, c = lax.axis_index("enc"), lax.axis_index("ctx")
    return e // 2, lax.rem(e, 2), c // SIDE, lax.rem(c, SIDE)


def at_device(z, core, y, x):
    return {"enc": z * 2 + core, "ctx": y * SIDE + x}


def ring(position, distance):
    return lax.rem(position + distance, SIDE)


def remote(source, target, send_sem, recv_sem, device):
    return pltpu.make_async_remote_copy(
        src_ref=source,
        dst_ref=target,
        send_sem=send_sem,
        recv_sem=recv_sem,
        device_id=device,
        device_id_type=MESH,
    )


def ring_peers():
    z, core, y, x = places()
    peers = []
    for d in range(1, SIDE):
        peers.append(at_device(z, core, y, ring(x, d)))
        peers.append(at_device(z, core, ring(y, d), x))
        peers.append(at_device(ring(z, d), core, y, x))
    peers.append(at_device(z, 1 - core, y, x))
    return peers


def greet():
    for peer in ring_peers():
        pl.semaphore_signal(
            pltpu.get_barrier_semaphore(), inc=1, device_id=peer, device_id_type=MESH
        )


def meet():
    pl.semaphore_wait(pltpu.get_barrier_semaphore(), len(ring_peers()))


def row_of(ref, first, count):
    return jnp.concatenate([ref[pl.ds(first + g, 1), :] for g in range(count)], axis=1)


def column_of(ref, first, count):
    return jnp.concatenate(
        [jnp.broadcast_to(ref[pl.ds(first + g, 1), :], (128, 128)).T for g in range(count)],
        axis=0,
    )


class Gather:
    def __init__(self, buf, own, parts, sems, own_sem=None):
        self.buf, self.own, self.own_sem = buf, own, own_sem
        self.send, self.recv = sems
        self.part_a, self.part_b = parts

    def start(self, phase, pairs, distances):
        z, core, y, x = places()
        copies = {}
        for d in distances:
            for way, (source, target) in enumerate(pairs):
                along_x = way == phase
                device = (
                    at_device(z, core, y, ring(x, d))
                    if along_x
                    else at_device(z, core, ring(y, d), x)
                )
                sem = (2 * phase + way, d - 1)
                copies[way, d] = remote(
                    source, target, self.send.at[sem], self.recv.at[sem], device
                )
        for copy in copies.values():
            copy.start()
        return copies

    def first(self):
        z, core, y, x = places()
        if self.own_sem is not None:
            self.own_copy = pltpu.make_async_copy(self.own, self.buf.at[y, x], self.own_sem)
            self.own_copy.start()
        self.one = self.start(
            0,
            [
                (self.own.at[part], self.buf.at[(y, x) + part])
                for part in (self.part_a, self.part_b)
            ],
            (1, 2, 3),
        )

    def lines(self, row, column, some=slice(None)):
        return (
            self.buf.at[(row, some) + self.part_a],
            self.buf.at[(some, column) + self.part_b],
        )

    def second(self, relayed=False):
        z, core, y, x = places()
        if self.own_sem is not None:
            self.own_copy.wait()
        for copy in self.one.values():
            copy.wait_recv()
        self.relayed = relayed
        self.two = self.start(
            1, [(line, line) for line in self.lines(y, x)], (1, 3) if relayed else (1, 2, 3)
        )
        self.handed = {}

    def relay(self):
        z, core, y, x = places()
        for index, (d, some) in enumerate(((1, slice(0, 2)), (3, slice(2, 4)))):
            for way in range(2):
                self.two[way, d].wait_recv()
                line = self.lines(ring(y, SIDE - d), ring(x, SIDE - d), some)[way]
                device = (
                    at_device(z, core, ring(y, d), x)
                    if way == 0
                    else at_device(z, core, y, ring(x, d))
                )
                sem = (2 + way, 1 + 2 * index)
                self.handed[way, d] = remote(
                    line, line, self.send.at[sem], self.recv.at[sem], device
                )
                self.handed[way, d].start()

    def finish(self):
        for copy in (self.handed if self.relayed else self.two).values():
            copy.wait_recv()

    def drain(self):
        for copies in (self.one, self.two, self.handed):
            for copy in copies.values():
                copy.wait_send()


class EncGather:
    def __init__(self, buf, sems):
        self.buf = buf
        self.send, self.recv = sems

    def first(self, own):
        z, core, y, x = places()
        slot = z * 2 + core
        copies = [
            remote(
                own,
                self.buf.at[slot],
                self.send.at[d - 1],
                self.recv.at[d - 1],
                at_device(ring(z, d), core, y, x),
            )
            for d in range(1, SIDE)
        ]
        copies.append(
            remote(
                own,
                self.buf.at[slot],
                self.send.at[3],
                self.recv.at[3],
                at_device(z, 1 - core, y, x),
            )
        )
        for copy in copies:
            copy.start()
        self.copies = copies

    def second(self):
        z, core, y, x = places()
        self.handed = []
        for d in range(1, SIDE):
            self.copies[d - 1].wait_recv()
            slot = ring(z, SIDE - d) * 2 + core
            copy = remote(
                self.buf.at[slot],
                self.buf.at[slot],
                self.send.at[3 + d],
                self.recv.at[3 + d],
                at_device(z, 1 - core, y, x),
            )
            copy.start()
            self.handed.append(copy)

    def finish(self):
        self.copies[3].wait_recv()
        for copy in self.handed:
            copy.wait_recv()

    def drain(self):
        for copy in self.copies + self.handed:
            copy.wait_send()


class RelayGather:
    def __init__(self, buf, sems):
        self.buf = buf
        self.send, self.recv = sems
        self.copies = {}

    def copy(self, index, source, target, device):
        copy = remote(source, target, self.send.at[index], self.recv.at[index], device)
        copy.start()
        self.copies[index] = copy

    def first(self, own, high):
        z, core, y, x = places()
        middle, rows = self.buf.shape[1] // 2, self.buf.shape[1]
        slot = z * 2 + core
        part = slice(middle, rows) if high else slice(0, middle)
        for index, d in ((8, 1), (9, 3)) if high else ((0, 1), (1, 3)):
            self.copy(
                index,
                own.at[part],
                self.buf.at[slot, part],
                at_device(ring(z, d), core, y, x),
            )
        if not high:
            self.copy(2, own, self.buf.at[slot], at_device(z, 1 - core, y, x))

    def relay(self):
        z, core, y, x = places()
        middle = self.buf.shape[1] // 2
        left, right = ring(z, 3) * 2 + core, ring(z, 1) * 2 + core
        self.copies[0].wait_recv()
        low = self.buf.at[left, 0:middle]
        self.copy(3, low, low, at_device(ring(z, 1), core, y, x))
        self.copies[9].wait_recv()
        high = self.buf.at[right, middle:]
        self.copy(4, high, high, at_device(ring(z, 3), core, y, x))
        self.copies[1].wait_recv()
        self.copies[8].wait_recv()
        for index, block in ((5, left), (6, right)):
            whole = self.buf.at[block]
            self.copy(index, whole, whole, at_device(z, 1 - core, y, x))

    def second(self):
        z, core, y, x = places()
        self.copies[3].wait_recv()
        self.copies[4].wait_recv()
        far = self.buf.at[ring(z, 2) * 2 + core]
        self.copy(7, far, far, at_device(z, 1 - core, y, x))

    def finish(self):
        for index in (2, 5, 6, 7):
            self.copies[index].wait_recv()

    def drain(self):
        for copy in self.copies.values():
            copy.wait_send()


def halves(rows):
    return (slice(0, rows // 2), slice(None)), (slice(rows // 2, rows), slice(None))


def normed(wide, gain):
    center = wide - jnp.mean(wide, axis=1, keepdims=True)
    spread = jnp.mean(center * center, axis=1, keepdims=True)
    return (center * lax.rsqrt(spread + EPSILON) * gain).astype(BF16)


def gelu(x):
    return 0.5 * x * (1.0 + lax.erf(x * math.sqrt(0.5)))


def row_scale(total, count):
    return lax.rsqrt(total / count + EPSILON)


def tower_kernel(
    image,
    gain_rows,
    merge_gain_rows,
    dec_gain,
    doc,
    placeholder,
    patches_hbm,
    qkv_hbm,
    proj_hbm,
    up_hbm,
    text_hbm,
    down_hbm,
    wq_hbm,
    wk_hbm,
    wv_hbm,
    text_q,
    text_kv,
    unit_qkv,
    unit_code,
    patches,
    qkv,
    proj,
    up,
    down,
    w_s,
    q_s,
    k_s,
    v_s,
    o_s,
    lhs_s,
    norm_s,
    heads_all,
    proj_all,
    text_a,
    text_b,
    hidden_all,
    part_a,
    part_b,
    got_a,
    got_b,
    both_a,
    both_b,
    sum_a,
    sum_b,
    got_a2,
    got_b2,
    rows_all,
    acc_s,
    kv_own_a,
    kv_own_b,
    unit_own,
    code_s,
    local_sem,
    proj_s,
    proj_r,
    heads_s,
    heads_r,
    swap_s,
    swap_r,
    text_as,
    text_ar,
    text_bs,
    text_br,
    hid_s,
    hid_r,
    rs_s,
    rs_r,
    row_s,
    row_r,
    kva_s,
    kva_r,
    kvb_s,
    kvb_r,
    uq_s,
    uq_r,
):
    z, core, y, x = places()
    slot = z * 2 + core
    rows, width = patches.shape
    head = proj.shape[0]
    groups = heads_all.shape[3] // head
    group_rows = rows // groups
    side_cols = pl.ds(pl.multiple_of(core * (width // 2), 128), width // 2)
    blocks, tokens, cols = text_a.shape
    model = blocks * cols
    nq, nk = wq_hbm.shape[1], wk_hbm.shape[1]
    wide = nq + 2 * nk
    own_units = 2 * unit_own.shape[1]
    half = cols // 2
    chunk = 256

    def load(index, source, target):
        copy = pltpu.make_async_copy(source, target, local_sem.at[index])
        copy.start()
        return copy

    patches_load = load(1, patches_hbm, patches)
    qkv_load = load(2, qkv_hbm, qkv)
    proj_load = load(0, proj_hbm, proj)
    greet()
    text_loads = [
        load(3, text_hbm.at[0:tokens], text_a.at[slot]),
        load(4, text_hbm.at[tokens:], text_b.at[slot]),
    ]
    w_loads = [
        load(7, wq_hbm, w_s.at[:, 0:nq]),
        load(8, wk_hbm, w_s.at[:, nq : nq + nk]),
        load(9, wv_hbm, w_s.at[:, nq + nk : wide]),
    ]
    up_load = load(5, up_hbm, up)
    down_load = load(6, down_hbm, down)

    gain = row_of(gain_rows, 0, width // 128)
    merge_gain = row_of(merge_gain_rows, 0, width // 128)
    image_row = row_of(image, 0, rows // 128)
    patches_load.wait()
    qkv_load.wait()

    def project(i, _):
        here = pl.ds(pl.multiple_of(i * chunk, chunk), chunk)
        block = normed(patches[here, :].astype(F32), gain)
        packed = lax.dot_general(
            block, qkv[...], (((1,), (1,)), ((), ())), preferred_element_type=F32
        )
        q_s[here, :] = packed[:, 0:head].astype(BF16)
        k_s[here, :] = packed[:, head : 2 * head].astype(BF16)
        v_s[here, :] = packed[:, 2 * head : 3 * head].astype(BF16)
        return 0

    lax.fori_loop(0, rows // chunk, project, 0)

    proj_load.wait()
    proj_all[y, x, :, side_cols] = proj[:, side_cols]
    meet()
    proj_gather = Gather(
        proj_all,
        proj,
        ((slice(0, 48), side_cols), (slice(48, head), side_cols)),
        (proj_s, proj_r),
    )
    proj_gather.first()
    text_gathers = [
        RelayGather(text_a, (text_as, text_ar)),
        RelayGather(text_b, (text_bs, text_br)),
    ]
    text_gathers[0].first(text_hbm.at[0:tokens], False)
    text_gathers[0].first(text_hbm.at[0:tokens], True)

    scaling = head ** (-0.5)

    def attend(i, _):
        here = pl.ds(pl.multiple_of(i * chunk, chunk), chunk)
        ids_col = column_of(image, i * (chunk // 128), chunk // 128)[:, 0:1]
        scores = lax.dot_general(
            q_s[here, :], k_s[...], (((1,), (1,)), ((), ())), preferred_element_type=F32
        )
        scores = jnp.where(ids_col == image_row, scores * scaling, NEGATIVE)
        highest = jnp.max(scores, axis=1, keepdims=True)
        weights = jnp.exp(scores - highest)
        totals = jnp.sum(weights, axis=1, keepdims=True)
        mixture = jnp.dot(weights.astype(BF16), v_s[...], preferred_element_type=F32)
        o_s[here, :] = mixture / totals
        return 0

    lax.fori_loop(0, rows // chunk, attend, 0)
    heads_all[y, x] = jnp.concatenate(
        [o_s[j * group_rows : (j + 1) * group_rows, :] for j in range(groups)], axis=1
    ).astype(BF16)
    heads_gather = Gather(
        heads_all, heads_all.at[y, x], halves(group_rows), (heads_s, heads_r)
    )
    heads_gather.first()

    def scale_of(source):
        squares = jnp.zeros((source.shape[1], 128), F32)
        for b in range(blocks):
            for g in range(cols // 128):
                piece = source[b, :, g * 128 : (g + 1) * 128].astype(F32)
                squares = squares + piece * piece
        return row_scale(jnp.sum(squares, axis=1, keepdims=True), model)

    def decode_some(source, scale, first, last):
        count = source.shape[1]

        def one_block(b, _):
            block = (
                source[b].astype(F32)
                * scale
                * row_of(dec_gain, b * (cols // 128), cols // 128)
            )
            here = pl.ds(pl.multiple_of(b * cols, cols), cols)
            acc_s[0:count, :] += jnp.dot(
                block.astype(BF16), w_s[here, :], preferred_element_type=F32
            )
            return 0

        if first == 0:
            acc_s[0:count, :] = jnp.zeros((count, wide), F32)
        lax.fori_loop(first, last, one_block, 0)

    def text_begin(index, source):
        text_loads[index].wait()
        text_gathers[index].finish()
        scale = scale_of(source)
        decode_some(source, scale, 0, blocks // 2)
        return scale

    def text_end(index, source, scale, kv_own):
        decode_some(source, scale, blocks // 2, blocks)
        text_q[index] = acc_s[:, 0:nq].astype(BF16)
        kv_own[...] = acc_s[:, nq:].astype(BF16)

    lane_unit = lax.broadcasted_iota(jnp.int32, (128, 128), 0)
    position = lax.broadcasted_iota(jnp.int32, doc.shape, 0) * 128 + lax.broadcasted_iota(
        jnp.int32, doc.shape, 1
    )
    code_s[...] = position * 64 + doc[...]

    def units_block(b, _):
        unit = lane_unit + b * 128
        found = jnp.zeros((128, 128), jnp.int32)
        for r in range(placeholder.shape[0]):
            found = found + jnp.where(
                placeholder[r : r + 1, :] == unit, code_s[r : r + 1, :], 0
            )
        unit_code[pl.ds(b, 1), :] = jnp.sum(found.T, axis=0, keepdims=True)
        return 0

    proj_gather.second(relayed=True)
    heads_gather.second(relayed=True)
    text_gathers[0].relay()
    text_gathers[1].first(text_hbm.at[tokens:], False)
    text_gathers[1].first(text_hbm.at[tokens:], True)
    lax.fori_loop(0, unit_code.shape[0] // 2, units_block, 0)
    proj_gather.relay()
    lax.fori_loop(unit_code.shape[0] // 2, unit_code.shape[0], units_block, 0)
    text_gathers[0].second()
    heads_gather.relay()
    for w_load in w_loads:
        w_load.wait()
    text_scale = text_begin(0, text_a)
    proj_gather.finish()
    swap = remote(
        proj_all.at[:, :, :, side_cols],
        proj_all.at[:, :, :, side_cols],
        swap_s,
        swap_r,
        at_device(z, 1 - core, y, x),
    )
    swap.start()
    text_end(0, text_a, text_scale, kv_own_a)
    kv_a = Gather(
        text_kv.at[0], kv_own_a, halves(tokens), (kva_s, kva_r), own_sem=local_sem.at[10]
    )
    kv_a.first()
    heads_gather.finish()
    text_gathers[1].relay()

    for j in range(groups):
        lhs_s[j * group_rows : (j + 1) * group_rows, :] = jnp.concatenate(
            [
                heads_all[a, b, :, j * head : (j + 1) * head].astype(F32)
                for a in range(SIDE)
                for b in range(SIDE)
            ],
            axis=1,
        ).astype(BF16)

    swap.wait_recv()
    share = own_units // 2
    piece = 4 * share
    pieces = rows // piece // 2
    hidden_gathers = []
    for h in range(2):

        def merge(v, _):
            here = pl.ds(pl.multiple_of((2 * v + h) * piece, piece), piece)
            terms = jnp.dot(
                lhs_s[here, :], proj_all[...].reshape(width, width), preferred_element_type=F32
            )
            out = (patches[here, :].astype(F32) + terms).astype(BF16)
            ready = normed(out.astype(F32), merge_gain).astype(F32)
            for g in range(width // 128):
                norm_s[g, here, :] = ready[:, g * 128 : (g + 1) * 128]
            return 0

        lax.fori_loop(0, pieces, merge, 0)
        if h == 0:
            up_load.wait()
        total = jnp.zeros((pieces * share, up.shape[0]), F32)
        for k in range(4):
            quarter = jnp.concatenate(
                [
                    jnp.concatenate(
                        [
                            norm_s[g, pl.ds((2 * v + h) * piece + k, share, stride=4), :]
                            for g in range(width // 128)
                        ],
                        axis=1,
                    )
                    for v in range(pieces)
                ],
                axis=0,
            ).astype(BF16)
            total = total + lax.dot_general(
                quarter,
                up[:, k * width : (k + 1) * width],
                (((1,), (1,)), ((), ())),
                preferred_element_type=F32,
            )
        hidden_all[h, slot] = gelu(total).astype(BF16)
        hidden_gathers.append(EncGather(hidden_all.at[h], (hid_s.at[h], hid_r.at[h])))
        hidden_gathers[h].first(hidden_all.at[h, slot])
        if h == 0:
            kv_a.second(relayed=True)
    text_gathers[1].second()
    down_load.wait()

    one, two = [{}, {}], [[], []]

    def share_rows(index):
        return pl.ds(pl.multiple_of(index * share, share), share)

    def summed(own, others):
        return sum((others[d].astype(F32) for d in range(SIDE - 1)), own.astype(F32))

    ring_ways = (
        (part_a, got_a, both_a, slice(0, half)),
        (part_b, got_b, both_b, slice(half, cols)),
    )
    low, high = slice(0, half // 2), slice(half // 2, half)

    def neighbour(way, d):
        return at_device(z, core, y, ring(x, d)) if way == 0 else at_device(z, core, ring(y, d), x)

    def pass_on(h, way, index, source, d):
        copy = remote(
            source,
            ring_ways[way][1].at[h, index],
            rs_s.at[h, way, index],
            rs_r.at[h, way, index],
            neighbour(way, d),
        )
        copy.start()
        one[h][way, index] = copy

    def terms(h):
        for d in (2, 1, 3, 0):
            xp, yp = ring(x, d), ring(y, d)
            lhs_a = jnp.concatenate(
                [
                    hidden_all[h, 2 * v + xp // 2, share_rows(lax.rem(xp, 2)), :]
                    for v in range(SIDE)
                ],
                axis=0,
            )
            lhs_b = jnp.concatenate(
                [hidden_all[h, 2 * yp + v // 2, share_rows(v % 2), :] for v in range(SIDE)],
                axis=0,
            )
            for way, lhs in enumerate((lhs_a, lhs_b)):
                part, got, both, columns = ring_ways[way]
                part[h, d] = jnp.dot(
                    lhs, down[:, columns], preferred_element_type=F32
                ).astype(BF16)
                if d == 2:
                    pass_on(h, way, 0, part.at[h, d, :, low], 1)
                    pass_on(h, way, 1, part.at[h, d, :, high], 3)
                elif d == 1:
                    pass_on(h, way, 2, part.at[h, d, :, high], 1)
                elif d == 3:
                    pass_on(h, way, 3, part.at[h, d, :, low], 3)

    def combine(h):
        for way in range(2):
            part, got, both, columns = ring_ways[way]
            for index, (d, side) in enumerate(((1, low), (3, high))):
                one[h][way, index].wait_recv()
                both[h, index] = (
                    part[h, d, :, side].astype(F32) + got[h, index].astype(F32)
                ).astype(BF16)
                pass_on(h, way, 4 + index, both.at[h, index], d)

    def ring_total(h, way):
        part, got, both, columns = ring_ways[way]
        for index in range(2, 6):
            one[h][way, index].wait_recv()
        others = jnp.concatenate(
            [
                got[h, 4].astype(F32) + got[h, 3].astype(F32),
                got[h, 2].astype(F32) + got[h, 5].astype(F32),
            ],
            axis=1,
        )
        return (part[h, 0].astype(F32) + others).astype(BF16)

    def ring_sums(h):
        sum_a[h] = ring_total(h, 0)
        sum_b[h] = ring_total(h, 1)
        for d in range(1, SIDE):
            xp, yp = ring(x, d), ring(y, d)
            for way, (total_s, place, got, device) in enumerate(
                (
                    (sum_a, yp, got_a2, at_device(z, core, yp, x)),
                    (sum_b, xp, got_b2, at_device(z, core, y, xp)),
                )
            ):
                copy = remote(
                    total_s.at[h, share_rows(place)],
                    got.at[h, d - 1],
                    rs_s.at[h, 2 + way, d - 1],
                    rs_r.at[h, 2 + way, d - 1],
                    device,
                )
                copy.start()
                two[h].append(copy)

    rows_gathers = [
        EncGather(rows_all.at[h], (row_s.at[h], row_r.at[h])) for h in range(2)
    ]

    def full_sums(h):
        for copy in two[h]:
            copy.wait_recv()
        rows_all[h, slot] = jnp.concatenate(
            [
                summed(sum_a[h, share_rows(y), :], got_a2.at[h]),
                summed(sum_b[h, share_rows(x), :], got_b2.at[h]),
            ],
            axis=1,
        ).astype(BF16)
        rows_gathers[h].first(rows_all.at[h, slot])

    unit_parts = (
        (slice(0, share), slice(0, wide // 2)),
        (slice(0, share), slice(wide // 2, wide)),
    )
    unit_gathers = [
        Gather(
            unit_qkv.at[h],
            unit_own.at[h],
            unit_parts,
            (uq_s.at[h], uq_r.at[h]),
            own_sem=local_sem.at[12 + h],
        )
        for h in range(2)
    ]

    def decode_units(h):
        source = rows_all.at[h]
        decode_some(source, scale_of(source), 0, blocks)
        unit_own[h] = acc_s[0:share, :].astype(BF16)
        unit_gathers[h].first()

    hidden_gathers[0].second()
    hidden_gathers[0].finish()
    terms(0)
    kv_a.relay()
    hidden_gathers[1].second()
    text_scale = text_begin(1, text_b)
    hidden_gathers[1].finish()
    combine(0)
    terms(1)
    text_end(1, text_b, text_scale, kv_own_b)
    kv_b = Gather(
        text_kv.at[1], kv_own_b, halves(tokens), (kvb_s, kvb_r), own_sem=local_sem.at[11]
    )
    ring_sums(0)
    combine(1)
    kv_b.first()
    full_sums(0)
    ring_sums(1)
    rows_gathers[0].second()
    full_sums(1)
    kv_b.second(relayed=True)
    rows_gathers[0].finish()
    decode_units(0)
    rows_gathers[1].second()
    rows_gathers[1].finish()
    unit_gathers[0].second(relayed=True)
    kv_b.relay()
    decode_units(1)
    unit_gathers[0].relay()
    unit_gathers[1].second()
    for gather in unit_gathers + [kv_a, kv_b]:
        gather.finish()
    swap.wait_send()
    for copy in [*one[0].values(), *one[1].values(), *two[0], *two[1]]:
        copy.wait_send()
    for gather in [proj_gather, heads_gather, kv_a, kv_b] + unit_gathers:
        gather.drain()
    for gather in text_gathers + hidden_gathers + rows_gathers:
        gather.drain()


def tower(
    image,
    gain,
    merge_gain,
    dec_gain,
    doc,
    placeholder,
    patches,
    qkv,
    proj,
    up,
    text,
    down,
    wq,
    wk,
    wv,
):
    rows, width = patches.shape
    head = proj.shape[0]
    groups = 8
    units = rows // 4
    cols = text.shape[1]
    tokens = text.shape[0] // 2
    nq, nk = wq.shape[1], wk.shape[1]
    wide = nq + 2 * nk
    own_units = 8 * units // (SIDE * SIDE)
    share = own_units // 2
    half = cols // 2
    dma = pltpu.SemaphoreType.DMA
    whole = pl.BlockSpec(memory_space=VMEM)
    anywhere = pl.BlockSpec(memory_space=pl.ANY)

    def both(shape):
        return [dma(shape), dma(shape)]

    return pl.pallas_call(
        tower_kernel,
        out_shape=(
            jax.ShapeDtypeStruct((2, tokens, nq), BF16),
            jax.ShapeDtypeStruct((2, SIDE, SIDE, tokens, 2 * nk), BF16),
            jax.ShapeDtypeStruct((2, SIDE, SIDE, share, wide), BF16),
            jax.ShapeDtypeStruct((own_units * 16 // 128, 128), jnp.int32),
        ),
        in_specs=[whole] * 6 + [anywhere] * 9,
        out_specs=(whole, anywhere, anywhere, whole),
        scratch_shapes=[
            VMEM((rows, width), BF16),
            VMEM(qkv.shape, BF16),
            VMEM((head, width), BF16),
            VMEM(up.shape, BF16),
            VMEM(down.shape, BF16),
            VMEM((8 * cols, wide), BF16),
            VMEM((rows, head), BF16),
            VMEM((rows, head), BF16),
            VMEM((rows, head), BF16),
            VMEM((rows, head), F32),
            VMEM((rows, width), BF16),
            VMEM((width // 128, rows, 128), F32),
            VMEM((SIDE, SIDE, rows // groups, groups * head), BF16),
            VMEM((SIDE, SIDE, head, width), BF16),
            VMEM((8, tokens, cols), BF16),
            VMEM((8, tokens, cols), BF16),
            VMEM((2, 8, units // 2, up.shape[0]), BF16),
            VMEM((2, SIDE, SIDE * share, half), BF16),
            VMEM((2, SIDE, SIDE * share, half), BF16),
            VMEM((2, 6, SIDE * share, half // 2), BF16),
            VMEM((2, 6, SIDE * share, half // 2), BF16),
            VMEM((2, 2, SIDE * share, half // 2), BF16),
            VMEM((2, 2, SIDE * share, half // 2), BF16),
            VMEM((2, SIDE * share, half), BF16),
            VMEM((2, SIDE * share, half), BF16),
            VMEM((2, SIDE - 1, share, half), BF16),
            VMEM((2, SIDE - 1, share, half), BF16),
            VMEM((2, 8, share, cols), BF16),
            VMEM((tokens, wide), F32),
            VMEM((tokens, 2 * nk), BF16),
            VMEM((tokens, 2 * nk), BF16),
            VMEM((2, share, wide), BF16),
            VMEM(doc.shape, jnp.int32),
            dma((14,)),
            *both((4, 4)),
            *both((4, 4)),
            *both(()),
            *both((10,)),
            *both((10,)),
            *both((2, 7)),
            *both((2, 4, 6)),
            *both((2, 7)),
            *both((4, 4)),
            *both((4, 4)),
            *both((2, 4, 4)),
        ],
        compiler_params=pltpu.CompilerParams(
            collective_id=1, has_side_effects=True, vmem_limit_bytes=60 * 2**20
        ),
        name="tower",
    )(
        image,
        gain,
        merge_gain,
        dec_gain,
        doc,
        placeholder,
        patches,
        qkv,
        proj,
        up,
        text,
        down,
        wq,
        wk,
        wv,
    )


def attention_kernel(
    where_ref,
    doc_smem,
    text_q,
    unit_code,
    doc_rows,
    unit_rows,
    text_kv_hbm,
    unit_qkv_hbm,
    out,
    text_kv,
    unit_qkv,
    load_sem,
    q_s,
    peak_s,
    mix_s,
    bias_s,
):
    tokens, nq = text_q.shape
    nk = text_kv.shape[2] // 2
    unit_loads = []
    for p in range(2):
        share = unit_qkv.shape[1] // 2
        here = slice(p * share, (p + 1) * share)
        unit_loads.append(
            pltpu.make_async_copy(
                unit_qkv_hbm.at[p], unit_qkv.at[:, here, :], load_sem.at[2 + p]
            )
        )
        unit_loads[p].start()
    text_loads = []
    for p in range(2):
        here = slice(p * (tokens // 2), (p + 1) * (tokens // 2))
        text_loads.append(
            pltpu.make_async_copy(text_kv_hbm.at[p], text_kv.at[:, here, :], load_sem.at[p])
        )
        text_loads[p].start()
    heads = nq // HD
    units = unit_qkv.shape[0] * unit_qkv.shape[1]
    mine = where_ref[0]
    first_doc = doc_smem[mine * tokens]
    scale = HD ** (-0.5) * math.log2(math.e)

    lines = tokens // 128
    query_doc = column_of(doc_rows, mine * lines, lines)
    query_unit = column_of(unit_rows, mine * lines, lines)
    query_at = mine * tokens + lax.broadcasted_iota(jnp.int32, (tokens, 128), 0)
    lane = lax.broadcasted_iota(jnp.int32, (tokens, 128), 1)

    picked = jnp.zeros((tokens, nq), F32)
    chunk = 384
    for unit_load in unit_loads:
        unit_load.wait()
    per_chunk = chunk // unit_qkv.shape[1]
    for b in range(units // chunk):
        chosen = jnp.concatenate(
            [
                (query_unit == lane + (b * chunk + g * 128)).astype(F32)
                for g in range(chunk // 128)
            ],
            axis=1,
        ).astype(BF16)
        source = unit_qkv[b * per_chunk : (b + 1) * per_chunk, :, 0:nq].reshape(chunk, nq)
        picked = picked + jnp.dot(chosen, source, preferred_element_type=F32)
    for j in range(heads):
        part = slice(j * HD, (j + 1) * HD)
        q_s[j] = jnp.where(query_unit >= 0, picked[:, part], text_q[:, part].astype(F32)).astype(
            BF16
        )
    peak_s[...] = jnp.full_like(peak_s, NEGATIVE)
    mix_s[...] = jnp.zeros_like(mix_s)
    row_chunk = 128

    def fold(keys, values):
        values = jnp.concatenate([values, jnp.ones_like(values)], axis=1)
        for r in range(0, tokens, row_chunk):
            here = slice(r, r + row_chunk)
            for j in range(heads):
                scores = lax.dot_general(
                    q_s[j, here, :], keys, (((1,), (1,)), ((), ())), preferred_element_type=F32
                )
                scores = scores + bias_s[here, :]
                before = peak_s[j, here, :]
                peak = jnp.maximum(before, jnp.max(scores, axis=1, keepdims=True))
                factor = jnp.exp2((before - peak) * scale)
                wide_peak = jnp.concatenate([peak] * (scores.shape[1] // 128), axis=1)
                weights = jnp.exp2((scores - wide_peak) * scale).astype(BF16)
                peak_s[j, here, :] = peak
                mix_s[j, here, :] = mix_s[j, here, :] * jnp.concatenate(
                    [factor] * 2, axis=1
                ) + jnp.dot(weights, values, preferred_element_type=F32)

    def text_block(i, _):
        blocks = []
        for t in range(2):
            s = begin + 2 * i + t
            held = jnp.minimum(s, text_kv.shape[0] - 1)
            for g in range(lines):
                key_at = s * tokens + g * 128 + lane
                same = query_doc == doc_rows[pl.ds(held * lines + g, 1), :]
                text = unit_rows[pl.ds(held * lines + g, 1), :] < 0
                allowed = same & (key_at <= query_at) & text
                bias_s[:, t * tokens + g * 128 : t * tokens + (g + 1) * 128] = jnp.where(
                    allowed, 0.0, NEGATIVE
                )
            blocks.append(text_kv[held])
        both = jnp.concatenate(blocks, axis=0)
        fold(both[:, 0:nk], both[:, nk:])
        return 0

    begin = jnp.int32(0)
    for s in range(text_kv.shape[0]):
        begin = begin + (doc_smem[(s + 1) * tokens - 1] < first_doc).astype(jnp.int32)
    for text_load in text_loads:
        text_load.wait()
    lax.fori_loop(0, (mine + 2 - begin) // 2, text_block, 0)

    pair = 2 * chunk

    def unit_block(b, _):
        for g in range(pair // 128):
            code = unit_code[pl.ds(b * (pair // 128) + g, 1), :]
            allowed = (query_doc == (code & 63)) & ((code >> 6) <= query_at)
            bias_s[:, g * 128 : (g + 1) * 128] = jnp.where(allowed, 0.0, NEGATIVE)
        block = unit_qkv[pl.ds(b * 2 * per_chunk, 2 * per_chunk), :, nq:].reshape(pair, 2 * nk)
        fold(block[:, 0:nk], block[:, nk:])
        return 0

    lax.fori_loop(0, units // pair, unit_block, 0)
    for j in range(heads):
        out[:, j * HD : (j + 1) * HD] = (mix_s[j, :, 0:HD] / mix_s[j, :, HD:]).astype(BF16)


def attention(where, doc, text_q, text_kv, unit_qkv, unit_code, placeholder):
    tokens, nq = text_q.shape
    heads = nq // HD
    shards = text_kv.shape[1]
    whole = pl.BlockSpec(memory_space=VMEM)
    anywhere = pl.BlockSpec(memory_space=pl.ANY)
    scalars = pl.BlockSpec(memory_space=pltpu.SMEM)
    return pl.pallas_call(
        attention_kernel,
        out_shape=jax.ShapeDtypeStruct((tokens, nq), BF16),
        in_specs=[scalars, scalars] + [whole] * 4 + [anywhere] * 2,
        out_specs=whole,
        scratch_shapes=[
            VMEM((shards, tokens, text_kv.shape[3]), BF16),
            VMEM((shards, 2 * unit_qkv.shape[2], unit_qkv.shape[3]), BF16),
            pltpu.SemaphoreType.DMA((4,)),
            VMEM((heads, tokens, HD), BF16),
            VMEM((heads, tokens, 128), F32),
            VMEM((heads, tokens, 2 * HD), F32),
            VMEM((tokens, 2 * tokens), F32),
        ],
        compiler_params=pltpu.CompilerParams(vmem_limit_bytes=60 * 2**20),
        name="attention",
    )(
        where,
        doc,
        text_q,
        unit_code,
        doc.reshape(-1, 128),
        placeholder.reshape(-1, 128),
        text_kv,
        unit_qkv,
    )


def body(
    patches,
    patch_image,
    vit_gain,
    vit_qkv,
    vit_proj,
    merge_gain,
    merge_up,
    merge_down,
    text_embed,
    placeholder_unit,
    doc_id,
    dec_gain,
    dec_wq,
    dec_wk,
    dec_wv,
):
    tokens = text_embed.shape[0]
    text_q, text_kv, unit_qkv, unit_code = tower(
        patch_image.reshape(-1, 128),
        vit_gain.reshape(-1, 128),
        merge_gain.reshape(-1, 128),
        dec_gain.reshape(-1, 128),
        doc_id.reshape(-1, 128),
        placeholder_unit.reshape(-1, 128),
        patches,
        vit_qkv.transpose(1, 2, 0).reshape(-1, vit_qkv.shape[0]),
        vit_proj,
        merge_up.T,
        text_embed,
        merge_down,
        dec_wq,
        dec_wk,
        dec_wv,
    )
    where = lax.axis_index("ctx").astype(jnp.int32).reshape(1)
    return attention(
        where,
        doc_id,
        text_q.reshape(tokens, -1),
        text_kv.reshape(2, 16, tokens // 2, -1),
        unit_qkv.reshape(2, 16, -1, unit_qkv.shape[-1]),
        unit_code,
        placeholder_unit,
    )


def solution(mesh):
    placed = (
        P("enc", None),
        P("enc"),
        P(),
        P(None, "ctx", None),
        P("ctx", None),
        P(),
        P(None, "ctx"),
        P("ctx", "enc"),
        P("ctx", "enc"),
        P(),
        P(),
        P(),
        P(None, "enc"),
        P(None, "enc"),
        P(None, "enc"),
    )
    return jax.shard_map(
        body, mesh=mesh, in_specs=placed, out_specs=P("ctx", "enc"), check_vma=False
    )
```

```python
import functools
import math

import jax
import jax.numpy as jnp
from jax import lax
from jax.experimental import pallas as pl
from jax.experimental.pallas import tpu as pltpu
from jax.sharding import PartitionSpec as P

MESH = pl.DeviceIdType.MESH
VMEM = pltpu.VMEM
F32 = jnp.float32
BF16 = jnp.bfloat16

HD = 128
QPK = 4
EPSILON = 1e-06
NEGATIVE = -1e30
SIDE = 4


def places():
    e, c = lax.axis_index("enc"), lax.axis_index("ctx")
    return e // 2, lax.rem(e, 2), c // SIDE, lax.rem(c, SIDE)


def at_device(z, core, y, x):
    return {"enc": z * 2 + core, "ctx": y * SIDE + x}


def ring(position, distance):
    return lax.rem(position + distance, SIDE)


def remote(source, target, send_sem, recv_sem, device):
    return pltpu.make_async_remote_copy(
        src_ref=source,
        dst_ref=target,
        send_sem=send_sem,
        recv_sem=recv_sem,
        device_id=device,
        device_id_type=MESH,
    )


def ring_peers():
    z, core, y, x = places()
    peers = []
    for d in range(1, SIDE):
        peers.append(at_device(z, core, y, ring(x, d)))
        peers.append(at_device(z, core, ring(y, d), x))
        peers.append(at_device(ring(z, d), core, y, x))
    peers.append(at_device(z, 1 - core, y, x))
    return peers


def greet():
    for peer in ring_peers():
        pl.semaphore_signal(
            pltpu.get_barrier_semaphore(), inc=1, device_id=peer, device_id_type=MESH
        )


def meet():
    pl.semaphore_wait(pltpu.get_barrier_semaphore(), len(ring_peers()))


def row_of(ref, first, count):
    return jnp.concatenate([ref[pl.ds(first + g, 1), :] for g in range(count)], axis=1)


def column_of(ref, first, count):
    return jnp.concatenate(
        [jnp.broadcast_to(ref[pl.ds(first + g, 1), :], (128, 128)).T for g in range(count)],
        axis=0,
    )


class Gather:
    def __init__(self, buf, own, parts, sems, own_sem=None):
        self.buf, self.own, self.own_sem = buf, own, own_sem
        self.send, self.recv = sems
        self.part_a, self.part_b = parts

    def start(self, phase, pairs, distances):
        z, core, y, x = places()
        copies = {}
        for d in distances:
            for way, (source, target) in enumerate(pairs):
                along_x = way == phase
                device = (
                    at_device(z, core, y, ring(x, d))
                    if along_x
                    else at_device(z, core, ring(y, d), x)
                )
                sem = (2 * phase + way, d - 1)
                copies[way, d] = remote(
                    source, target, self.send.at[sem], self.recv.at[sem], device
                )
        for copy in copies.values():
            copy.start()
        return copies

    def first(self):
        z, core, y, x = places()
        if self.own_sem is not None:
            self.own_copy = pltpu.make_async_copy(self.own, self.buf.at[y, x], self.own_sem)
            self.own_copy.start()
        self.one = self.start(
            0,
            [
                (self.own.at[part], self.buf.at[(y, x) + part])
                for part in (self.part_a, self.part_b)
            ],
            (1, 2, 3),
        )

    def lines(self, row, column, some=slice(None)):
        return (
            self.buf.at[(row, some) + self.part_a],
            self.buf.at[(some, column) + self.part_b],
        )

    def second(self, relayed=False):
        z, core, y, x = places()
        if self.own_sem is not None:
            self.own_copy.wait()
        for copy in self.one.values():
            copy.wait_recv()
        self.relayed = relayed
        self.two = self.start(
            1, [(line, line) for line in self.lines(y, x)], (1, 3) if relayed else (1, 2, 3)
        )
        self.handed = {}

    def relay(self):
        z, core, y, x = places()
        for index, (d, some) in enumerate(((1, slice(0, 2)), (3, slice(2, 4)))):
            for way in range(2):
                self.two[way, d].wait_recv()
                line = self.lines(ring(y, SIDE - d), ring(x, SIDE - d), some)[way]
                device = (
                    at_device(z, core, ring(y, d), x)
                    if way == 0
                    else at_device(z, core, y, ring(x, d))
                )
                sem = (2 + way, 1 + 2 * index)
                self.handed[way, d] = remote(
                    line, line, self.send.at[sem], self.recv.at[sem], device
                )
                self.handed[way, d].start()

    def finish(self):
        for copy in (self.handed if self.relayed else self.two).values():
            copy.wait_recv()

    def drain(self):
        for copies in (self.one, self.two, self.handed):
            for copy in copies.values():
                copy.wait_send()


class EncGather:
    def __init__(self, buf, sems):
        self.buf = buf
        self.send, self.recv = sems

    def first(self, own):
        z, core, y, x = places()
        slot = z * 2 + core
        copies = [
            remote(
                own,
                self.buf.at[slot],
                self.send.at[d - 1],
                self.recv.at[d - 1],
                at_device(ring(z, d), core, y, x),
            )
            for d in range(1, SIDE)
        ]
        copies.append(
            remote(
                own,
                self.buf.at[slot],
                self.send.at[3],
                self.recv.at[3],
                at_device(z, 1 - core, y, x),
            )
        )
        for copy in copies:
            copy.start()
        self.copies = copies

    def second(self):
        z, core, y, x = places()
        self.handed = []
        for d in range(1, SIDE):
            self.copies[d - 1].wait_recv()
            slot = ring(z, SIDE - d) * 2 + core
            copy = remote(
                self.buf.at[slot],
                self.buf.at[slot],
                self.send.at[3 + d],
                self.recv.at[3 + d],
                at_device(z, 1 - core, y, x),
            )
            copy.start()
            self.handed.append(copy)

    def finish(self):
        self.copies[3].wait_recv()
        for copy in self.handed:
            copy.wait_recv()

    def drain(self):
        for copy in self.copies + self.handed:
            copy.wait_send()


class RelayGather:
    def __init__(self, buf, sems):
        self.buf = buf
        self.send, self.recv = sems
        self.copies = {}

    def copy(self, index, source, target, device):
        copy = remote(source, target, self.send.at[index], self.recv.at[index], device)
        copy.start()
        self.copies[index] = copy

    def first(self, own, high):
        z, core, y, x = places()
        middle, rows = self.buf.shape[1] // 2, self.buf.shape[1]
        slot = z * 2 + core
        part = slice(middle, rows) if high else slice(0, middle)
        for index, d in ((8, 1), (9, 3)) if high else ((0, 1), (1, 3)):
            self.copy(
                index,
                own.at[part],
                self.buf.at[slot, part],
                at_device(ring(z, d), core, y, x),
            )
        if not high:
            self.copy(2, own, self.buf.at[slot], at_device(z, 1 - core, y, x))

    def relay(self):
        z, core, y, x = places()
        middle = self.buf.shape[1] // 2
        left, right = ring(z, 3) * 2 + core, ring(z, 1) * 2 + core
        self.copies[0].wait_recv()
        low = self.buf.at[left, 0:middle]
        self.copy(3, low, low, at_device(ring(z, 1), core, y, x))
        self.copies[9].wait_recv()
        high = self.buf.at[right, middle:]
        self.copy(4, high, high, at_device(ring(z, 3), core, y, x))
        self.copies[1].wait_recv()
        self.copies[8].wait_recv()
        for index, block in ((5, left), (6, right)):
            whole = self.buf.at[block]
            self.copy(index, whole, whole, at_device(z, 1 - core, y, x))

    def second(self):
        z, core, y, x = places()
        self.copies[3].wait_recv()
        self.copies[4].wait_recv()
        far = self.buf.at[ring(z, 2) * 2 + core]
        self.copy(7, far, far, at_device(z, 1 - core, y, x))

    def finish(self):
        for index in (2, 5, 6, 7):
            self.copies[index].wait_recv()

    def drain(self):
        for copy in self.copies.values():
            copy.wait_send()


def halves(rows):
    return (slice(0, rows // 2), slice(None)), (slice(rows // 2, rows), slice(None))


def normed(wide, gain):
    center = wide - jnp.mean(wide, axis=1, keepdims=True)
    spread = jnp.mean(center * center, axis=1, keepdims=True)
    return (center * lax.rsqrt(spread + EPSILON) * gain).astype(BF16)


def gelu(x):
    return 0.5 * x * (1.0 + lax.erf(x * math.sqrt(0.5)))


def row_scale(total, count):
    return lax.rsqrt(total / count + EPSILON)


def tower_kernel(
    image,
    gain_rows,
    merge_gain_rows,
    dec_gain,
    doc,
    placeholder,
    patches_hbm,
    qkv_hbm,
    proj_hbm,
    up_hbm,
    text_hbm,
    down_hbm,
    wq_hbm,
    wk_hbm,
    wv_hbm,
    text_q,
    text_kv,
    unit_qkv,
    unit_code,
    patches,
    qkv,
    proj,
    up,
    down,
    w_s,
    q_s,
    k_s,
    v_s,
    o_s,
    lhs_s,
    norm_s,
    heads_all,
    proj_all,
    text_a,
    text_b,
    hidden_all,
    part_a,
    part_b,
    got_a,
    got_b,
    both_a,
    both_b,
    sum_a,
    sum_b,
    got_a2,
    got_b2,
    rows_all,
    acc_s,
    kv_own_a,
    kv_own_b,
    unit_own,
    code_s,
    local_sem,
    proj_s,
    proj_r,
    heads_s,
    heads_r,
    swap_s,
    swap_r,
    text_as,
    text_ar,
    text_bs,
    text_br,
    hid_s,
    hid_r,
    rs_s,
    rs_r,
    row_s,
    row_r,
    kva_s,
    kva_r,
    kvb_s,
    kvb_r,
    uq_s,
    uq_r,
):
    z, core, y, x = places()
    slot = z * 2 + core
    rows, width = patches.shape
    head = proj.shape[0]
    groups = heads_all.shape[3] // head
    group_rows = rows // groups
    side_cols = pl.ds(pl.multiple_of(core * (width // 2), 128), width // 2)
    blocks, tokens, cols = text_a.shape
    model = blocks * cols
    nq, nk = wq_hbm.shape[1], wk_hbm.shape[1]
    wide = nq + 2 * nk
    own_units = 2 * unit_own.shape[1]
    half = cols // 2
    chunk = 256

    def load(index, source, target):
        copy = pltpu.make_async_copy(source, target, local_sem.at[index])
        copy.start()
        return copy

    greet()
    proj_load = load(0, proj_hbm, proj)
    qkv_load = load(2, qkv_hbm, qkv)
    patches_load = load(1, patches_hbm, patches)
    text_loads = [
        load(3, text_hbm.at[0:tokens], text_a.at[slot]),
        load(4, text_hbm.at[tokens:], text_b.at[slot]),
    ]
    w_loads = [
        load(7, wq_hbm, w_s.at[:, 0:nq]),
        load(8, wk_hbm, w_s.at[:, nq : nq + nk]),
        load(9, wv_hbm, w_s.at[:, nq + nk : wide]),
    ]
    up_load = load(5, up_hbm, up)
    down_load = load(6, down_hbm, down)

    proj_load.wait()
    proj_all[y, x, :, side_cols] = proj[:, side_cols]
    meet()
    proj_gather = Gather(
        proj_all,
        proj,
        ((slice(0, 48), side_cols), (slice(48, head), side_cols)),
        (proj_s, proj_r),
    )
    proj_gather.first()
    text_gathers = [
        RelayGather(text_a, (text_as, text_ar)),
        RelayGather(text_b, (text_bs, text_br)),
    ]
    text_gathers[0].first(text_hbm.at[0:tokens], False)
    text_gathers[0].first(text_hbm.at[0:tokens], True)

    gain = row_of(gain_rows, 0, width // 128)
    merge_gain = row_of(merge_gain_rows, 0, width // 128)
    image_row = row_of(image, 0, rows // 128)
    patches_load.wait()
    qkv_load.wait()

    def project(i, _):
        here = pl.ds(pl.multiple_of(i * chunk, chunk), chunk)
        block = normed(patches[here, :].astype(F32), gain)
        packed = lax.dot_general(
            block, qkv[...], (((1,), (1,)), ((), ())), preferred_element_type=F32
        )
        q_s[here, :] = packed[:, 0:head].astype(BF16)
        k_s[here, :] = packed[:, head : 2 * head].astype(BF16)
        v_s[here, :] = packed[:, 2 * head : 3 * head].astype(BF16)
        return 0

    lax.fori_loop(0, rows // chunk, project, 0)

    scaling = head ** (-0.5)

    def attend(i, _):
        here = pl.ds(pl.multiple_of(i * chunk, chunk), chunk)
        ids_col = column_of(image, i * (chunk // 128), chunk // 128)[:, 0:1]
        scores = lax.dot_general(
            q_s[here, :], k_s[...], (((1,), (1,)), ((), ())), preferred_element_type=F32
        )
        scores = jnp.where(ids_col == image_row, scores * scaling, NEGATIVE)
        highest = jnp.max(scores, axis=1, keepdims=True)
        weights = jnp.exp(scores - highest)
        totals = jnp.sum(weights, axis=1, keepdims=True)
        mixture = jnp.dot(weights.astype(BF16), v_s[...], preferred_element_type=F32)
        o_s[here, :] = mixture / totals
        return 0

    lax.fori_loop(0, rows // chunk, attend, 0)
    heads_all[y, x] = jnp.concatenate(
        [o_s[j * group_rows : (j + 1) * group_rows, :] for j in range(groups)], axis=1
    ).astype(BF16)
    heads_gather = Gather(
        heads_all, heads_all.at[y, x], halves(group_rows), (heads_s, heads_r)
    )
    heads_gather.first()

    def scale_of(source):
        squares = jnp.zeros((source.shape[1], 128), F32)
        for b in range(blocks):
            for g in range(cols // 128):
                piece = source[b, :, g * 128 : (g + 1) * 128].astype(F32)
                squares = squares + piece * piece
        return row_scale(jnp.sum(squares, axis=1, keepdims=True), model)

    def decode_some(source, scale, first, last):
        count = source.shape[1]

        def one_block(b, _):
            block = (
                source[b].astype(F32)
                * scale
                * row_of(dec_gain, b * (cols // 128), cols // 128)
            )
            here = pl.ds(pl.multiple_of(b * cols, cols), cols)
            acc_s[0:count, :] += jnp.dot(
                block.astype(BF16), w_s[here, :], preferred_element_type=F32
            )
            return 0

        if first == 0:
            acc_s[0:count, :] = jnp.zeros((count, wide), F32)
        lax.fori_loop(first, last, one_block, 0)

    def text_begin(index, source):
        text_loads[index].wait()
        text_gathers[index].finish()
        scale = scale_of(source)
        decode_some(source, scale, 0, blocks // 2)
        return scale

    def text_end(index, source, scale, kv_own):
        decode_some(source, scale, blocks // 2, blocks)
        text_q[index] = acc_s[:, 0:nq].astype(BF16)
        kv_own[...] = acc_s[:, nq:].astype(BF16)

    lane_unit = lax.broadcasted_iota(jnp.int32, (128, 128), 0)
    position = lax.broadcasted_iota(jnp.int32, doc.shape, 0) * 128 + lax.broadcasted_iota(
        jnp.int32, doc.shape, 1
    )
    code_s[...] = position * 64 + doc[...]

    def units_block(b, _):
        unit = lane_unit + b * 128
        found = jnp.zeros((128, 128), jnp.int32)
        for r in range(placeholder.shape[0]):
            found = found + jnp.where(
                placeholder[r : r + 1, :] == unit, code_s[r : r + 1, :], 0
            )
        unit_code[pl.ds(b, 1), :] = jnp.sum(found.T, axis=0, keepdims=True)
        return 0

    proj_gather.second(relayed=True)
    heads_gather.second(relayed=True)
    text_gathers[0].relay()
    text_gathers[1].first(text_hbm.at[tokens:], False)
    text_gathers[1].first(text_hbm.at[tokens:], True)
    lax.fori_loop(0, unit_code.shape[0] // 2, units_block, 0)
    proj_gather.relay()
    lax.fori_loop(unit_code.shape[0] // 2, unit_code.shape[0], units_block, 0)
    text_gathers[0].second()
    heads_gather.relay()
    for w_load in w_loads:
        w_load.wait()
    text_scale = text_begin(0, text_a)
    proj_gather.finish()
    swap = remote(
        proj_all.at[:, :, :, side_cols],
        proj_all.at[:, :, :, side_cols],
        swap_s,
        swap_r,
        at_device(z, 1 - core, y, x),
    )
    swap.start()
    text_end(0, text_a, text_scale, kv_own_a)
    kv_a = Gather(
        text_kv.at[0], kv_own_a, halves(tokens), (kva_s, kva_r), own_sem=local_sem.at[10]
    )
    kv_a.first()
    heads_gather.finish()
    text_gathers[1].relay()

    for j in range(groups):
        lhs_s[j * group_rows : (j + 1) * group_rows, :] = jnp.concatenate(
            [
                heads_all[a, b, :, j * head : (j + 1) * head].astype(F32)
                for a in range(SIDE)
                for b in range(SIDE)
            ],
            axis=1,
        ).astype(BF16)

    swap.wait_recv()
    share = own_units // 2
    piece = 4 * share
    pieces = rows // piece // 2
    hidden_gathers = []
    for h in range(2):

        def merge(v, _):
            here = pl.ds(pl.multiple_of((2 * v + h) * piece, piece), piece)
            terms = jnp.dot(
                lhs_s[here, :], proj_all[...].reshape(width, width), preferred_element_type=F32
            )
            out = (patches[here, :].astype(F32) + terms).astype(BF16)
            ready = normed(out.astype(F32), merge_gain).astype(F32)
            for g in range(width // 128):
                norm_s[g, here, :] = ready[:, g * 128 : (g + 1) * 128]
            return 0

        lax.fori_loop(0, pieces, merge, 0)
        if h == 0:
            up_load.wait()
        total = jnp.zeros((pieces * share, up.shape[0]), F32)
        for k in range(4):
            quarter = jnp.concatenate(
                [
                    jnp.concatenate(
                        [
                            norm_s[g, pl.ds((2 * v + h) * piece + k, share, stride=4), :]
                            for g in range(width // 128)
                        ],
                        axis=1,
                    )
                    for v in range(pieces)
                ],
                axis=0,
            ).astype(BF16)
            total = total + lax.dot_general(
                quarter,
                up[:, k * width : (k + 1) * width],
                (((1,), (1,)), ((), ())),
                preferred_element_type=F32,
            )
        hidden_all[h, slot] = gelu(total).astype(BF16)
        hidden_gathers.append(EncGather(hidden_all.at[h], (hid_s.at[h], hid_r.at[h])))
        hidden_gathers[h].first(hidden_all.at[h, slot])
        if h == 0:
            kv_a.second(relayed=True)
    text_gathers[1].second()
    down_load.wait()

    one, two = [{}, {}], [[], []]

    def share_rows(index):
        return pl.ds(pl.multiple_of(index * share, share), share)

    def summed(own, others):
        return sum((others[d].astype(F32) for d in range(SIDE - 1)), own.astype(F32))

    ring_ways = (
        (part_a, got_a, both_a, slice(0, half)),
        (part_b, got_b, both_b, slice(half, cols)),
    )
    low, high = slice(0, half // 2), slice(half // 2, half)

    def neighbour(way, d):
        return at_device(z, core, y, ring(x, d)) if way == 0 else at_device(z, core, ring(y, d), x)

    def pass_on(h, way, index, source, d):
        copy = remote(
            source,
            ring_ways[way][1].at[h, index],
            rs_s.at[h, way, index],
            rs_r.at[h, way, index],
            neighbour(way, d),
        )
        copy.start()
        one[h][way, index] = copy

    def terms(h):
        for d in (2, 1, 3, 0):
            xp, yp = ring(x, d), ring(y, d)
            lhs_a = jnp.concatenate(
                [
                    hidden_all[h, 2 * v + xp // 2, share_rows(lax.rem(xp, 2)), :]
                    for v in range(SIDE)
                ],
                axis=0,
            )
            lhs_b = jnp.concatenate(
                [hidden_all[h, 2 * yp + v // 2, share_rows(v % 2), :] for v in range(SIDE)],
                axis=0,
            )
            for way, lhs in enumerate((lhs_a, lhs_b)):
                part, got, both, columns = ring_ways[way]
                part[h, d] = jnp.dot(
                    lhs, down[:, columns], preferred_element_type=F32
                ).astype(BF16)
                if d == 2:
                    pass_on(h, way, 0, part.at[h, d, :, low], 1)
                    pass_on(h, way, 1, part.at[h, d, :, high], 3)
                elif d == 1:
                    pass_on(h, way, 2, part.at[h, d, :, high], 1)
                elif d == 3:
                    pass_on(h, way, 3, part.at[h, d, :, low], 3)

    def combine(h):
        for way in range(2):
            part, got, both, columns = ring_ways[way]
            for index, (d, side) in enumerate(((1, low), (3, high))):
                one[h][way, index].wait_recv()
                both[h, index] = (
                    part[h, d, :, side].astype(F32) + got[h, index].astype(F32)
                ).astype(BF16)
                pass_on(h, way, 4 + index, both.at[h, index], d)

    def ring_total(h, way):
        part, got, both, columns = ring_ways[way]
        for index in range(2, 6):
            one[h][way, index].wait_recv()
        others = jnp.concatenate(
            [
                got[h, 4].astype(F32) + got[h, 3].astype(F32),
                got[h, 2].astype(F32) + got[h, 5].astype(F32),
            ],
            axis=1,
        )
        return (part[h, 0].astype(F32) + others).astype(BF16)

    def ring_sums(h):
        sum_a[h] = ring_total(h, 0)
        sum_b[h] = ring_total(h, 1)
        for d in range(1, SIDE):
            xp, yp = ring(x, d), ring(y, d)
            for way, (total_s, place, got, device) in enumerate(
                (
                    (sum_a, yp, got_a2, at_device(z, core, yp, x)),
                    (sum_b, xp, got_b2, at_device(z, core, y, xp)),
                )
            ):
                copy = remote(
                    total_s.at[h, share_rows(place)],
                    got.at[h, d - 1],
                    rs_s.at[h, 2 + way, d - 1],
                    rs_r.at[h, 2 + way, d - 1],
                    device,
                )
                copy.start()
                two[h].append(copy)

    rows_gathers = [
        EncGather(rows_all.at[h], (row_s.at[h], row_r.at[h])) for h in range(2)
    ]

    def full_sums(h):
        for copy in two[h]:
            copy.wait_recv()
        rows_all[h, slot] = jnp.concatenate(
            [
                summed(sum_a[h, share_rows(y), :], got_a2.at[h]),
                summed(sum_b[h, share_rows(x), :], got_b2.at[h]),
            ],
            axis=1,
        ).astype(BF16)
        rows_gathers[h].first(rows_all.at[h, slot])

    unit_parts = (
        (slice(0, share), slice(0, wide // 2)),
        (slice(0, share), slice(wide // 2, wide)),
    )
    unit_gathers = [
        Gather(
            unit_qkv.at[h],
            unit_own.at[h],
            unit_parts,
            (uq_s.at[h], uq_r.at[h]),
            own_sem=local_sem.at[12 + h],
        )
        for h in range(2)
    ]

    def decode_units(h):
        source = rows_all.at[h]
        decode_some(source, scale_of(source), 0, blocks)
        unit_own[h] = acc_s[0:share, :].astype(BF16)
        unit_gathers[h].first()

    hidden_gathers[0].second()
    hidden_gathers[0].finish()
    terms(0)
    kv_a.relay()
    hidden_gathers[1].second()
    text_scale = text_begin(1, text_b)
    hidden_gathers[1].finish()
    combine(0)
    terms(1)
    text_end(1, text_b, text_scale, kv_own_b)
    kv_b = Gather(
        text_kv.at[1], kv_own_b, halves(tokens), (kvb_s, kvb_r), own_sem=local_sem.at[11]
    )
    ring_sums(0)
    combine(1)
    kv_b.first()
    full_sums(0)
    ring_sums(1)
    rows_gathers[0].second()
    full_sums(1)
    kv_b.second(relayed=True)
    rows_gathers[0].finish()
    decode_units(0)
    rows_gathers[1].second()
    rows_gathers[1].finish()
    unit_gathers[0].second(relayed=True)
    kv_b.relay()
    decode_units(1)
    unit_gathers[0].relay()
    unit_gathers[1].second()
    for gather in unit_gathers + [kv_a, kv_b]:
        gather.finish()
    swap.wait_send()
    for copy in [*one[0].values(), *one[1].values(), *two[0], *two[1]]:
        copy.wait_send()
    for gather in [proj_gather, heads_gather, kv_a, kv_b] + unit_gathers:
        gather.drain()
    for gather in text_gathers + hidden_gathers + rows_gathers:
        gather.drain()


def tower(
    image,
    gain,
    merge_gain,
    dec_gain,
    doc,
    placeholder,
    patches,
    qkv,
    proj,
    up,
    text,
    down,
    wq,
    wk,
    wv,
):
    rows, width = patches.shape
    head = proj.shape[0]
    groups = 8
    units = rows // 4
    cols = text.shape[1]
    tokens = text.shape[0] // 2
    nq, nk = wq.shape[1], wk.shape[1]
    wide = nq + 2 * nk
    own_units = 8 * units // (SIDE * SIDE)
    share = own_units // 2
    half = cols // 2
    dma = pltpu.SemaphoreType.DMA
    whole = pl.BlockSpec(memory_space=VMEM)
    anywhere = pl.BlockSpec(memory_space=pl.ANY)

    def both(shape):
        return [dma(shape), dma(shape)]

    return pl.pallas_call(
        tower_kernel,
        out_shape=(
            jax.ShapeDtypeStruct((2, tokens, nq), BF16),
            jax.ShapeDtypeStruct((2, SIDE, SIDE, tokens, 2 * nk), BF16),
            jax.ShapeDtypeStruct((2, SIDE, SIDE, share, wide), BF16),
            jax.ShapeDtypeStruct((own_units * 16 // 128, 128), jnp.int32),
        ),
        in_specs=[whole] * 6 + [anywhere] * 9,
        out_specs=(whole, anywhere, anywhere, whole),
        scratch_shapes=[
            VMEM((rows, width), BF16),
            VMEM(qkv.shape, BF16),
            VMEM((head, width), BF16),
            VMEM(up.shape, BF16),
            VMEM(down.shape, BF16),
            VMEM((8 * cols, wide), BF16),
            VMEM((rows, head), BF16),
            VMEM((rows, head), BF16),
            VMEM((rows, head), BF16),
            VMEM((rows, head), F32),
            VMEM((rows, width), BF16),
            VMEM((width // 128, rows, 128), F32),
            VMEM((SIDE, SIDE, rows // groups, groups * head), BF16),
            VMEM((SIDE, SIDE, head, width), BF16),
            VMEM((8, tokens, cols), BF16),
            VMEM((8, tokens, cols), BF16),
            VMEM((2, 8, units // 2, up.shape[0]), BF16),
            VMEM((2, SIDE, SIDE * share, half), BF16),
            VMEM((2, SIDE, SIDE * share, half), BF16),
            VMEM((2, 6, SIDE * share, half // 2), BF16),
            VMEM((2, 6, SIDE * share, half // 2), BF16),
            VMEM((2, 2, SIDE * share, half // 2), BF16),
            VMEM((2, 2, SIDE * share, half // 2), BF16),
            VMEM((2, SIDE * share, half), BF16),
            VMEM((2, SIDE * share, half), BF16),
            VMEM((2, SIDE - 1, share, half), BF16),
            VMEM((2, SIDE - 1, share, half), BF16),
            VMEM((2, 8, share, cols), BF16),
            VMEM((tokens, wide), F32),
            VMEM((tokens, 2 * nk), BF16),
            VMEM((tokens, 2 * nk), BF16),
            VMEM((2, share, wide), BF16),
            VMEM(doc.shape, jnp.int32),
            dma((14,)),
            *both((4, 4)),
            *both((4, 4)),
            *both(()),
            *both((10,)),
            *both((10,)),
            *both((2, 7)),
            *both((2, 4, 6)),
            *both((2, 7)),
            *both((4, 4)),
            *both((4, 4)),
            *both((2, 4, 4)),
        ],
        compiler_params=pltpu.CompilerParams(
            collective_id=1, has_side_effects=True, vmem_limit_bytes=60 * 2**20
        ),
        name="tower",
    )(
        image,
        gain,
        merge_gain,
        dec_gain,
        doc,
        placeholder,
        patches,
        qkv,
        proj,
        up,
        text,
        down,
        wq,
        wk,
        wv,
    )


def attention_kernel(
    where_ref,
    doc_hbm,
    text_q_hbm,
    unit_code_hbm,
    doc_rows_hbm,
    unit_rows_hbm,
    text_kv_hbm,
    unit_qkv_hbm,
    out,
    text_kv,
    unit_qkv,
    load_sem,
    q_s,
    peak_s,
    mix_s,
    bias_s,
    text_q,
    doc_smem,
    unit_code,
    doc_rows,
    unit_rows,
):
    tokens, nq = text_q.shape
    nk = text_kv.shape[2] // 2
    small_loads = []
    for index, (source, target) in enumerate(
        (
            (doc_rows_hbm, doc_rows),
            (unit_rows_hbm, unit_rows),
            (text_q_hbm, text_q),
            (unit_code_hbm, unit_code),
            (doc_hbm, doc_smem),
        )
    ):
        small_loads.append(pltpu.make_async_copy(source, target, load_sem.at[4 + index]))
        small_loads[index].start()
    unit_loads = []
    for p in range(2):
        share = unit_qkv.shape[1] // 2
        here = slice(p * share, (p + 1) * share)
        unit_loads.append(
            pltpu.make_async_copy(
                unit_qkv_hbm.at[p], unit_qkv.at[:, here, :], load_sem.at[2 + p]
            )
        )
        unit_loads[p].start()
    text_loads = []
    for p in range(2):
        here = slice(p * (tokens // 2), (p + 1) * (tokens // 2))
        text_loads.append(
            pltpu.make_async_copy(text_kv_hbm.at[p], text_kv.at[:, here, :], load_sem.at[p])
        )
        text_loads[p].start()
    heads = nq // HD
    units = unit_qkv.shape[0] * unit_qkv.shape[1]
    mine = where_ref[0]
    scale = HD ** (-0.5) * math.log2(math.e)

    lines = tokens // 128
    for small_load in small_loads:
        small_load.wait()
    first_doc = doc_smem[mine * tokens]
    query_doc = column_of(doc_rows, mine * lines, lines)
    query_unit = column_of(unit_rows, mine * lines, lines)
    query_at = mine * tokens + lax.broadcasted_iota(jnp.int32, (tokens, 128), 0)
    lane = lax.broadcasted_iota(jnp.int32, (tokens, 128), 1)

    picked = jnp.zeros((tokens, nq), F32)
    chunk = 384
    for unit_load in unit_loads:
        unit_load.wait()
    per_chunk = chunk // unit_qkv.shape[1]
    for b in range(units // chunk):
        chosen = jnp.concatenate(
            [
                (query_unit == lane + (b * chunk + g * 128)).astype(F32)
                for g in range(chunk // 128)
            ],
            axis=1,
        ).astype(BF16)
        source = unit_qkv[b * per_chunk : (b + 1) * per_chunk, :, 0:nq].reshape(chunk, nq)
        picked = picked + jnp.dot(chosen, source, preferred_element_type=F32)
    for j in range(heads):
        part = slice(j * HD, (j + 1) * HD)
        q_s[j] = jnp.where(query_unit >= 0, picked[:, part], text_q[:, part].astype(F32)).astype(
            BF16
        )
    peak_s[...] = jnp.full_like(peak_s, NEGATIVE)
    mix_s[...] = jnp.zeros_like(mix_s)
    row_chunk = 128

    def fold(keys, values):
        values = jnp.concatenate([values, jnp.ones_like(values)], axis=1)
        for r in range(0, tokens, row_chunk):
            here = slice(r, r + row_chunk)
            for j in range(heads):
                scores = lax.dot_general(
                    q_s[j, here, :], keys, (((1,), (1,)), ((), ())), preferred_element_type=F32
                )
                scores = scores + bias_s[here, :]
                before = peak_s[j, here, :]
                peak = jnp.maximum(before, jnp.max(scores, axis=1, keepdims=True))
                factor = jnp.exp2((before - peak) * scale)
                wide_peak = jnp.concatenate([peak] * (scores.shape[1] // 128), axis=1)
                weights = jnp.exp2((scores - wide_peak) * scale).astype(BF16)
                peak_s[j, here, :] = peak
                mix_s[j, here, :] = mix_s[j, here, :] * jnp.concatenate(
                    [factor] * 2, axis=1
                ) + jnp.dot(weights, values, preferred_element_type=F32)

    def text_block(i, _):
        blocks = []
        for t in range(2):
            s = begin + 2 * i + t
            held = jnp.minimum(s, text_kv.shape[0] - 1)
            for g in range(lines):
                key_at = s * tokens + g * 128 + lane
                same = query_doc == doc_rows[pl.ds(held * lines + g, 1), :]
                text = unit_rows[pl.ds(held * lines + g, 1), :] < 0
                allowed = same & (key_at <= query_at) & text
                bias_s[:, t * tokens + g * 128 : t * tokens + (g + 1) * 128] = jnp.where(
                    allowed, 0.0, NEGATIVE
                )
            blocks.append(text_kv[held])
        both = jnp.concatenate(blocks, axis=0)
        fold(both[:, 0:nk], both[:, nk:])
        return 0

    begin = jnp.int32(0)
    for s in range(text_kv.shape[0]):
        begin = begin + (doc_smem[(s + 1) * tokens - 1] < first_doc).astype(jnp.int32)
    for text_load in text_loads:
        text_load.wait()
    lax.fori_loop(0, (mine + 2 - begin) // 2, text_block, 0)

    pair = 2 * chunk

    def unit_block(b, _):
        for g in range(pair // 128):
            code = unit_code[pl.ds(b * (pair // 128) + g, 1), :]
            allowed = (query_doc == (code & 63)) & ((code >> 6) <= query_at)
            bias_s[:, g * 128 : (g + 1) * 128] = jnp.where(allowed, 0.0, NEGATIVE)
        block = unit_qkv[pl.ds(b * 2 * per_chunk, 2 * per_chunk), :, nq:].reshape(pair, 2 * nk)
        fold(block[:, 0:nk], block[:, nk:])
        return 0

    lax.fori_loop(0, units // pair, unit_block, 0)
    for j in range(heads):
        out[:, j * HD : (j + 1) * HD] = (mix_s[j, :, 0:HD] / mix_s[j, :, HD:]).astype(BF16)


def attention(where, doc, text_q, text_kv, unit_qkv, unit_code, placeholder):
    tokens, nq = text_q.shape
    heads = nq // HD
    shards = text_kv.shape[1]
    whole = pl.BlockSpec(memory_space=VMEM)
    anywhere = pl.BlockSpec(memory_space=pl.ANY)
    scalars = pl.BlockSpec(memory_space=pltpu.SMEM)
    return pl.pallas_call(
        attention_kernel,
        out_shape=jax.ShapeDtypeStruct((tokens, nq), BF16),
        in_specs=[scalars] + [anywhere] * 7,
        out_specs=whole,
        scratch_shapes=[
            VMEM((shards, tokens, text_kv.shape[3]), BF16),
            VMEM((shards, 2 * unit_qkv.shape[2], unit_qkv.shape[3]), BF16),
            pltpu.SemaphoreType.DMA((9,)),
            VMEM((heads, tokens, HD), BF16),
            VMEM((heads, tokens, 128), F32),
            VMEM((heads, tokens, 2 * HD), F32),
            VMEM((tokens, 2 * tokens), F32),
            VMEM(text_q.shape, BF16),
            pltpu.SMEM(doc.shape, jnp.int32),
            VMEM(unit_code.shape, jnp.int32),
            VMEM((doc.shape[0] // 128, 128), jnp.int32),
            VMEM((doc.shape[0] // 128, 128), jnp.int32),
        ],
        compiler_params=pltpu.CompilerParams(vmem_limit_bytes=60 * 2**20),
        name="attention",
    )(
        where,
        doc,
        text_q,
        unit_code,
        doc.reshape(-1, 128),
        placeholder.reshape(-1, 128),
        text_kv,
        unit_qkv,
    )


def body(
    patches,
    patch_image,
    vit_gain,
    vit_qkv,
    vit_proj,
    merge_gain,
    merge_up,
    merge_down,
    text_embed,
    placeholder_unit,
    doc_id,
    dec_gain,
    dec_wq,
    dec_wk,
    dec_wv,
):
    tokens = text_embed.shape[0]
    text_q, text_kv, unit_qkv, unit_code = tower(
        patch_image.reshape(-1, 128),
        vit_gain.reshape(-1, 128),
        merge_gain.reshape(-1, 128),
        dec_gain.reshape(-1, 128),
        doc_id.reshape(-1, 128),
        placeholder_unit.reshape(-1, 128),
        patches,
        vit_qkv.transpose(1, 2, 0).reshape(-1, vit_qkv.shape[0]),
        vit_proj,
        merge_up.T,
        text_embed,
        merge_down,
        dec_wq,
        dec_wk,
        dec_wv,
    )
    where = lax.axis_index("ctx").astype(jnp.int32).reshape(1)
    return attention(
        where,
        doc_id,
        text_q.reshape(tokens, -1),
        text_kv.reshape(2, 16, tokens // 2, -1),
        unit_qkv.reshape(2, 16, -1, unit_qkv.shape[-1]),
        unit_code,
        placeholder_unit,
    )


def solution(mesh):
    placed = (
        P("enc", None),
        P("enc"),
        P(),
        P(None, "ctx", None),
        P("ctx", None),
        P(),
        P(None, "ctx"),
        P("ctx", "enc"),
        P("ctx", "enc"),
        P(),
        P(),
        P(),
        P(None, "enc"),
        P(None, "enc"),
        P(None, "enc"),
    )
    return jax.shard_map(
        body, mesh=mesh, in_specs=placed, out_specs=P("ctx", "enc"), check_vma=False
    )
```

```python
import functools
import math

import jax
import jax.numpy as jnp
from jax import lax
from jax.experimental import pallas as pl
from jax.experimental.pallas import tpu as pltpu
from jax.sharding import PartitionSpec as P

MESH = pl.DeviceIdType.MESH
VMEM = pltpu.VMEM
F32 = jnp.float32
BF16 = jnp.bfloat16

HD = 128
QPK = 4
EPSILON = 1e-06
NEGATIVE = -1e30
SIDE = 4


def places():
    e, c = lax.axis_index("enc"), lax.axis_index("ctx")
    return e // 2, lax.rem(e, 2), c // SIDE, lax.rem(c, SIDE)


def at_device(z, core, y, x):
    return {"enc": z * 2 + core, "ctx": y * SIDE + x}


def ring(position, distance):
    return lax.rem(position + distance, SIDE)


def remote(source, target, send_sem, recv_sem, device):
    return pltpu.make_async_remote_copy(
        src_ref=source,
        dst_ref=target,
        send_sem=send_sem,
        recv_sem=recv_sem,
        device_id=device,
        device_id_type=MESH,
    )


def ring_peers():
    z, core, y, x = places()
    peers = []
    for d in range(1, SIDE):
        peers.append(at_device(z, core, y, ring(x, d)))
        peers.append(at_device(z, core, ring(y, d), x))
        peers.append(at_device(ring(z, d), core, y, x))
    peers.append(at_device(z, 1 - core, y, x))
    return peers


def greet():
    for peer in ring_peers():
        pl.semaphore_signal(
            pltpu.get_barrier_semaphore(), inc=1, device_id=peer, device_id_type=MESH
        )


def meet():
    pl.semaphore_wait(pltpu.get_barrier_semaphore(), len(ring_peers()))


def row_of(ref, first, count):
    return jnp.concatenate([ref[pl.ds(first + g, 1), :] for g in range(count)], axis=1)


def column_of(ref, first, count):
    return jnp.concatenate(
        [jnp.broadcast_to(ref[pl.ds(first + g, 1), :], (128, 128)).T for g in range(count)],
        axis=0,
    )


class Gather:
    def __init__(self, buf, own, parts, sems, own_sem=None):
        self.buf, self.own, self.own_sem = buf, own, own_sem
        self.send, self.recv = sems
        self.part_a, self.part_b = parts

    def start(self, phase, pairs, distances):
        z, core, y, x = places()
        copies = {}
        for d in distances:
            for way, (source, target) in enumerate(pairs):
                along_x = way == phase
                device = (
                    at_device(z, core, y, ring(x, d))
                    if along_x
                    else at_device(z, core, ring(y, d), x)
                )
                sem = (2 * phase + way, d - 1)
                copies[way, d] = remote(
                    source, target, self.send.at[sem], self.recv.at[sem], device
                )
        for copy in copies.values():
            copy.start()
        return copies

    def first(self):
        z, core, y, x = places()
        if self.own_sem is not None:
            self.own_copy = pltpu.make_async_copy(self.own, self.buf.at[y, x], self.own_sem)
            self.own_copy.start()
        self.one = self.start(
            0,
            [
                (self.own.at[part], self.buf.at[(y, x) + part])
                for part in (self.part_a, self.part_b)
            ],
            (1, 2, 3),
        )

    def lines(self, row, column, some=slice(None)):
        return (
            self.buf.at[(row, some) + self.part_a],
            self.buf.at[(some, column) + self.part_b],
        )

    def second(self, relayed=False):
        z, core, y, x = places()
        if self.own_sem is not None:
            self.own_copy.wait()
        for copy in self.one.values():
            copy.wait_recv()
        self.relayed = relayed
        self.two = self.start(
            1, [(line, line) for line in self.lines(y, x)], (1, 3) if relayed else (1, 2, 3)
        )
        self.handed = {}

    def relay(self):
        z, core, y, x = places()
        for index, (d, some) in enumerate(((1, slice(0, 2)), (3, slice(2, 4)))):
            for way in range(2):
                self.two[way, d].wait_recv()
                line = self.lines(ring(y, SIDE - d), ring(x, SIDE - d), some)[way]
                device = (
                    at_device(z, core, ring(y, d), x)
                    if way == 0
                    else at_device(z, core, y, ring(x, d))
                )
                sem = (2 + way, 1 + 2 * index)
                self.handed[way, d] = remote(
                    line, line, self.send.at[sem], self.recv.at[sem], device
                )
                self.handed[way, d].start()

    def finish(self):
        for copy in (self.handed if self.relayed else self.two).values():
            copy.wait_recv()

    def drain(self):
        for copies in (self.one, self.two, self.handed):
            for copy in copies.values():
                copy.wait_send()


class EncGather:
    def __init__(self, buf, sems):
        self.buf = buf
        self.send, self.recv = sems

    def first(self, own):
        z, core, y, x = places()
        slot = z * 2 + core
        copies = [
            remote(
                own,
                self.buf.at[slot],
                self.send.at[d - 1],
                self.recv.at[d - 1],
                at_device(ring(z, d), core, y, x),
            )
            for d in range(1, SIDE)
        ]
        copies.append(
            remote(
                own,
                self.buf.at[slot],
                self.send.at[3],
                self.recv.at[3],
                at_device(z, 1 - core, y, x),
            )
        )
        for copy in copies:
            copy.start()
        self.copies = copies

    def second(self):
        z, core, y, x = places()
        self.handed = []
        for d in range(1, SIDE):
            self.copies[d - 1].wait_recv()
            slot = ring(z, SIDE - d) * 2 + core
            copy = remote(
                self.buf.at[slot],
                self.buf.at[slot],
                self.send.at[3 + d],
                self.recv.at[3 + d],
                at_device(z, 1 - core, y, x),
            )
            copy.start()
            self.handed.append(copy)

    def finish(self):
        self.copies[3].wait_recv()
        for copy in self.handed:
            copy.wait_recv()

    def drain(self):
        for copy in self.copies + self.handed:
            copy.wait_send()


class RelayGather:
    def __init__(self, buf, sems):
        self.buf = buf
        self.send, self.recv = sems
        self.copies = {}

    def copy(self, index, source, target, device):
        copy = remote(source, target, self.send.at[index], self.recv.at[index], device)
        copy.start()
        self.copies[index] = copy

    def first(self, own, high):
        z, core, y, x = places()
        middle, rows = self.buf.shape[1] // 2, self.buf.shape[1]
        slot = z * 2 + core
        part = slice(middle, rows) if high else slice(0, middle)
        for index, d in ((8, 1), (9, 3)) if high else ((0, 1), (1, 3)):
            self.copy(
                index,
                own.at[part],
                self.buf.at[slot, part],
                at_device(ring(z, d), core, y, x),
            )
        if not high:
            self.copy(2, own, self.buf.at[slot], at_device(z, 1 - core, y, x))

    def relay(self):
        z, core, y, x = places()
        middle = self.buf.shape[1] // 2
        left, right = ring(z, 3) * 2 + core, ring(z, 1) * 2 + core
        self.copies[0].wait_recv()
        low = self.buf.at[left, 0:middle]
        self.copy(3, low, low, at_device(ring(z, 1), core, y, x))
        self.copies[9].wait_recv()
        high = self.buf.at[right, middle:]
        self.copy(4, high, high, at_device(ring(z, 3), core, y, x))
        self.copies[1].wait_recv()
        self.copies[8].wait_recv()
        for index, block in ((5, left), (6, right)):
            whole = self.buf.at[block]
            self.copy(index, whole, whole, at_device(z, 1 - core, y, x))

    def second(self):
        z, core, y, x = places()
        self.copies[3].wait_recv()
        self.copies[4].wait_recv()
        far = self.buf.at[ring(z, 2) * 2 + core]
        self.copy(7, far, far, at_device(z, 1 - core, y, x))

    def finish(self):
        for index in (2, 5, 6, 7):
            self.copies[index].wait_recv()

    def drain(self):
        for copy in self.copies.values():
            copy.wait_send()


def halves(rows):
    return (slice(0, rows // 2), slice(None)), (slice(rows // 2, rows), slice(None))


def normed(wide, gain):
    center = wide - jnp.mean(wide, axis=1, keepdims=True)
    spread = jnp.mean(center * center, axis=1, keepdims=True)
    return (center * lax.rsqrt(spread + EPSILON) * gain).astype(BF16)


def gelu(x):
    return 0.5 * x * (1.0 + lax.erf(x * math.sqrt(0.5)))


def row_scale(total, count):
    return lax.rsqrt(total / count + EPSILON)


def tower_kernel(
    image,
    gain_rows,
    merge_gain_rows,
    dec_gain,
    doc,
    placeholder,
    patches_hbm,
    qkv_hbm,
    proj_hbm,
    up_hbm,
    text_hbm,
    down_hbm,
    wq_hbm,
    wk_hbm,
    wv_hbm,
    text_q,
    text_kv,
    unit_qkv,
    unit_code,
    patches,
    qkv,
    proj,
    up,
    down,
    w_s,
    q_s,
    k_s,
    v_s,
    o_s,
    lhs_s,
    norm_s,
    heads_all,
    proj_all,
    text_a,
    text_b,
    hidden_all,
    part_a,
    part_b,
    got_a,
    got_b,
    both_a,
    both_b,
    sum_a,
    sum_b,
    got_a2,
    got_b2,
    rows_all,
    acc_s,
    kv_own_a,
    kv_own_b,
    unit_own,
    code_s,
    local_sem,
    proj_s,
    proj_r,
    heads_s,
    heads_r,
    swap_s,
    swap_r,
    text_as,
    text_ar,
    text_bs,
    text_br,
    hid_s,
    hid_r,
    rs_s,
    rs_r,
    row_s,
    row_r,
    kva_s,
    kva_r,
    kvb_s,
    kvb_r,
    uq_s,
    uq_r,
):
    z, core, y, x = places()
    slot = z * 2 + core
    rows, width = patches.shape
    head = proj.shape[0]
    groups = heads_all.shape[3] // head
    group_rows = rows // groups
    side_cols = pl.ds(pl.multiple_of(core * (width // 2), 128), width // 2)
    blocks, tokens, cols = text_a.shape
    model = blocks * cols
    nq, nk = wq_hbm.shape[1], wk_hbm.shape[1]
    wide = nq + 2 * nk
    own_units = 2 * unit_own.shape[1]
    half = cols // 2
    chunk = 256

    def load(index, source, target):
        copy = pltpu.make_async_copy(source, target, local_sem.at[index])
        copy.start()
        return copy

    greet()
    proj_load = load(0, proj_hbm, proj)
    qkv_load = load(2, qkv_hbm, qkv)
    patches_load = load(1, patches_hbm, patches)
    text_loads = [
        load(3, text_hbm.at[0:tokens], text_a.at[slot]),
        load(4, text_hbm.at[tokens:], text_b.at[slot]),
    ]
    w_loads = [
        load(7, wq_hbm, w_s.at[:, 0:nq]),
        load(8, wk_hbm, w_s.at[:, nq : nq + nk]),
        load(9, wv_hbm, w_s.at[:, nq + nk : wide]),
    ]
    up_load = load(5, up_hbm, up)
    down_load = load(6, down_hbm, down)

    proj_load.wait()
    proj_all[y, x, :, side_cols] = proj[:, side_cols]
    meet()
    proj_gather = Gather(
        proj_all,
        proj,
        ((slice(0, 48), side_cols), (slice(48, head), side_cols)),
        (proj_s, proj_r),
    )
    proj_gather.first()
    text_gathers = [
        RelayGather(text_a, (text_as, text_ar)),
        RelayGather(text_b, (text_bs, text_br)),
    ]
    text_gathers[0].first(text_hbm.at[0:tokens], False)
    text_gathers[0].first(text_hbm.at[0:tokens], True)

    gain = row_of(gain_rows, 0, width // 128)
    merge_gain = row_of(merge_gain_rows, 0, width // 128)
    image_row = row_of(image, 0, rows // 128)
    patches_load.wait()
    qkv_load.wait()

    def project(i, _):
        here = pl.ds(pl.multiple_of(i * chunk, chunk), chunk)
        block = normed(patches[here, :].astype(F32), gain)
        packed = lax.dot_general(
            block, qkv[...], (((1,), (1,)), ((), ())), preferred_element_type=F32
        )
        q_s[here, :] = packed[:, 0:head].astype(BF16)
        k_s[here, :] = packed[:, head : 2 * head].astype(BF16)
        v_s[here, :] = packed[:, 2 * head : 3 * head].astype(BF16)
        return 0

    lax.fori_loop(0, rows // chunk, project, 0)

    scaling = head ** (-0.5)

    def attend(i, _):
        here = pl.ds(pl.multiple_of(i * chunk, chunk), chunk)
        ids_col = column_of(image, i * (chunk // 128), chunk // 128)[:, 0:1]
        scores = lax.dot_general(
            q_s[here, :], k_s[...], (((1,), (1,)), ((), ())), preferred_element_type=F32
        )
        scores = jnp.where(ids_col == image_row, scores * scaling, NEGATIVE)
        highest = jnp.max(scores, axis=1, keepdims=True)
        weights = jnp.exp(scores - highest)
        totals = jnp.sum(weights, axis=1, keepdims=True)
        mixture = jnp.dot(weights.astype(BF16), v_s[...], preferred_element_type=F32)
        o_s[here, :] = mixture / totals
        return 0

    lax.fori_loop(0, rows // chunk, attend, 0)
    heads_all[y, x] = jnp.concatenate(
        [o_s[j * group_rows : (j + 1) * group_rows, :] for j in range(groups)], axis=1
    ).astype(BF16)
    heads_gather = Gather(
        heads_all, heads_all.at[y, x], halves(group_rows), (heads_s, heads_r)
    )
    heads_gather.first()

    def scale_of(source):
        squares = jnp.zeros((source.shape[1], 128), F32)
        for b in range(blocks):
            for g in range(cols // 128):
                piece = source[b, :, g * 128 : (g + 1) * 128].astype(F32)
                squares = squares + piece * piece
        return row_scale(jnp.sum(squares, axis=1, keepdims=True), model)

    def decode_some(source, scale, first, last):
        count = source.shape[1]

        def one_block(b, _):
            block = (
                source[b].astype(F32)
                * scale
                * row_of(dec_gain, b * (cols // 128), cols // 128)
            )
            here = pl.ds(pl.multiple_of(b * cols, cols), cols)
            acc_s[0:count, :] += jnp.dot(
                block.astype(BF16), w_s[here, :], preferred_element_type=F32
            )
            return 0

        if first == 0:
            acc_s[0:count, :] = jnp.zeros((count, wide), F32)
        lax.fori_loop(first, last, one_block, 0)

    def text_begin(index, source):
        text_loads[index].wait()
        text_gathers[index].finish()
        scale = scale_of(source)
        decode_some(source, scale, 0, blocks // 2)
        return scale

    def text_end(index, source, scale, kv_own):
        decode_some(source, scale, blocks // 2, blocks)
        text_q[index] = acc_s[:, 0:nq].astype(BF16)
        kv_own[...] = acc_s[:, nq:].astype(BF16)

    lane_unit = lax.broadcasted_iota(jnp.int32, (128, 128), 0)
    position = lax.broadcasted_iota(jnp.int32, doc.shape, 0) * 128 + lax.broadcasted_iota(
        jnp.int32, doc.shape, 1
    )
    code_s[...] = position * 64 + doc[...]

    def units_block(b, _):
        unit = lane_unit + b * 128
        found = jnp.zeros((128, 128), jnp.int32)
        for r in range(placeholder.shape[0]):
            found = found + jnp.where(
                placeholder[r : r + 1, :] == unit, code_s[r : r + 1, :], 0
            )
        unit_code[pl.ds(b, 1), :] = jnp.sum(found.T, axis=0, keepdims=True)
        return 0

    proj_gather.second(relayed=True)
    heads_gather.second(relayed=True)
    text_gathers[0].relay()
    text_gathers[1].first(text_hbm.at[tokens:], False)
    text_gathers[1].first(text_hbm.at[tokens:], True)
    lax.fori_loop(0, unit_code.shape[0] // 2, units_block, 0)
    proj_gather.relay()
    lax.fori_loop(unit_code.shape[0] // 2, unit_code.shape[0], units_block, 0)
    text_gathers[0].second()
    heads_gather.relay()
    for w_load in w_loads:
        w_load.wait()
    text_scale = text_begin(0, text_a)
    proj_gather.finish()
    swap = remote(
        proj_all.at[:, :, :, side_cols],
        proj_all.at[:, :, :, side_cols],
        swap_s,
        swap_r,
        at_device(z, 1 - core, y, x),
    )
    swap.start()
    text_end(0, text_a, text_scale, kv_own_a)
    kv_a = Gather(
        text_kv.at[0], kv_own_a, halves(tokens), (kva_s, kva_r), own_sem=local_sem.at[10]
    )
    kv_a.first()
    heads_gather.finish()
    text_gathers[1].relay()

    for j in range(groups):
        lhs_s[j * group_rows : (j + 1) * group_rows, :] = jnp.concatenate(
            [
                heads_all[a, b, :, j * head : (j + 1) * head].astype(F32)
                for a in range(SIDE)
                for b in range(SIDE)
            ],
            axis=1,
        ).astype(BF16)

    swap.wait_recv()
    share = own_units // 2
    piece = 4 * share
    pieces = rows // piece // 2
    hidden_gathers = []
    for h in range(2):

        def merge(v, _):
            here = pl.ds(pl.multiple_of((2 * v + h) * piece, piece), piece)
            terms = jnp.dot(
                lhs_s[here, :], proj_all[...].reshape(width, width), preferred_element_type=F32
            )
            out = (patches[here, :].astype(F32) + terms).astype(BF16)
            ready = normed(out.astype(F32), merge_gain).astype(F32)
            for g in range(width // 128):
                norm_s[g, here, :] = ready[:, g * 128 : (g + 1) * 128]
            return 0

        lax.fori_loop(0, pieces, merge, 0)
        if h == 0:
            up_load.wait()
        total = jnp.zeros((pieces * share, up.shape[0]), F32)
        for k in range(4):
            quarter = jnp.concatenate(
                [
                    jnp.concatenate(
                        [
                            norm_s[g, pl.ds((2 * v + h) * piece + k, share, stride=4), :]
                            for g in range(width // 128)
                        ],
                        axis=1,
                    )
                    for v in range(pieces)
                ],
                axis=0,
            ).astype(BF16)
            total = total + lax.dot_general(
                quarter,
                up[:, k * width : (k + 1) * width],
                (((1,), (1,)), ((), ())),
                preferred_element_type=F32,
            )
        hidden_all[h, slot] = gelu(total).astype(BF16)
        hidden_gathers.append(EncGather(hidden_all.at[h], (hid_s.at[h], hid_r.at[h])))
        hidden_gathers[h].first(hidden_all.at[h, slot])
        if h == 0:
            kv_a.second(relayed=True)
    text_gathers[1].second()
    down_load.wait()

    one, two = [{}, {}], [[], []]

    def share_rows(index):
        return pl.ds(pl.multiple_of(index * share, share), share)

    def summed(own, others):
        return sum((others[d].astype(F32) for d in range(SIDE - 1)), own.astype(F32))

    ring_ways = (
        (part_a, got_a, both_a, slice(0, half)),
        (part_b, got_b, both_b, slice(half, cols)),
    )
    low, high = slice(0, half // 2), slice(half // 2, half)

    def neighbour(way, d):
        return at_device(z, core, y, ring(x, d)) if way == 0 else at_device(z, core, ring(y, d), x)

    def pass_on(h, way, index, source, d):
        copy = remote(
            source,
            ring_ways[way][1].at[h, index],
            rs_s.at[h, way, index],
            rs_r.at[h, way, index],
            neighbour(way, d),
        )
        copy.start()
        one[h][way, index] = copy

    def terms(h):
        for d in (2, 1, 3, 0):
            xp, yp = ring(x, d), ring(y, d)
            lhs_a = jnp.concatenate(
                [
                    hidden_all[h, 2 * v + xp // 2, share_rows(lax.rem(xp, 2)), :]
                    for v in range(SIDE)
                ],
                axis=0,
            )
            lhs_b = jnp.concatenate(
                [hidden_all[h, 2 * yp + v // 2, share_rows(v % 2), :] for v in range(SIDE)],
                axis=0,
            )
            for way, lhs in enumerate((lhs_a, lhs_b)):
                part, got, both, columns = ring_ways[way]
                part[h, d] = jnp.dot(
                    lhs, down[:, columns], preferred_element_type=F32
                ).astype(BF16)
                if d == 2:
                    pass_on(h, way, 0, part.at[h, d, :, low], 1)
                    pass_on(h, way, 1, part.at[h, d, :, high], 3)
                elif d == 1:
                    pass_on(h, way, 2, part.at[h, d, :, high], 1)
                elif d == 3:
                    pass_on(h, way, 3, part.at[h, d, :, low], 3)

    def combine(h):
        for way in range(2):
            part, got, both, columns = ring_ways[way]
            for index, (d, side) in enumerate(((1, low), (3, high))):
                one[h][way, index].wait_recv()
                both[h, index] = (
                    part[h, d, :, side].astype(F32) + got[h, index].astype(F32)
                ).astype(BF16)
                pass_on(h, way, 4 + index, both.at[h, index], d)

    def ring_total(h, way):
        part, got, both, columns = ring_ways[way]
        for index in range(2, 6):
            one[h][way, index].wait_recv()
        others = jnp.concatenate(
            [
                got[h, 4].astype(F32) + got[h, 3].astype(F32),
                got[h, 2].astype(F32) + got[h, 5].astype(F32),
            ],
            axis=1,
        )
        return (part[h, 0].astype(F32) + others).astype(BF16)

    def ring_sums(h):
        sum_a[h] = ring_total(h, 0)
        sum_b[h] = ring_total(h, 1)
        for d in range(1, SIDE):
            xp, yp = ring(x, d), ring(y, d)
            for way, (total_s, place, got, device) in enumerate(
                (
                    (sum_a, yp, got_a2, at_device(z, core, yp, x)),
                    (sum_b, xp, got_b2, at_device(z, core, y, xp)),
                )
            ):
                copy = remote(
                    total_s.at[h, share_rows(place)],
                    got.at[h, d - 1],
                    rs_s.at[h, 2 + way, d - 1],
                    rs_r.at[h, 2 + way, d - 1],
                    device,
                )
                copy.start()
                two[h].append(copy)

    rows_gathers = [
        EncGather(rows_all.at[h], (row_s.at[h], row_r.at[h])) for h in range(2)
    ]

    def full_sums(h):
        for copy in two[h]:
            copy.wait_recv()
        rows_all[h, slot] = jnp.concatenate(
            [
                summed(sum_a[h, share_rows(y), :], got_a2.at[h]),
                summed(sum_b[h, share_rows(x), :], got_b2.at[h]),
            ],
            axis=1,
        ).astype(BF16)
        rows_gathers[h].first(rows_all.at[h, slot])

    unit_parts = (
        (slice(0, share), slice(0, wide // 2)),
        (slice(0, share), slice(wide // 2, wide)),
    )
    unit_gathers = [
        Gather(
            unit_qkv.at[h],
            unit_own.at[h],
            unit_parts,
            (uq_s.at[h], uq_r.at[h]),
            own_sem=local_sem.at[12 + h],
        )
        for h in range(2)
    ]

    def add_block(b):
        block = rows_all[1, b].astype(F32) * row_of(dec_gain, b * (cols // 128), cols // 128)
        here = pl.ds(pl.multiple_of(b * cols, cols), cols)
        acc_s[0:share, :] += jnp.dot(
            block.astype(BF16), w_s[here, :], preferred_element_type=F32
        )

    def add_blocks(first, side):
        def one(d, _):
            add_block(ring(z, d) * 2 + side)
            return 0

        lax.fori_loop(first, SIDE, one, 0)

    def decode_units(h):
        source = rows_all.at[h]
        decode_some(source, scale_of(source), 0, blocks)
        unit_own[h] = acc_s[0:share, :].astype(BF16)
        unit_gathers[h].first()

    hidden_gathers[0].second()
    hidden_gathers[0].finish()
    terms(0)
    kv_a.relay()
    hidden_gathers[1].second()
    text_scale = text_begin(1, text_b)
    hidden_gathers[1].finish()
    combine(0)
    terms(1)
    text_end(1, text_b, text_scale, kv_own_b)
    kv_b = Gather(
        text_kv.at[1], kv_own_b, halves(tokens), (kvb_s, kvb_r), own_sem=local_sem.at[11]
    )
    ring_sums(0)
    combine(1)
    kv_b.first()
    full_sums(0)
    ring_sums(1)
    rows_gathers[0].second()
    full_sums(1)
    kv_b.second(relayed=True)
    rows_gathers[0].finish()
    decode_units(0)
    acc_s[0:share, :] = jnp.zeros((share, wide), F32)
    add_block(slot)
    rows_gathers[1].second()
    add_blocks(1, core)
    rows_gathers[1].finish()
    unit_gathers[0].second(relayed=True)
    kv_b.relay()
    add_blocks(0, 1 - core)
    unit_own[1] = (acc_s[0:share, :] * scale_of(rows_all.at[1])).astype(BF16)
    unit_gathers[1].first()
    unit_gathers[0].relay()
    unit_gathers[1].second()
    for gather in unit_gathers + [kv_a, kv_b]:
        gather.finish()
    swap.wait_send()
    for copy in [*one[0].values(), *one[1].values(), *two[0], *two[1]]:
        copy.wait_send()
    for gather in [proj_gather, heads_gather, kv_a, kv_b] + unit_gathers:
        gather.drain()
    for gather in text_gathers + hidden_gathers + rows_gathers:
        gather.drain()


def tower(
    image,
    gain,
    merge_gain,
    dec_gain,
    doc,
    placeholder,
    patches,
    qkv,
    proj,
    up,
    text,
    down,
    wq,
    wk,
    wv,
):
    rows, width = patches.shape
    head = proj.shape[0]
    groups = 8
    units = rows // 4
    cols = text.shape[1]
    tokens = text.shape[0] // 2
    nq, nk = wq.shape[1], wk.shape[1]
    wide = nq + 2 * nk
    own_units = 8 * units // (SIDE * SIDE)
    share = own_units // 2
    half = cols // 2
    dma = pltpu.SemaphoreType.DMA
    whole = pl.BlockSpec(memory_space=VMEM)
    anywhere = pl.BlockSpec(memory_space=pl.ANY)

    def both(shape):
        return [dma(shape), dma(shape)]

    return pl.pallas_call(
        tower_kernel,
        out_shape=(
            jax.ShapeDtypeStruct((2, tokens, nq), BF16),
            jax.ShapeDtypeStruct((2, SIDE, SIDE, tokens, 2 * nk), BF16),
            jax.ShapeDtypeStruct((2, SIDE, SIDE, share, wide), BF16),
            jax.ShapeDtypeStruct((own_units * 16 // 128, 128), jnp.int32),
        ),
        in_specs=[whole] * 6 + [anywhere] * 9,
        out_specs=(whole, anywhere, anywhere, whole),
        scratch_shapes=[
            VMEM((rows, width), BF16),
            VMEM(qkv.shape, BF16),
            VMEM((head, width), BF16),
            VMEM(up.shape, BF16),
            VMEM(down.shape, BF16),
            VMEM((8 * cols, wide), BF16),
            VMEM((rows, head), BF16),
            VMEM((rows, head), BF16),
            VMEM((rows, head), BF16),
            VMEM((rows, head), F32),
            VMEM((rows, width), BF16),
            VMEM((width // 128, rows, 128), F32),
            VMEM((SIDE, SIDE, rows // groups, groups * head), BF16),
            VMEM((SIDE, SIDE, head, width), BF16),
            VMEM((8, tokens, cols), BF16),
            VMEM((8, tokens, cols), BF16),
            VMEM((2, 8, units // 2, up.shape[0]), BF16),
            VMEM((2, SIDE, SIDE * share, half), BF16),
            VMEM((2, SIDE, SIDE * share, half), BF16),
            VMEM((2, 6, SIDE * share, half // 2), BF16),
            VMEM((2, 6, SIDE * share, half // 2), BF16),
            VMEM((2, 2, SIDE * share, half // 2), BF16),
            VMEM((2, 2, SIDE * share, half // 2), BF16),
            VMEM((2, SIDE * share, half), BF16),
            VMEM((2, SIDE * share, half), BF16),
            VMEM((2, SIDE - 1, share, half), BF16),
            VMEM((2, SIDE - 1, share, half), BF16),
            VMEM((2, 8, share, cols), BF16),
            VMEM((tokens, wide), F32),
            VMEM((tokens, 2 * nk), BF16),
            VMEM((tokens, 2 * nk), BF16),
            VMEM((2, share, wide), BF16),
            VMEM(doc.shape, jnp.int32),
            dma((14,)),
            *both((4, 4)),
            *both((4, 4)),
            *both(()),
            *both((10,)),
            *both((10,)),
            *both((2, 7)),
            *both((2, 4, 6)),
            *both((2, 7)),
            *both((4, 4)),
            *both((4, 4)),
            *both((2, 4, 4)),
        ],
        compiler_params=pltpu.CompilerParams(
            collective_id=1, has_side_effects=True, vmem_limit_bytes=60 * 2**20
        ),
        name="tower",
    )(
        image,
        gain,
        merge_gain,
        dec_gain,
        doc,
        placeholder,
        patches,
        qkv,
        proj,
        up,
        text,
        down,
        wq,
        wk,
        wv,
    )


def attention_kernel(
    where_ref,
    doc_hbm,
    text_q_hbm,
    unit_code_hbm,
    doc_rows_hbm,
    unit_rows_hbm,
    text_kv_hbm,
    unit_qkv_hbm,
    out,
    text_kv,
    unit_qkv,
    load_sem,
    q_s,
    peak_s,
    mix_s,
    bias_s,
    text_q,
    doc_smem,
    unit_code,
    doc_rows,
    unit_rows,
):
    tokens, nq = text_q.shape
    nk = text_kv.shape[2] // 2
    small_loads = []
    for index, (source, target) in enumerate(
        (
            (doc_rows_hbm, doc_rows),
            (unit_rows_hbm, unit_rows),
            (text_q_hbm, text_q),
            (unit_code_hbm, unit_code),
            (doc_hbm, doc_smem),
        )
    ):
        small_loads.append(pltpu.make_async_copy(source, target, load_sem.at[4 + index]))
        small_loads[index].start()
    unit_loads = []
    for p in range(2):
        share = unit_qkv.shape[1] // 2
        here = slice(p * share, (p + 1) * share)
        unit_loads.append(
            pltpu.make_async_copy(
                unit_qkv_hbm.at[p], unit_qkv.at[:, here, :], load_sem.at[2 + p]
            )
        )
        unit_loads[p].start()
    text_loads = []
    for p in range(2):
        here = slice(p * (tokens // 2), (p + 1) * (tokens // 2))
        text_loads.append(
            pltpu.make_async_copy(text_kv_hbm.at[p], text_kv.at[:, here, :], load_sem.at[p])
        )
        text_loads[p].start()
    heads = nq // HD
    units = unit_qkv.shape[0] * unit_qkv.shape[1]
    mine = where_ref[0]
    scale = HD ** (-0.5) * math.log2(math.e)

    lines = tokens // 128
    for small_load in small_loads:
        small_load.wait()
    first_doc = doc_smem[mine * tokens]
    query_doc = column_of(doc_rows, mine * lines, lines)
    query_unit = column_of(unit_rows, mine * lines, lines)
    query_at = mine * tokens + lax.broadcasted_iota(jnp.int32, (tokens, 128), 0)
    lane = lax.broadcasted_iota(jnp.int32, (tokens, 128), 1)

    picked = jnp.zeros((tokens, nq), F32)
    chunk = 384
    for unit_load in unit_loads:
        unit_load.wait()
    per_chunk = chunk // unit_qkv.shape[1]
    for b in range(units // chunk):
        chosen = jnp.concatenate(
            [
                (query_unit == lane + (b * chunk + g * 128)).astype(F32)
                for g in range(chunk // 128)
            ],
            axis=1,
        ).astype(BF16)
        source = unit_qkv[b * per_chunk : (b + 1) * per_chunk, :, 0:nq].reshape(chunk, nq)
        picked = picked + jnp.dot(chosen, source, preferred_element_type=F32)
    for j in range(heads):
        part = slice(j * HD, (j + 1) * HD)
        q_s[j] = jnp.where(query_unit >= 0, picked[:, part], text_q[:, part].astype(F32)).astype(
            BF16
        )
    peak_s[...] = jnp.full_like(peak_s, NEGATIVE)
    mix_s[...] = jnp.zeros_like(mix_s)
    row_chunk = 128

    def fold(keys, values):
        values = jnp.concatenate([values, jnp.ones_like(values)], axis=1)
        for r in range(0, tokens, row_chunk):
            here = slice(r, r + row_chunk)
            for j in range(heads):
                scores = lax.dot_general(
                    q_s[j, here, :], keys, (((1,), (1,)), ((), ())), preferred_element_type=F32
                )
                scores = scores + bias_s[here, :]
                before = peak_s[j, here, :]
                peak = jnp.maximum(before, jnp.max(scores, axis=1, keepdims=True))
                factor = jnp.exp2((before - peak) * scale)
                wide_peak = jnp.concatenate([peak] * (scores.shape[1] // 128), axis=1)
                weights = jnp.exp2((scores - wide_peak) * scale).astype(BF16)
                peak_s[j, here, :] = peak
                mix_s[j, here, :] = mix_s[j, here, :] * jnp.concatenate(
                    [factor] * 2, axis=1
                ) + jnp.dot(weights, values, preferred_element_type=F32)

    def text_block(i, _):
        blocks = []
        for t in range(2):
            s = begin + 2 * i + t
            held = jnp.minimum(s, text_kv.shape[0] - 1)
            for g in range(lines):
                key_at = s * tokens + g * 128 + lane
                same = query_doc == doc_rows[pl.ds(held * lines + g, 1), :]
                text = unit_rows[pl.ds(held * lines + g, 1), :] < 0
                allowed = same & (key_at <= query_at) & text
                bias_s[:, t * tokens + g * 128 : t * tokens + (g + 1) * 128] = jnp.where(
                    allowed, 0.0, NEGATIVE
                )
            blocks.append(text_kv[held])
        both = jnp.concatenate(blocks, axis=0)
        fold(both[:, 0:nk], both[:, nk:])
        return 0

    begin = jnp.int32(0)
    for s in range(text_kv.shape[0]):
        begin = begin + (doc_smem[(s + 1) * tokens - 1] < first_doc).astype(jnp.int32)
    for text_load in text_loads:
        text_load.wait()
    lax.fori_loop(0, (mine + 2 - begin) // 2, text_block, 0)

    pair = 2 * chunk

    def unit_block(b, _):
        for g in range(pair // 128):
            code = unit_code[pl.ds(b * (pair // 128) + g, 1), :]
            allowed = (query_doc == (code & 63)) & ((code >> 6) <= query_at)
            bias_s[:, g * 128 : (g + 1) * 128] = jnp.where(allowed, 0.0, NEGATIVE)
        block = unit_qkv[pl.ds(b * 2 * per_chunk, 2 * per_chunk), :, nq:].reshape(pair, 2 * nk)
        fold(block[:, 0:nk], block[:, nk:])
        return 0

    lax.fori_loop(0, units // pair, unit_block, 0)
    for j in range(heads):
        out[:, j * HD : (j + 1) * HD] = (mix_s[j, :, 0:HD] / mix_s[j, :, HD:]).astype(BF16)


def attention(where, doc, text_q, text_kv, unit_qkv, unit_code, placeholder):
    tokens, nq = text_q.shape
    heads = nq // HD
    shards = text_kv.shape[1]
    whole = pl.BlockSpec(memory_space=VMEM)
    anywhere = pl.BlockSpec(memory_space=pl.ANY)
    scalars = pl.BlockSpec(memory_space=pltpu.SMEM)
    return pl.pallas_call(
        attention_kernel,
        out_shape=jax.ShapeDtypeStruct((tokens, nq), BF16),
        in_specs=[scalars] + [anywhere] * 7,
        out_specs=whole,
        scratch_shapes=[
            VMEM((shards, tokens, text_kv.shape[3]), BF16),
            VMEM((shards, 2 * unit_qkv.shape[2], unit_qkv.shape[3]), BF16),
            pltpu.SemaphoreType.DMA((9,)),
            VMEM((heads, tokens, HD), BF16),
            VMEM((heads, tokens, 128), F32),
            VMEM((heads, tokens, 2 * HD), F32),
            VMEM((tokens, 2 * tokens), F32),
            VMEM(text_q.shape, BF16),
            pltpu.SMEM(doc.shape, jnp.int32),
            VMEM(unit_code.shape, jnp.int32),
            VMEM((doc.shape[0] // 128, 128), jnp.int32),
            VMEM((doc.shape[0] // 128, 128), jnp.int32),
        ],
        compiler_params=pltpu.CompilerParams(vmem_limit_bytes=60 * 2**20),
        name="attention",
    )(
        where,
        doc,
        text_q,
        unit_code,
        doc.reshape(-1, 128),
        placeholder.reshape(-1, 128),
        text_kv,
        unit_qkv,
    )


def body(
    patches,
    patch_image,
    vit_gain,
    vit_qkv,
    vit_proj,
    merge_gain,
    merge_up,
    merge_down,
    text_embed,
    placeholder_unit,
    doc_id,
    dec_gain,
    dec_wq,
    dec_wk,
    dec_wv,
):
    tokens = text_embed.shape[0]
    text_q, text_kv, unit_qkv, unit_code = tower(
        patch_image.reshape(-1, 128),
        vit_gain.reshape(-1, 128),
        merge_gain.reshape(-1, 128),
        dec_gain.reshape(-1, 128),
        doc_id.reshape(-1, 128),
        placeholder_unit.reshape(-1, 128),
        patches,
        vit_qkv.transpose(1, 2, 0).reshape(-1, vit_qkv.shape[0]),
        vit_proj,
        merge_up.T,
        text_embed,
        merge_down,
        dec_wq,
        dec_wk,
        dec_wv,
    )
    where = lax.axis_index("ctx").astype(jnp.int32).reshape(1)
    return attention(
        where,
        doc_id,
        text_q.reshape(tokens, -1),
        text_kv.reshape(2, 16, tokens // 2, -1),
        unit_qkv.reshape(2, 16, -1, unit_qkv.shape[-1]),
        unit_code,
        placeholder_unit,
    )


def solution(mesh):
    placed = (
        P("enc", None),
        P("enc"),
        P(),
        P(None, "ctx", None),
        P("ctx", None),
        P(),
        P(None, "ctx"),
        P("ctx", "enc"),
        P("ctx", "enc"),
        P(),
        P(),
        P(),
        P(None, "enc"),
        P(None, "enc"),
        P(None, "enc"),
    )
    return jax.shard_map(
        body, mesh=mesh, in_specs=placed, out_specs=P("ctx", "enc"), check_vma=False
    )
```

```python
import functools
import math

import jax
import jax.numpy as jnp
from jax import lax
from jax.experimental import pallas as pl
from jax.experimental.pallas import tpu as pltpu
from jax.sharding import PartitionSpec as P

MESH = pl.DeviceIdType.MESH
VMEM = pltpu.VMEM
F32 = jnp.float32
BF16 = jnp.bfloat16

HD = 128
QPK = 4
EPSILON = 1e-06
NEGATIVE = -1e30
SIDE = 4


def places():
    e, c = lax.axis_index("enc"), lax.axis_index("ctx")
    return e // 2, lax.rem(e, 2), c // SIDE, lax.rem(c, SIDE)


def at_device(z, core, y, x):
    return {"enc": z * 2 + core, "ctx": y * SIDE + x}


def ring(position, distance):
    return lax.rem(position + distance, SIDE)


def remote(source, target, send_sem, recv_sem, device):
    return pltpu.make_async_remote_copy(
        src_ref=source,
        dst_ref=target,
        send_sem=send_sem,
        recv_sem=recv_sem,
        device_id=device,
        device_id_type=MESH,
    )


def ring_peers():
    z, core, y, x = places()
    peers = []
    for d in range(1, SIDE):
        peers.append(at_device(z, core, y, ring(x, d)))
        peers.append(at_device(z, core, ring(y, d), x))
        peers.append(at_device(ring(z, d), core, y, x))
    peers.append(at_device(z, 1 - core, y, x))
    return peers


def greet():
    for peer in ring_peers():
        pl.semaphore_signal(
            pltpu.get_barrier_semaphore(), inc=1, device_id=peer, device_id_type=MESH
        )


def meet():
    pl.semaphore_wait(pltpu.get_barrier_semaphore(), len(ring_peers()))


def row_of(ref, first, count):
    return jnp.concatenate([ref[pl.ds(first + g, 1), :] for g in range(count)], axis=1)


def column_of(ref, first, count):
    return jnp.concatenate(
        [jnp.broadcast_to(ref[pl.ds(first + g, 1), :], (128, 128)).T for g in range(count)],
        axis=0,
    )


class Gather:
    def __init__(self, buf, own, parts, sems, own_sem=None):
        self.buf, self.own, self.own_sem = buf, own, own_sem
        self.send, self.recv = sems
        self.part_a, self.part_b = parts

    def start(self, phase, pairs, distances):
        z, core, y, x = places()
        copies = {}
        for d in distances:
            for way, (source, target) in enumerate(pairs):
                along_x = way == phase
                device = (
                    at_device(z, core, y, ring(x, d))
                    if along_x
                    else at_device(z, core, ring(y, d), x)
                )
                sem = (2 * phase + way, d - 1)
                copies[way, d] = remote(
                    source, target, self.send.at[sem], self.recv.at[sem], device
                )
        for copy in copies.values():
            copy.start()
        return copies

    def first(self):
        z, core, y, x = places()
        if self.own_sem is not None:
            self.own_copy = pltpu.make_async_copy(self.own, self.buf.at[y, x], self.own_sem)
            self.own_copy.start()
        self.one = self.start(
            0,
            [
                (self.own.at[part], self.buf.at[(y, x) + part])
                for part in (self.part_a, self.part_b)
            ],
            (1, 2, 3),
        )

    def lines(self, row, column, some=slice(None)):
        return (
            self.buf.at[(row, some) + self.part_a],
            self.buf.at[(some, column) + self.part_b],
        )

    def second(self, relayed=False):
        z, core, y, x = places()
        if self.own_sem is not None:
            self.own_copy.wait()
        for copy in self.one.values():
            copy.wait_recv()
        self.relayed = relayed
        self.two = self.start(
            1, [(line, line) for line in self.lines(y, x)], (1, 3) if relayed else (1, 2, 3)
        )
        self.handed = {}

    def relay(self):
        z, core, y, x = places()
        for index, (d, some) in enumerate(((1, slice(0, 2)), (3, slice(2, 4)))):
            for way in range(2):
                self.two[way, d].wait_recv()
                line = self.lines(ring(y, SIDE - d), ring(x, SIDE - d), some)[way]
                device = (
                    at_device(z, core, ring(y, d), x)
                    if way == 0
                    else at_device(z, core, y, ring(x, d))
                )
                sem = (2 + way, 1 + 2 * index)
                self.handed[way, d] = remote(
                    line, line, self.send.at[sem], self.recv.at[sem], device
                )
                self.handed[way, d].start()

    def finish(self):
        for copy in (self.handed if self.relayed else self.two).values():
            copy.wait_recv()

    def drain(self):
        for copies in (self.one, self.two, self.handed):
            for copy in copies.values():
                copy.wait_send()


class EncGather:
    def __init__(self, buf, sems):
        self.buf = buf
        self.send, self.recv = sems

    def first(self, own):
        z, core, y, x = places()
        slot = z * 2 + core
        copies = [
            remote(
                own,
                self.buf.at[slot],
                self.send.at[d - 1],
                self.recv.at[d - 1],
                at_device(ring(z, d), core, y, x),
            )
            for d in range(1, SIDE)
        ]
        copies.append(
            remote(
                own,
                self.buf.at[slot],
                self.send.at[3],
                self.recv.at[3],
                at_device(z, 1 - core, y, x),
            )
        )
        for copy in copies:
            copy.start()
        self.copies = copies

    def second(self):
        z, core, y, x = places()
        self.handed = []
        for d in range(1, SIDE):
            self.copies[d - 1].wait_recv()
            slot = ring(z, SIDE - d) * 2 + core
            copy = remote(
                self.buf.at[slot],
                self.buf.at[slot],
                self.send.at[3 + d],
                self.recv.at[3 + d],
                at_device(z, 1 - core, y, x),
            )
            copy.start()
            self.handed.append(copy)

    def finish(self):
        self.copies[3].wait_recv()
        for copy in self.handed:
            copy.wait_recv()

    def drain(self):
        for copy in self.copies + self.handed:
            copy.wait_send()


class RelayGather:
    def __init__(self, buf, sems):
        self.buf = buf
        self.send, self.recv = sems
        self.copies = {}

    def copy(self, index, source, target, device):
        copy = remote(source, target, self.send.at[index], self.recv.at[index], device)
        copy.start()
        self.copies[index] = copy

    def first(self, own, high):
        z, core, y, x = places()
        middle, rows = self.buf.shape[1] // 2, self.buf.shape[1]
        slot = z * 2 + core
        part = slice(middle, rows) if high else slice(0, middle)
        for index, d in ((8, 1), (9, 3)) if high else ((0, 1), (1, 3)):
            self.copy(
                index,
                own.at[part],
                self.buf.at[slot, part],
                at_device(ring(z, d), core, y, x),
            )
        if not high:
            self.copy(2, own, self.buf.at[slot], at_device(z, 1 - core, y, x))

    def relay(self):
        z, core, y, x = places()
        middle = self.buf.shape[1] // 2
        left, right = ring(z, 3) * 2 + core, ring(z, 1) * 2 + core
        self.copies[0].wait_recv()
        low = self.buf.at[left, 0:middle]
        self.copy(3, low, low, at_device(ring(z, 1), core, y, x))
        self.copies[9].wait_recv()
        high = self.buf.at[right, middle:]
        self.copy(4, high, high, at_device(ring(z, 3), core, y, x))
        self.copies[1].wait_recv()
        self.copies[8].wait_recv()
        for index, block in ((5, left), (6, right)):
            whole = self.buf.at[block]
            self.copy(index, whole, whole, at_device(z, 1 - core, y, x))

    def second(self):
        z, core, y, x = places()
        self.copies[3].wait_recv()
        self.copies[4].wait_recv()
        far = self.buf.at[ring(z, 2) * 2 + core]
        self.copy(7, far, far, at_device(z, 1 - core, y, x))

    def finish(self):
        for index in (2, 5, 6, 7):
            self.copies[index].wait_recv()

    def drain(self):
        for copy in self.copies.values():
            copy.wait_send()


def halves(rows):
    return (slice(0, rows // 2), slice(None)), (slice(rows // 2, rows), slice(None))


def normed(wide, gain):
    center = wide - jnp.mean(wide, axis=1, keepdims=True)
    spread = jnp.mean(center * center, axis=1, keepdims=True)
    return (center * lax.rsqrt(spread + EPSILON) * gain).astype(BF16)


def gelu(x):
    return 0.5 * x * (1.0 + lax.erf(x * math.sqrt(0.5)))


def row_scale(total, count):
    return lax.rsqrt(total / count + EPSILON)


def tower_kernel(
    image,
    gain_rows,
    merge_gain_rows,
    dec_gain,
    doc,
    placeholder,
    patches_hbm,
    qkv_hbm,
    proj_hbm,
    up_hbm,
    text_hbm,
    down_hbm,
    wq_hbm,
    wk_hbm,
    wv_hbm,
    text_q,
    text_kv,
    unit_qkv,
    unit_code,
    patches,
    qkv,
    proj,
    up,
    down,
    w_s,
    q_s,
    k_s,
    v_s,
    o_s,
    lhs_s,
    norm_s,
    heads_all,
    proj_all,
    text_a,
    text_b,
    hidden_all,
    part_a,
    part_b,
    got_a,
    got_b,
    both_a,
    both_b,
    sum_a,
    sum_b,
    got_a2,
    got_b2,
    rows_all,
    acc_s,
    kv_own_a,
    kv_own_b,
    unit_own,
    code_s,
    local_sem,
    proj_s,
    proj_r,
    heads_s,
    heads_r,
    swap_s,
    swap_r,
    text_as,
    text_ar,
    text_bs,
    text_br,
    hid_s,
    hid_r,
    rs_s,
    rs_r,
    row_s,
    row_r,
    kva_s,
    kva_r,
    kvb_s,
    kvb_r,
    uq_s,
    uq_r,
):
    z, core, y, x = places()
    slot = z * 2 + core
    rows, width = patches.shape
    head = proj.shape[0]
    groups = heads_all.shape[3] // head
    group_rows = rows // groups
    side_cols = pl.ds(pl.multiple_of(core * (width // 2), 128), width // 2)
    blocks, tokens, cols = text_a.shape
    model = blocks * cols
    nq, nk = wq_hbm.shape[1], wk_hbm.shape[1]
    wide = nq + 2 * nk
    own_units = 2 * unit_own.shape[1]
    half = cols // 2
    chunk = 256

    def load(index, source, target):
        copy = pltpu.make_async_copy(source, target, local_sem.at[index])
        copy.start()
        return copy

    greet()
    proj_load = load(0, proj_hbm, proj)
    qkv_load = load(2, qkv_hbm, qkv)
    patches_load = load(1, patches_hbm, patches)
    text_loads = [
        load(3, text_hbm.at[0:tokens], text_a.at[slot]),
        load(4, text_hbm.at[tokens:], text_b.at[slot]),
    ]
    w_loads = [
        load(7, wq_hbm, w_s.at[:, 0:nq]),
        load(8, wk_hbm, w_s.at[:, nq : nq + nk]),
        load(9, wv_hbm, w_s.at[:, nq + nk : wide]),
    ]
    up_load = load(5, up_hbm, up)
    down_load = load(6, down_hbm, down)

    proj_load.wait()
    proj_all[y, x, :, side_cols] = proj[:, side_cols]
    meet()
    proj_gather = Gather(
        proj_all,
        proj,
        ((slice(0, 48), side_cols), (slice(48, head), side_cols)),
        (proj_s, proj_r),
    )
    proj_gather.first()
    text_gathers = [
        RelayGather(text_a, (text_as, text_ar)),
        RelayGather(text_b, (text_bs, text_br)),
    ]
    text_gathers[0].first(text_hbm.at[0:tokens], False)
    text_gathers[0].first(text_hbm.at[0:tokens], True)

    gain = row_of(gain_rows, 0, width // 128)
    merge_gain = row_of(merge_gain_rows, 0, width // 128)
    image_row = row_of(image, 0, rows // 128)
    patches_load.wait()
    qkv_load.wait()

    def project(i, _):
        here = pl.ds(pl.multiple_of(i * chunk, chunk), chunk)
        block = normed(patches[here, :].astype(F32), gain)
        packed = lax.dot_general(
            block, qkv[...], (((1,), (1,)), ((), ())), preferred_element_type=F32
        )
        q_s[here, :] = packed[:, 0:head].astype(BF16)
        k_s[here, :] = packed[:, head : 2 * head].astype(BF16)
        v_s[here, :] = packed[:, 2 * head : 3 * head].astype(BF16)
        return 0

    lax.fori_loop(0, rows // chunk, project, 0)

    scaling = head ** (-0.5)

    def attend(i, _):
        here = pl.ds(pl.multiple_of(i * chunk, chunk), chunk)
        ids_col = column_of(image, i * (chunk // 128), chunk // 128)[:, 0:1]
        scores = lax.dot_general(
            q_s[here, :], k_s[...], (((1,), (1,)), ((), ())), preferred_element_type=F32
        )
        scores = jnp.where(ids_col == image_row, scores * scaling, NEGATIVE)
        highest = jnp.max(scores, axis=1, keepdims=True)
        weights = jnp.exp(scores - highest)
        totals = jnp.sum(weights, axis=1, keepdims=True)
        mixture = jnp.dot(weights.astype(BF16), v_s[...], preferred_element_type=F32)
        o_s[here, :] = mixture / totals
        return 0

    lax.fori_loop(0, rows // chunk, attend, 0)
    heads_all[y, x] = jnp.concatenate(
        [o_s[j * group_rows : (j + 1) * group_rows, :] for j in range(groups)], axis=1
    ).astype(BF16)
    heads_gather = Gather(
        heads_all, heads_all.at[y, x], halves(group_rows), (heads_s, heads_r)
    )
    heads_gather.first()

    def scale_of(source):
        squares = jnp.zeros((source.shape[1], 128), F32)
        for b in range(blocks):
            for g in range(cols // 128):
                piece = source[b, :, g * 128 : (g + 1) * 128].astype(F32)
                squares = squares + piece * piece
        return row_scale(jnp.sum(squares, axis=1, keepdims=True), model)

    def decode_some(source, scale, first, last):
        count = source.shape[1]

        def one_block(b, _):
            block = (
                source[b].astype(F32)
                * scale
                * row_of(dec_gain, b * (cols // 128), cols // 128)
            )
            here = pl.ds(pl.multiple_of(b * cols, cols), cols)
            acc_s[0:count, :] += jnp.dot(
                block.astype(BF16), w_s[here, :], preferred_element_type=F32
            )
            return 0

        if first == 0:
            acc_s[0:count, :] = jnp.zeros((count, wide), F32)
        lax.fori_loop(first, last, one_block, 0)

    def text_begin(index, source):
        text_loads[index].wait()
        text_gathers[index].finish()
        scale = scale_of(source)
        decode_some(source, scale, 0, blocks // 2)
        return scale

    def text_end(index, source, scale, kv_own):
        decode_some(source, scale, blocks // 2, blocks)
        text_q[index] = acc_s[:, 0:nq].astype(BF16)
        kv_own[...] = acc_s[:, nq:].astype(BF16)

    lane_unit = lax.broadcasted_iota(jnp.int32, (128, 128), 0)
    position = lax.broadcasted_iota(jnp.int32, doc.shape, 0) * 128 + lax.broadcasted_iota(
        jnp.int32, doc.shape, 1
    )
    code_s[...] = position * 64 + doc[...]

    def units_block(b, _):
        unit = lane_unit + b * 128
        found = jnp.zeros((128, 128), jnp.int32)
        for r in range(placeholder.shape[0]):
            found = found + jnp.where(
                placeholder[r : r + 1, :] == unit, code_s[r : r + 1, :], 0
            )
        unit_code[pl.ds(b, 1), :] = jnp.sum(found.T, axis=0, keepdims=True)
        return 0

    proj_gather.second(relayed=True)
    heads_gather.second(relayed=True)
    text_gathers[0].relay()
    text_gathers[1].first(text_hbm.at[tokens:], False)
    text_gathers[1].first(text_hbm.at[tokens:], True)
    lax.fori_loop(0, unit_code.shape[0] // 2, units_block, 0)
    proj_gather.relay()
    lax.fori_loop(unit_code.shape[0] // 2, unit_code.shape[0], units_block, 0)
    text_gathers[0].second()
    heads_gather.relay()
    for w_load in w_loads:
        w_load.wait()
    text_scale = text_begin(0, text_a)
    proj_gather.finish()
    swap = remote(
        proj_all.at[:, :, :, side_cols],
        proj_all.at[:, :, :, side_cols],
        swap_s,
        swap_r,
        at_device(z, 1 - core, y, x),
    )
    swap.start()
    text_end(0, text_a, text_scale, kv_own_a)
    kv_a = Gather(
        text_kv.at[0], kv_own_a, halves(tokens), (kva_s, kva_r), own_sem=local_sem.at[10]
    )
    kv_a.first()
    heads_gather.finish()
    text_gathers[1].relay()

    for j in range(groups):
        lhs_s[j * group_rows : (j + 1) * group_rows, :] = jnp.concatenate(
            [
                heads_all[a, b, :, j * head : (j + 1) * head].astype(F32)
                for a in range(SIDE)
                for b in range(SIDE)
            ],
            axis=1,
        ).astype(BF16)

    swap.wait_recv()
    share = own_units // 2
    piece = 4 * share
    pieces = rows // piece // 2
    hidden_gathers = []
    for h in range(2):

        def merge(v, _):
            here = pl.ds(pl.multiple_of((2 * v + h) * piece, piece), piece)
            terms = jnp.dot(
                lhs_s[here, :], proj_all[...].reshape(width, width), preferred_element_type=F32
            )
            out = (patches[here, :].astype(F32) + terms).astype(BF16)
            ready = normed(out.astype(F32), merge_gain).astype(F32)
            for g in range(width // 128):
                norm_s[g, here, :] = ready[:, g * 128 : (g + 1) * 128]
            return 0

        lax.fori_loop(0, pieces, merge, 0)
        if h == 0:
            up_load.wait()
        total = jnp.zeros((pieces * share, up.shape[0]), F32)
        for k in range(4):
            quarter = jnp.concatenate(
                [
                    jnp.concatenate(
                        [
                            norm_s[g, pl.ds((2 * v + h) * piece + k, share, stride=4), :]
                            for g in range(width // 128)
                        ],
                        axis=1,
                    )
                    for v in range(pieces)
                ],
                axis=0,
            ).astype(BF16)
            total = total + lax.dot_general(
                quarter,
                up[:, k * width : (k + 1) * width],
                (((1,), (1,)), ((), ())),
                preferred_element_type=F32,
            )
        hidden_all[h, slot] = gelu(total).astype(BF16)
        hidden_gathers.append(EncGather(hidden_all.at[h], (hid_s.at[h], hid_r.at[h])))
        hidden_gathers[h].first(hidden_all.at[h, slot])
        if h == 0:
            kv_a.second(relayed=True)
    text_gathers[1].second()
    down_load.wait()

    one, two = [{}, {}], [[], []]

    def share_rows(index):
        return pl.ds(pl.multiple_of(index * share, share), share)

    def summed(own, others):
        return sum((others[d].astype(F32) for d in range(SIDE - 1)), own.astype(F32))

    ring_ways = (
        (part_a, got_a, both_a, slice(0, half)),
        (part_b, got_b, both_b, slice(half, cols)),
    )
    low, high = slice(0, half // 2), slice(half // 2, half)

    def neighbour(way, d):
        return at_device(z, core, y, ring(x, d)) if way == 0 else at_device(z, core, ring(y, d), x)

    def pass_on(h, way, index, source, d):
        copy = remote(
            source,
            ring_ways[way][1].at[h, index],
            rs_s.at[h, way, index],
            rs_r.at[h, way, index],
            neighbour(way, d),
        )
        copy.start()
        one[h][way, index] = copy

    def terms(h):
        for d in (2, 1, 3, 0):
            xp, yp = ring(x, d), ring(y, d)
            lhs_a = jnp.concatenate(
                [
                    hidden_all[h, 2 * v + xp // 2, share_rows(lax.rem(xp, 2)), :]
                    for v in range(SIDE)
                ],
                axis=0,
            )
            lhs_b = jnp.concatenate(
                [hidden_all[h, 2 * yp + v // 2, share_rows(v % 2), :] for v in range(SIDE)],
                axis=0,
            )
            for way, lhs in enumerate((lhs_a, lhs_b)):
                part, got, both, columns = ring_ways[way]
                part[h, d] = jnp.dot(
                    lhs, down[:, columns], preferred_element_type=F32
                ).astype(BF16)
                if d == 2:
                    pass_on(h, way, 0, part.at[h, d, :, low], 1)
                    pass_on(h, way, 1, part.at[h, d, :, high], 3)
                elif d == 1:
                    pass_on(h, way, 2, part.at[h, d, :, high], 1)
                elif d == 3:
                    pass_on(h, way, 3, part.at[h, d, :, low], 3)

    def combine(h):
        for way in range(2):
            part, got, both, columns = ring_ways[way]
            for index, (d, side) in enumerate(((1, low), (3, high))):
                one[h][way, index].wait_recv()
                both[h, index] = (
                    part[h, d, :, side].astype(F32) + got[h, index].astype(F32)
                ).astype(BF16)
                pass_on(h, way, 4 + index, both.at[h, index], d)

    def ring_total(h, way):
        part, got, both, columns = ring_ways[way]
        for index in range(2, 6):
            one[h][way, index].wait_recv()
        others = jnp.concatenate(
            [
                got[h, 4].astype(F32) + got[h, 3].astype(F32),
                got[h, 2].astype(F32) + got[h, 5].astype(F32),
            ],
            axis=1,
        )
        return (part[h, 0].astype(F32) + others).astype(BF16)

    def ring_sums(h):
        sum_a[h] = ring_total(h, 0)
        sum_b[h] = ring_total(h, 1)
        for d in range(1, SIDE):
            xp, yp = ring(x, d), ring(y, d)
            for way, (total_s, place, got, device) in enumerate(
                (
                    (sum_a, yp, got_a2, at_device(z, core, yp, x)),
                    (sum_b, xp, got_b2, at_device(z, core, y, xp)),
                )
            ):
                copy = remote(
                    total_s.at[h, share_rows(place)],
                    got.at[h, d - 1],
                    rs_s.at[h, 2 + way, d - 1],
                    rs_r.at[h, 2 + way, d - 1],
                    device,
                )
                copy.start()
                two[h].append(copy)

    rows_gathers = [
        EncGather(rows_all.at[h], (row_s.at[h], row_r.at[h])) for h in range(2)
    ]

    def full_sums(h):
        for copy in two[h]:
            copy.wait_recv()
        rows_all[h, slot] = jnp.concatenate(
            [
                summed(sum_a[h, share_rows(y), :], got_a2.at[h]),
                summed(sum_b[h, share_rows(x), :], got_b2.at[h]),
            ],
            axis=1,
        ).astype(BF16)
        rows_gathers[h].first(rows_all.at[h, slot])

    unit_parts = (
        (slice(0, share), slice(0, wide // 2)),
        (slice(0, share), slice(wide // 2, wide)),
    )
    unit_gathers = [
        Gather(
            unit_qkv.at[h],
            unit_own.at[h],
            unit_parts,
            (uq_s.at[h], uq_r.at[h]),
            own_sem=local_sem.at[12 + h],
        )
        for h in range(2)
    ]

    def add_block(b):
        block = rows_all[1, b].astype(F32) * row_of(dec_gain, b * (cols // 128), cols // 128)
        here = pl.ds(pl.multiple_of(b * cols, cols), cols)
        acc_s[0:share, :] += jnp.dot(
            block.astype(BF16), w_s[here, :], preferred_element_type=F32
        )

    def add_blocks(first, side):
        def one(d, _):
            add_block(ring(z, d) * 2 + side)
            return 0

        lax.fori_loop(first, SIDE, one, 0)

    def decode_units(h):
        source = rows_all.at[h]
        decode_some(source, scale_of(source), 0, blocks)
        unit_own[h] = acc_s[0:share, :].astype(BF16)
        unit_gathers[h].first()

    hidden_gathers[0].second()
    hidden_gathers[0].finish()
    terms(0)
    kv_a.relay()
    hidden_gathers[1].second()
    text_scale = text_begin(1, text_b)
    hidden_gathers[1].finish()
    combine(0)
    terms(1)
    text_end(1, text_b, text_scale, kv_own_b)
    kv_b = Gather(
        text_kv.at[1], kv_own_b, halves(tokens), (kvb_s, kvb_r), own_sem=local_sem.at[11]
    )
    ring_sums(0)
    combine(1)
    kv_b.first()
    full_sums(0)
    ring_sums(1)
    rows_gathers[0].second()
    full_sums(1)
    kv_b.second(relayed=True)
    rows_gathers[0].finish()
    decode_units(0)
    acc_s[0:share, :] = jnp.zeros((share, wide), F32)
    add_block(slot)
    rows_gathers[1].second()
    add_blocks(1, core)
    rows_gathers[1].finish()
    unit_gathers[0].second(relayed=True)
    add_blocks(0, 1 - core)
    unit_own[1] = (acc_s[0:share, :] * scale_of(rows_all.at[1])).astype(BF16)
    unit_gathers[1].first()
    kv_b.relay()
    unit_gathers[0].relay()
    unit_gathers[1].second()
    for gather in unit_gathers + [kv_a, kv_b]:
        gather.finish()
    swap.wait_send()
    for copy in [*one[0].values(), *one[1].values(), *two[0], *two[1]]:
        copy.wait_send()
    for gather in [proj_gather, heads_gather, kv_a, kv_b] + unit_gathers:
        gather.drain()
    for gather in text_gathers + hidden_gathers + rows_gathers:
        gather.drain()


def tower(
    image,
    gain,
    merge_gain,
    dec_gain,
    doc,
    placeholder,
    patches,
    qkv,
    proj,
    up,
    text,
    down,
    wq,
    wk,
    wv,
):
    rows, width = patches.shape
    head = proj.shape[0]
    groups = 8
    units = rows // 4
    cols = text.shape[1]
    tokens = text.shape[0] // 2
    nq, nk = wq.shape[1], wk.shape[1]
    wide = nq + 2 * nk
    own_units = 8 * units // (SIDE * SIDE)
    share = own_units // 2
    half = cols // 2
    dma = pltpu.SemaphoreType.DMA
    whole = pl.BlockSpec(memory_space=VMEM)
    anywhere = pl.BlockSpec(memory_space=pl.ANY)

    def both(shape):
        return [dma(shape), dma(shape)]

    return pl.pallas_call(
        tower_kernel,
        out_shape=(
            jax.ShapeDtypeStruct((2, tokens, nq), BF16),
            jax.ShapeDtypeStruct((2, SIDE, SIDE, tokens, 2 * nk), BF16),
            jax.ShapeDtypeStruct((2, SIDE, SIDE, share, wide), BF16),
            jax.ShapeDtypeStruct((own_units * 16 // 128, 128), jnp.int32),
        ),
        in_specs=[whole] * 6 + [anywhere] * 9,
        out_specs=(whole, anywhere, anywhere, whole),
        scratch_shapes=[
            VMEM((rows, width), BF16),
            VMEM(qkv.shape, BF16),
            VMEM((head, width), BF16),
            VMEM(up.shape, BF16),
            VMEM(down.shape, BF16),
            VMEM((8 * cols, wide), BF16),
            VMEM((rows, head), BF16),
            VMEM((rows, head), BF16),
            VMEM((rows, head), BF16),
            VMEM((rows, head), F32),
            VMEM((rows, width), BF16),
            VMEM((width // 128, rows, 128), F32),
            VMEM((SIDE, SIDE, rows // groups, groups * head), BF16),
            VMEM((SIDE, SIDE, head, width), BF16),
            VMEM((8, tokens, cols), BF16),
            VMEM((8, tokens, cols), BF16),
            VMEM((2, 8, units // 2, up.shape[0]), BF16),
            VMEM((2, SIDE, SIDE * share, half), BF16),
            VMEM((2, SIDE, SIDE * share, half), BF16),
            VMEM((2, 6, SIDE * share, half // 2), BF16),
            VMEM((2, 6, SIDE * share, half // 2), BF16),
            VMEM((2, 2, SIDE * share, half // 2), BF16),
            VMEM((2, 2, SIDE * share, half // 2), BF16),
            VMEM((2, SIDE * share, half), BF16),
            VMEM((2, SIDE * share, half), BF16),
            VMEM((2, SIDE - 1, share, half), BF16),
            VMEM((2, SIDE - 1, share, half), BF16),
            VMEM((2, 8, share, cols), BF16),
            VMEM((tokens, wide), F32),
            VMEM((tokens, 2 * nk), BF16),
            VMEM((tokens, 2 * nk), BF16),
            VMEM((2, share, wide), BF16),
            VMEM(doc.shape, jnp.int32),
            dma((14,)),
            *both((4, 4)),
            *both((4, 4)),
            *both(()),
            *both((10,)),
            *both((10,)),
            *both((2, 7)),
            *both((2, 4, 6)),
            *both((2, 7)),
            *both((4, 4)),
            *both((4, 4)),
            *both((2, 4, 4)),
        ],
        compiler_params=pltpu.CompilerParams(
            collective_id=1, has_side_effects=True, vmem_limit_bytes=60 * 2**20
        ),
        name="tower",
    )(
        image,
        gain,
        merge_gain,
        dec_gain,
        doc,
        placeholder,
        patches,
        qkv,
        proj,
        up,
        text,
        down,
        wq,
        wk,
        wv,
    )


def attention_kernel(
    where_ref,
    doc_hbm,
    text_q_hbm,
    unit_code_hbm,
    doc_rows_hbm,
    unit_rows_hbm,
    text_kv_hbm,
    unit_qkv_hbm,
    out,
    text_kv,
    unit_qkv,
    load_sem,
    q_s,
    peak_s,
    mix_s,
    bias_s,
    text_q,
    doc_smem,
    unit_code,
    doc_rows,
    unit_rows,
):
    tokens, nq = text_q.shape
    nk = text_kv.shape[2] // 2
    small_loads = []
    for index, (source, target) in enumerate(
        (
            (doc_rows_hbm, doc_rows),
            (unit_rows_hbm, unit_rows),
            (text_q_hbm, text_q),
            (unit_code_hbm, unit_code),
            (doc_hbm, doc_smem),
        )
    ):
        small_loads.append(pltpu.make_async_copy(source, target, load_sem.at[4 + index]))
        small_loads[index].start()
    unit_loads = []
    for p in range(2):
        share = unit_qkv.shape[1] // 2
        here = slice(p * share, (p + 1) * share)
        unit_loads.append(
            pltpu.make_async_copy(
                unit_qkv_hbm.at[p], unit_qkv.at[:, here, :], load_sem.at[2 + p]
            )
        )
        unit_loads[p].start()
    text_loads = []
    for p in range(2):
        here = slice(p * (tokens // 2), (p + 1) * (tokens // 2))
        text_loads.append(
            pltpu.make_async_copy(text_kv_hbm.at[p], text_kv.at[:, here, :], load_sem.at[p])
        )
        text_loads[p].start()
    heads = nq // HD
    units = unit_qkv.shape[0] * unit_qkv.shape[1]
    mine = where_ref[0]
    scale = HD ** (-0.5) * math.log2(math.e)

    lines = tokens // 128
    for small_load in small_loads:
        small_load.wait()
    first_doc = doc_smem[mine * tokens]
    query_doc = column_of(doc_rows, mine * lines, lines)
    query_unit = column_of(unit_rows, mine * lines, lines)
    query_at = mine * tokens + lax.broadcasted_iota(jnp.int32, (tokens, 128), 0)
    lane = lax.broadcasted_iota(jnp.int32, (tokens, 128), 1)

    picked = jnp.zeros((tokens, nq), F32)
    chunk = 384
    for unit_load in unit_loads:
        unit_load.wait()
    per_chunk = chunk // unit_qkv.shape[1]
    for b in range(units // chunk):
        chosen = jnp.concatenate(
            [
                (query_unit == lane + (b * chunk + g * 128)).astype(F32)
                for g in range(chunk // 128)
            ],
            axis=1,
        ).astype(BF16)
        source = unit_qkv[b * per_chunk : (b + 1) * per_chunk, :, 0:nq].reshape(chunk, nq)
        picked = picked + jnp.dot(chosen, source, preferred_element_type=F32)
    for j in range(heads):
        part = slice(j * HD, (j + 1) * HD)
        q_s[j] = jnp.where(query_unit >= 0, picked[:, part], text_q[:, part].astype(F32)).astype(
            BF16
        )
    peak_s[...] = jnp.full_like(peak_s, NEGATIVE)
    mix_s[...] = jnp.zeros_like(mix_s)
    row_chunk = 128

    def fold(keys, values):
        values = jnp.concatenate([values, jnp.ones_like(values)], axis=1)
        for r in range(0, tokens, row_chunk):
            here = slice(r, r + row_chunk)
            for j in range(heads):
                scores = lax.dot_general(
                    q_s[j, here, :], keys, (((1,), (1,)), ((), ())), preferred_element_type=F32
                )
                scores = scores + bias_s[here, :]
                before = peak_s[j, here, :]
                peak = jnp.maximum(before, jnp.max(scores, axis=1, keepdims=True))
                factor = jnp.exp2((before - peak) * scale)
                wide_peak = jnp.concatenate([peak] * (scores.shape[1] // 128), axis=1)
                weights = jnp.exp2((scores - wide_peak) * scale).astype(BF16)
                peak_s[j, here, :] = peak
                mix_s[j, here, :] = mix_s[j, here, :] * jnp.concatenate(
                    [factor] * 2, axis=1
                ) + jnp.dot(weights, values, preferred_element_type=F32)

    def text_block(i, _):
        blocks = []
        for t in range(2):
            s = begin + 2 * i + t
            held = jnp.minimum(s, text_kv.shape[0] - 1)
            for g in range(lines):
                key_at = s * tokens + g * 128 + lane
                same = query_doc == doc_rows[pl.ds(held * lines + g, 1), :]
                text = unit_rows[pl.ds(held * lines + g, 1), :] < 0
                allowed = same & (key_at <= query_at) & text
                bias_s[:, t * tokens + g * 128 : t * tokens + (g + 1) * 128] = jnp.where(
                    allowed, 0.0, NEGATIVE
                )
            blocks.append(text_kv[held])
        both = jnp.concatenate(blocks, axis=0)
        fold(both[:, 0:nk], both[:, nk:])
        return 0

    begin = jnp.int32(0)
    for s in range(text_kv.shape[0]):
        begin = begin + (doc_smem[(s + 1) * tokens - 1] < first_doc).astype(jnp.int32)
    for text_load in text_loads:
        text_load.wait()
    lax.fori_loop(0, (mine + 2 - begin) // 2, text_block, 0)

    pair = 2 * chunk

    def unit_block(b, _):
        for g in range(pair // 128):
            code = unit_code[pl.ds(b * (pair // 128) + g, 1), :]
            allowed = (query_doc == (code & 63)) & ((code >> 6) <= query_at)
            bias_s[:, g * 128 : (g + 1) * 128] = jnp.where(allowed, 0.0, NEGATIVE)
        block = unit_qkv[pl.ds(b * 2 * per_chunk, 2 * per_chunk), :, nq:].reshape(pair, 2 * nk)
        fold(block[:, 0:nk], block[:, nk:])
        return 0

    lax.fori_loop(0, units // pair, unit_block, 0)
    for j in range(heads):
        out[:, j * HD : (j + 1) * HD] = (mix_s[j, :, 0:HD] / mix_s[j, :, HD:]).astype(BF16)


def attention(where, doc, text_q, text_kv, unit_qkv, unit_code, placeholder):
    tokens, nq = text_q.shape
    heads = nq // HD
    shards = text_kv.shape[1]
    whole = pl.BlockSpec(memory_space=VMEM)
    anywhere = pl.BlockSpec(memory_space=pl.ANY)
    scalars = pl.BlockSpec(memory_space=pltpu.SMEM)
    return pl.pallas_call(
        attention_kernel,
        out_shape=jax.ShapeDtypeStruct((tokens, nq), BF16),
        in_specs=[scalars] + [anywhere] * 7,
        out_specs=whole,
        scratch_shapes=[
            VMEM((shards, tokens, text_kv.shape[3]), BF16),
            VMEM((shards, 2 * unit_qkv.shape[2], unit_qkv.shape[3]), BF16),
            pltpu.SemaphoreType.DMA((9,)),
            VMEM((heads, tokens, HD), BF16),
            VMEM((heads, tokens, 128), F32),
            VMEM((heads, tokens, 2 * HD), F32),
            VMEM((tokens, 2 * tokens), F32),
            VMEM(text_q.shape, BF16),
            pltpu.SMEM(doc.shape, jnp.int32),
            VMEM(unit_code.shape, jnp.int32),
            VMEM((doc.shape[0] // 128, 128), jnp.int32),
            VMEM((doc.shape[0] // 128, 128), jnp.int32),
        ],
        compiler_params=pltpu.CompilerParams(vmem_limit_bytes=60 * 2**20),
        name="attention",
    )(
        where,
        doc,
        text_q,
        unit_code,
        doc.reshape(-1, 128),
        placeholder.reshape(-1, 128),
        text_kv,
        unit_qkv,
    )


def body(
    patches,
    patch_image,
    vit_gain,
    vit_qkv,
    vit_proj,
    merge_gain,
    merge_up,
    merge_down,
    text_embed,
    placeholder_unit,
    doc_id,
    dec_gain,
    dec_wq,
    dec_wk,
    dec_wv,
):
    tokens = text_embed.shape[0]
    text_q, text_kv, unit_qkv, unit_code = tower(
        patch_image.reshape(-1, 128),
        vit_gain.reshape(-1, 128),
        merge_gain.reshape(-1, 128),
        dec_gain.reshape(-1, 128),
        doc_id.reshape(-1, 128),
        placeholder_unit.reshape(-1, 128),
        patches,
        vit_qkv.transpose(1, 2, 0).reshape(-1, vit_qkv.shape[0]),
        vit_proj,
        merge_up.T,
        text_embed,
        merge_down,
        dec_wq,
        dec_wk,
        dec_wv,
    )
    where = lax.axis_index("ctx").astype(jnp.int32).reshape(1)
    return attention(
        where,
        doc_id,
        text_q.reshape(tokens, -1),
        text_kv.reshape(2, 16, tokens // 2, -1),
        unit_qkv.reshape(2, 16, -1, unit_qkv.shape[-1]),
        unit_code,
        placeholder_unit,
    )


def solution(mesh):
    placed = (
        P("enc", None),
        P("enc"),
        P(),
        P(None, "ctx", None),
        P("ctx", None),
        P(),
        P(None, "ctx"),
        P("ctx", "enc"),
        P("ctx", "enc"),
        P(),
        P(),
        P(),
        P(None, "enc"),
        P(None, "enc"),
        P(None, "enc"),
    )
    return jax.shard_map(
        body, mesh=mesh, in_specs=placed, out_specs=P("ctx", "enc"), check_vma=False
    )
```
